128 devices in a mesh: batch: 1, col: 16 (over z, y), row: 8 (over x, core).
Axes of the slice: x: 4, y: 4, z: 4, core: 2. Of those that a mesh axis runs over, the one named last changes fastest.
Arguments:
- lower_tri: float32 [6144, 6144], P(('batch', 'row'), 'col')
Outputs:
- output: float32 [6144, 6144], P(('batch', 'row'), 'col')
All inputs are finite; a program needn't handle non-finite values.
Results may differ from the reference program's by a relative error of at most 0.001.
Values sent between devices are 32-bit elements.
A program may use at most 1 GiB of HBM per device.

```python
import jax
import jax.numpy as jnp
from jax import lax

N = 6144
DEPTH = 4
HIGHEST = lax.Precision.HIGHEST


def setup_inputs(seed: int = 0, part: int = 0) -> dict:
    base_key = jax.random.fold_in(jax.random.key(seed), part)
    key_off, key_diag = jax.random.split(base_key)
    entries = jax.random.normal(key_off, (N, N), jnp.float32) * (N ** -0.5)
    diag_vals = jax.random.uniform(key_diag, (N,), jnp.float32, 2.0, 4.0)
    lower_tri = jnp.tril(entries, -1) + jnp.diag(diag_vals)
    return {"lower_tri": lower_tri}


def invert_lower(sub_block, depth_n):
    full_size = sub_block.shape[0]
    if depth_n == 0:
        unit_mat = jnp.eye(full_size, dtype=jnp.float32)
        return lax.linalg.triangular_solve(sub_block, unit_mat, left_side=True, lower=True)
    half_size = full_size // 2
    inv_a = invert_lower(sub_block[:half_size, :half_size], depth_n - 1)
    inv_b = invert_lower(sub_block[half_size:, half_size:], depth_n - 1)
    low_c = sub_block[half_size:, :half_size]
    prod_t = jnp.dot(low_c, inv_a, precision=HIGHEST, preferred_element_type=jnp.float32)
    low_x = -jnp.dot(inv_b, prod_t, precision=HIGHEST, preferred_element_type=jnp.float32)
    top_half = jnp.concatenate([inv_a, jnp.zeros_like(inv_a)], axis=1)
    bottom = jnp.concatenate([low_x, inv_b], axis=1)
    return jnp.concatenate([top_half, bottom], axis=0)


def reference(lower_tri):
    inv_l = invert_lower(lower_tri, DEPTH)
    contract_dims = (((0,), (0,)), ((), ()))
    return lax.dot_general(inv_l, inv_l, contract_dims, precision=HIGHEST, preferred_element_type=jnp.float32)
```

```python
import functools

import jax
import jax.numpy as jnp
from jax import lax
from jax.experimental import pallas as pl
from jax.experimental.pallas import tpu as pltpu
from jax.sharding import PartitionSpec as P

MESH = pl.DeviceIdType.MESH
HIGHEST = lax.Precision.HIGHEST
F32 = jnp.float32
VMEM_LIMIT = 60 * 1024 * 1024
BASE = 128


def coords():
    col = lax.axis_index("col")
    row = lax.axis_index("row")
    return {"x": row // 2, "y": col % 4, "z": col // 4, "e": row % 2}


def device(at):
    return (0, 4 * at["z"] + at["y"], 2 * at["x"] + at["e"])


def same(p, q):
    return (p["x"] == q["x"]) & (p["y"] == q["y"]) & (p["z"] == q["z"]) & (p["e"] == q["e"])


def mm(a, b, dims=((1,), (0,))):
    return lax.dot_general(a, b, (dims, ((), ())), precision=HIGHEST, preferred_element_type=F32)


def push(src, dst, send_sem, recv_sem, to, me):
    here = same(to, me)

    @pl.when(here)
    def _():
        dst[...] = src[...]

    @pl.when(jnp.logical_not(here))
    def _():
        pltpu.make_async_remote_copy(
            src_ref=src, dst_ref=dst, send_sem=send_sem, recv_sem=recv_sem, device_id=device(to), device_id_type=MESH
        ).start()


def sent(src, dst, send_sem, recv_sem, to, me):
    @pl.when(jnp.logical_not(same(to, me)))
    def _():
        pltpu.make_async_remote_copy(
            src_ref=src, dst_ref=dst, send_sem=send_sem, recv_sem=recv_sem, device_id=device(to), device_id_type=MESH
        ).wait_send()


def arrived(dst, send_sem, recv_sem, source, me):
    @pl.when(jnp.logical_not(same(source, me)))
    def _():
        pltpu.make_async_remote_copy(
            src_ref=dst, dst_ref=dst, send_sem=send_sem, recv_sem=recv_sem, device_id=device(source), device_id_type=MESH
        ).wait_recv()


def meet(sources, dests, me):
    barrier = pltpu.get_barrier_semaphore()

    def other(cond, at):
        apart = jnp.logical_not(same(at, me))
        return apart if cond is None else apart & cond

    for cond, at in sources:
        @pl.when(other(cond, at))
        def _(at=at):
            pl.semaphore_signal(barrier, inc=1, device_id=device(at), device_id_type=MESH)

    total = sum(other(cond, at).astype(jnp.int32) for cond, at in dests)

    @pl.when(total > 0)
    def _():
        pl.semaphore_wait(barrier, total)


def invert_block(left, corner, inv, base):
    half = 3 * base
    rows = lax.broadcasted_iota(jnp.int32, (base, base), 0)
    cols = lax.broadcasted_iota(jnp.int32, (base, base), 1)
    eye = rows == cols

    def block(i, j):
        if j < 3:
            return left[i * base:(i + 1) * base, j * base:(j + 1) * base]
        return corner[(i - 3) * base:(i - 2) * base, (j - 3) * base:(j - 2) * base]

    tri = [block(i, i) for i in range(6)]
    found = []
    for i in range(6):
        diag = jnp.sum(jnp.where(eye, tri[i], 0.0), axis=1, keepdims=True)
        found.append(jnp.where(eye, 1.0 / diag, 0.0))
    size = 1
    while size < base:
        below = ((rows // size) % 2 == 1) & (cols // size == rows // size - 1)
        half_way = [mm(jnp.where(below, tri[i], 0.0), found[i]) for i in range(6)]
        found = [found[i] - mm(found[i], half_way[i]) for i in range(6)]
        size = size * 2
    inv[...] = jnp.zeros(inv.shape, F32)
    for k in (0, 3):
        x0, x1, x2 = found[k:k + 3]
        x10 = -mm(x1, mm(block(k + 1, k), x0))
        x21 = -mm(x2, mm(block(k + 2, k + 1), x1))
        x20 = -mm(x2, mm(block(k + 2, k), x0) + mm(block(k + 2, k + 1), x10))
        for i, j, val in ((0, 0, x0), (1, 1, x1), (2, 2, x2), (1, 0, x10), (2, 1, x21), (2, 0, x20)):
            inv[(k + i) * base:(k + i + 1) * base, (k + j) * base:(k + j + 1) * base] = val
    low = mm(left[half:, :], inv[:half, :half])
    inv[half:, :half] = -mm(inv[half:, half:], low)


def stage0_kernel(n, l_ref, lt_ref, ct_out, d_out, g_out, dt_out,
                  left, corner, cmat, inv_a, inv_b, inv_t, slab_d, slab_t, slab_g,
                  ct_send, ct_recv, ab_send, ab_recv, c_send, c_recv, x_send, x_recv, t_send, t_recv):
    me = coords()
    x, y, z, e = me["x"], me["y"], me["z"], me["e"]
    big = n // 8
    half = n // 16
    quarter = n // 32
    tile = n // 128
    sib = dict(me, e=1 - e)
    diag = x == z

    slot = (x * (x - 1)) // 2 + z
    hops = [(ee, g, h) for g in range(4) for ee in range(2) for h in range(2)]

    def ct_args(ee, g, h):
        src = lt_ref.at[pl.ds(quarter * ee + tile * g, tile), pl.ds(half * h, half)]
        to = {"x": jnp.int32(g), "y": y, "z": 2 * e + h, "e": jnp.int32(ee)}
        return src, ct_out.at[slot], ct_send.at[ee * 8 + g * 2 + h], ct_recv.at[slot], to, me

    source = diag & (y // 2 == e)
    c_source = diag & (e == 1) & (y < 2)

    def at(b, along_y):
        return {"x": jnp.int32(b), "y": along_y, "z": jnp.int32(b), "e": e}

    odd = x % 2

    def dest(kind, g, j):
        if kind == 0:
            return {"x": jnp.int32(j), "y": y, "z": jnp.int32(g), "e": e}
        if kind == 1:
            return {"x": odd * g + (1 - odd) * j, "y": odd * j + (1 - odd) * g, "z": y, "e": e}
        return {"x": jnp.int32(g), "y": jnp.int32(j), "z": y, "e": e}

    every = [(kind, g, j) for kind in range(3) for g in range(4) for j in range(4)]
    pairs = [(b_row, b_col) for b_row in range(4) for b_col in range(b_row)]

    def ct_source(b_row, b_col):
        return {"x": jnp.int32(b_row), "y": y, "z": jnp.int32(b_col), "e": z // 2}

    sources = [(None, ct_source(*pair)) for pair in pairs] + [(diag, sib)]
    sources += [(diag, dict(me, y=2 * e + part)) for part in range(2)]
    sources += [(diag & (e == 1), dict(me, y=jnp.int32(part))) for part in range(2)]
    sources += [(None, at(b, v)) for b in range(4) for v in (y, z)] + [(None, at(1, z))]
    dests = [(x > z, ct_args(*hop)[4]) for hop in hops] + [(diag, sib)]
    dests += [(cond, dict(me, y=(y + k) % 4)) for cond in (source, c_source) for k in range(1, 4)]
    dests += [(diag if kind < 2 else diag & (x == 1), dest(kind, g, j)) for kind, g, j in every]
    meet(sources, dests, me)

    def ab_args(k, part):
        to = dict(me, y=(y + k) % 4)
        if part == 0:
            return l_ref, left, ab_send.at[k - 1], ab_recv.at[0], to, me
        return l_ref.at[pl.ds(half, half), :], corner, ab_send.at[k - 1], ab_recv.at[1], to, me

    for part in range(2):
        @pl.when(source & (y % 2 == part))
        def _(part=part):
            for k in (1, 3, 2):
                push(*ab_args(k, part))

    def c_args(k):
        to = dict(me, y=(y + k) % 4)
        return l_ref, cmat.at[y % 2], c_send.at[k - 1], c_recv.at[y % 2], to, me

    @pl.when(c_source)
    def _():
        for k in (1, 3, 2):
            push(*c_args(k))

    @pl.when(x > z)
    def _():
        for hop in hops:
            push(*ct_args(*hop))

    def swap_args(k):
        mine = [inv_a, inv_b, cmat.at[0], cmat.at[1]][k]
        return mine, mine, x_send.at[k], x_recv.at[k], sib, me

    @pl.when(diag)
    def _():
        for part, (dst, src_rows) in enumerate(((left, 0), (corner, half))):
            @pl.when(source & (y % 2 == part))
            def _(dst=dst, src_rows=src_rows):
                dst[...] = l_ref[src_rows:, :]

            arrived(dst, ab_send.at[0], ab_recv.at[part], dict(me, y=2 * e + part), me)

        invert_block(left, corner, inv_t, n // 48)
        for core, inv in ((0, inv_a), (1, inv_b)):
            @pl.when(e == core)
            def _(inv=inv):
                inv[...] = inv_t[...]

        @pl.when(e == 0)
        def _():
            push(*swap_args(0))
            for k in (1, 2, 3):
                arrived(swap_args(k)[1], x_send.at[k], x_recv.at[k], sib, me)
            sent(*swap_args(0))

        @pl.when(e == 1)
        def _():
            push(*swap_args(1))
            for part in range(2):
                @pl.when(y == part)
                def _(part=part):
                    cmat[part] = l_ref[...]

                arrived(cmat.at[part], c_send.at[0], c_recv.at[part], dict(me, y=jnp.int32(part)), me)
                push(*swap_args(2 + part))
            arrived(inv_a, x_send.at[0], x_recv.at[0], sib, me)
            for k in (1, 2, 3):
                sent(*swap_args(k))

        first = pl.multiple_of((y % 2) * half + e * quarter, 8)
        mine = pl.ds(first, quarter)

        def times_c(v):
            return jnp.concatenate([mm(v, cmat[0]), mm(v, cmat[1])], axis=1)

        @pl.when(y < 2)
        def _():
            slab_d[:, :big] = inv_a[mine, :]
            slab_d[:, big:] = jnp.zeros((quarter, big), F32)
            inv_t[...] = inv_a[...].T
            u_a = inv_t[mine, :]
            slab_t[:, :big] = u_a
            w = mm(u_a[:, :half], cmat[0], ((1,), (1,))) + mm(u_a[:, half:], cmat[1], ((1,), (1,)))
            slab_t[:, big:] = -mm(w, inv_b[...], ((1,), (1,)))
            q = mm(slab_t[:, big:], inv_b[...])
            slab_g[:, big:] = q
            slab_g[:, :big] = mm(slab_t[:, :big] - times_c(q), inv_a[...])

        @pl.when(y >= 2)
        def _():
            v_b = inv_b[mine, :]
            slab_d[:, big:] = v_b
            slab_d[:, :big] = -mm(times_c(v_b), inv_a[...])
            inv_t[...] = inv_b[...].T
            u_b = inv_t[mine, :]
            slab_t[:, :big] = jnp.zeros((quarter, big), F32)
            slab_t[:, big:] = u_b
            q = mm(u_b, inv_b[...])
            slab_g[:, big:] = q
            slab_g[:, :big] = -mm(times_c(q), inv_a[...])

        def spread(kind, g, j):
            rows, cols = pl.ds(tile * g, tile), pl.ds(half * j, half)
            src = (slab_d, slab_g, slab_t)[kind].at[rows, cols]
            dst = (d_out, g_out)[kind].at[x] if kind < 2 else dt_out.at[0]
            recv = t_recv.at[kind, x] if kind < 2 else t_recv.at[2, 0]
            return src, dst, t_send.at[kind * 16 + g * 4 + j], recv, dest(kind, g, j), me

        for use in (push, sent):
            for kind, g, j in every:
                if kind == 2:
                    @pl.when(x == 1)
                    def _(g=g, j=j, use=use):
                        use(*spread(2, g, j))
                else:
                    use(*spread(kind, g, j))

        for part in range(2):
            @pl.when(source & (y % 2 == part))
            def _(part=part):
                for k in (1, 2, 3):
                    sent(*ab_args(k, part))

        @pl.when(c_source)
        def _():
            for k in (1, 2, 3):
                sent(*c_args(k))

    for k, pair in enumerate(pairs):
        arrived(ct_out.at[k], ct_send.at[0], ct_recv.at[k], ct_source(*pair), me)

    @pl.when(x > z)
    def _():
        for hop in hops:
            sent(*ct_args(*hop))

    for b in range(4):
        arrived(d_out.at[b], t_send.at[0], t_recv.at[0, b], at(b, y), me)
        arrived(g_out.at[b], t_send.at[0], t_recv.at[1, b], at(b, z), me)
    arrived(dt_out.at[0], t_send.at[0], t_recv.at[2, 0], at(1, z), me)


NAMES = ("stage0", "w_half", "y_half", "h_half", "w_full", "y_full", "h_full", "final")


def vmem_call(kernel, outs, scratch, count, flops, name):
    spec = pl.BlockSpec(memory_space=pltpu.VMEM)
    return pl.pallas_call(
        kernel,
        out_shape=[jax.ShapeDtypeStruct(s, F32) for s in outs],
        in_specs=[spec] * count,
        out_specs=[spec] * len(outs),
        scratch_shapes=scratch,
        compiler_params=pltpu.CompilerParams(has_side_effects=True, vmem_limit_bytes=VMEM_LIMIT, collective_id=NAMES.index(name)),
        cost_estimate=pl.CostEstimate(flops=flops, bytes_accessed=8 << 20, transcendentals=0),
        name=name,
    )


def stage0(l_blk, lt_blk, n):
    big, half, quarter, tile = n // 8, n // 16, n // 32, n // 128
    dma = pltpu.SemaphoreType.DMA
    scratch = [
        pltpu.VMEM((big, half), F32), pltpu.VMEM((half, half), F32), pltpu.VMEM((2, big, half), F32),
        pltpu.VMEM((big, big), F32), pltpu.VMEM((big, big), F32), pltpu.VMEM((big, big), F32),
        pltpu.VMEM((quarter, 2 * big), F32), pltpu.VMEM((quarter, 2 * big), F32), pltpu.VMEM((quarter, 2 * big), F32),
        dma((16,)), dma((6,)), dma((3,)), dma((2,)), dma((3,)), dma((2,)), dma((4,)), dma((4,)), dma((48,)), dma((3, 4)),
    ]
    outs = [(6, tile, half), (4, tile, half), (4, tile, half), (1, tile, half)]
    call = vmem_call(functools.partial(stage0_kernel, n), outs, scratch, 2, 10 ** 10, "stage0")
    return call(l_blk, lt_blk)


def along(axis):
    def to(me, k):
        return dict(me, **{axis: jnp.int32(k)})

    return to, to, lambda me: me[axis]


ALONG = {axis: along(axis) for axis in ("x", "y", "z")}


def mapped(to, source, slot):
    return (lambda me, k: dict(to(me, k), e=me["e"]), lambda me, k: dict(source(me, k), e=me["e"]), slot)


W_TURN = mapped(
    lambda m, k: {"x": jnp.int32(k), "y": m["z"], "z": m["x"]},
    lambda m, k: {"x": m["z"], "y": jnp.int32(k), "z": m["y"]}, lambda m: m["y"])
H_TURN = mapped(
    lambda m, k: {"x": jnp.int32(k), "y": m["x"], "z": m["z"]},
    lambda m, k: {"x": m["y"], "y": jnp.int32(k), "z": m["z"]}, lambda m: m["y"])
Y_TURN = mapped(
    lambda m, k: {"x": jnp.int32(k), "y": m["x"], "z": m["y"]},
    lambda m, k: {"x": m["y"], "y": m["z"], "z": jnp.int32(k)}, lambda m: m["z"])
YT_TURN = mapped(
    lambda m, k: {"x": jnp.int32(k), "y": m["y"], "z": m["x"]},
    lambda m, k: {"x": m["z"], "y": m["y"], "z": jnp.int32(k)}, lambda m: m["z"])


def product_kernel(n, spec, *refs):
    pieces, ops, prods, axis, negate = spec
    tile, half = n // 128, n // 16
    count, made = len(pieces), len(prods)
    ins, outs = refs[:count], refs[count:count + made]
    rest = refs[count + made:]
    bufs, rest = rest[:len(ops)], rest[len(ops):]
    parts, rest = rest[:made], rest[made:]
    sibs, rest = rest[:made], rest[made:]
    adds, rest = rest[:made], rest[made:]
    lands, rest = rest[:made], rest[made:]
    g_send, g_recv, s_send, s_recv, r_send, r_recv = rest
    me = coords()
    e = me["e"]
    sib = dict(me, e=1 - e)

    def piece_args(p, k):
        op, (to, _, slot), down, across, wide = pieces[p]
        at = slot(me)
        dst = bufs[op].at[at, down, :, pl.ds(across * half, wide * half)]
        return ins[p].at[0] if len(ins[p].shape) == 3 else ins[p], dst, g_send.at[p, k], g_recv.at[p, at], to(me, k), me

    maps = {id(p[1]): p[1] for p in pieces}
    maps[id(ALONG[axis])] = ALONG[axis]
    meet([(None, m[1](me, k)) for m in maps.values() for k in range(4)] + [(None, sib)],
         [(None, m[0](me, k)) for m in maps.values() for k in range(4)] + [(None, sib)], me)
    for op, (down, across) in enumerate(ops):
        filled = {(d, a + i) for o, _, d, a, w in pieces if o == op for i in range(w)}
        for d in range(down):
            for a in range(across):
                if (d, a) not in filled:
                    bufs[op][:, d, :, a * half:(a + 1) * half] = jnp.zeros((4, tile, half), F32)
    for p in range(count):
        for k in range(4):
            push(*piece_args(p, k))
    for p in range(count):
        op, (_, source, _), down, across, wide = pieces[p]
        for k in range(4):
            dst = bufs[op].at[k, down, :, pl.ds(across * half, wide * half)]
            arrived(dst, g_send.at[p, 0], g_recv.at[p, k], source(me, k), me)

    def sib_args(q, d, core):
        rows = pl.ds(d * half + core * (half // 2), half // 2)
        return parts[q].at[rows, :], sibs[q].at[d], s_send.at[q, d], s_recv.at[q, d], sib, me

    for q, (lo, ro, down) in enumerate(prods):
        lhs = bufs[lo][...].reshape(-1, bufs[lo].shape[-1])
        rhs = bufs[ro][...].reshape(-1, bufs[ro].shape[-1])
        for d in range(down):
            parts[q][d * half:(d + 1) * half, :] = mm(lhs[:, d * half:(d + 1) * half], rhs, ((0,), (0,)))
            push(parts[q].at[pl.ds((1 - e) * (half // 2) + d * half, half // 2), :], sibs[q].at[d],
                 s_send.at[q, d], s_recv.at[q, d], sib, me)

    def red_args(q, k):
        at = me[axis]
        return adds[q].at[k], lands[q].at[at], r_send.at[q, k], r_recv.at[q, at], dict(me, **{axis: jnp.int32(k)}), me

    for q, (_, _, down) in enumerate(prods):
        for d in range(down):
            arrived(sibs[q].at[d], s_send.at[q, d], s_recv.at[q, d], sib, me)
            first = pl.multiple_of(e * (half // 2) + d * half, 8)
            for k in range(4):
                own = parts[q][pl.ds(first + k * tile, tile), :]
                adds[q][k, d] = own + sibs[q][d, k * tile:(k + 1) * tile, :]
        for k in range(4):
            push(*red_args(q, k))
    for q, (_, _, down) in enumerate(prods):
        for k in range(4):
            arrived(lands[q].at[k], r_send.at[q, k], r_recv.at[q, k], dict(me, **{axis: jnp.int32(k)}), me)
        total = lands[q][0] + lands[q][1] + lands[q][2] + lands[q][3]
        outs[q][...] = -total if negate[q] else total

    for p in range(count):
        for k in range(4):
            sent(*piece_args(p, k))
    for q, (_, _, down) in enumerate(prods):
        for d in range(down):
            push_args = (parts[q].at[pl.ds((1 - e) * (half // 2) + d * half, half // 2), :], sibs[q].at[d],
                         s_send.at[q, d], s_recv.at[q, d], sib, me)
            sent(*push_args)
        for k in range(4):
            sent(*red_args(q, k))


def product(n, pieces, ops, prods, axis, negate, name):
    tile, half = n // 128, n // 16
    dma = pltpu.SemaphoreType.DMA
    arrays = [p[0] for p in pieces]
    table = [(p[1], p[2], p[3], p[4], p[0].shape[-1] // half) for p in pieces]
    widths = [ops[ro][1] * half for _, ro, _ in prods]
    downs = [d for _, _, d in prods]
    scratch = [pltpu.VMEM((4, d, tile, a * half), F32) for d, a in ops]
    scratch += [pltpu.VMEM((d * half, w), F32) for d, w in zip(downs, widths)]
    scratch += [pltpu.VMEM((d, half // 2, w), F32) for d, w in zip(downs, widths)]
    scratch += [pltpu.VMEM((4, d, tile, w), F32) for d, w in zip(downs, widths)] * 2
    top = max(downs)
    scratch += [dma((len(pieces), 4)), dma((len(pieces), 4)), dma((len(prods), top)), dma((len(prods), top)),
                dma((len(prods), 4)), dma((len(prods), 4))]
    outs = [(d, tile, w) for d, w in zip(downs, widths)]
    kernel = functools.partial(product_kernel, n, (table, ops, prods, axis, negate))
    return vmem_call(kernel, outs, scratch, len(arrays), 3 * 10 ** 9, name)(*arrays)


def final_kernel(n, plan, *refs):
    tile, half, big = n // 128, n // 16, n // 8
    count = len(plan)
    ins, out = refs[:count], refs[count]
    flat, extra, turned, f_send, f_recv, a_recv, u_recv = refs[count + 1:]
    me = coords()
    x, y, z, e = me["x"], me["y"], me["z"], me["e"]

    def args(p):
        b_row, b_col, kind, rax, cax, gax = plan[p]
        a_r, a_c, g = me[rax], me[cax], me[gax]
        if kind == "turn":
            dst = turned.at[pl.ds(pl.multiple_of(e * (half // 2) + g * tile, 8), tile), pl.ds(pl.multiple_of((a_c % 2) * half, half), half)]
            to = {"x": jnp.int32(b_col), "y": a_r, "z": jnp.int32(b_row), "e": a_c // 2}
            return ins[p], dst, f_send.at[p], u_recv.at[a_c % 2, g, e], to, me
        rows = pl.ds(pl.multiple_of((a_r % 2) * half + e * (half // 2) + g * tile, 8), tile)
        to = {"x": jnp.int32(b_row), "y": a_c, "z": jnp.int32(b_col), "e": a_r // 2}
        if kind == "add":
            return ins[p], extra.at[rows, :], f_send.at[p], a_recv.at[a_r % 2, g, e], to, me
        return ins[p], flat.at[rows, :], f_send.at[p], f_recv.at[a_r % 2, g, e], to, me

    def incoming(p):
        b_row, b_col, kind, rax, cax, gax = plan[p]
        to_x, to_z = (b_col, b_row) if kind == "turn" else (b_row, b_col)
        found = []
        for h in range(2):
            a_r, a_c = (y, 2 * e + h) if kind == "turn" else (2 * e + h, y)
            found += [{rax: a_r, cax: a_c, gax: jnp.int32(g), "e": jnp.int32(ee)} for g in range(4) for ee in range(2)]
        return (x == to_x) & (z == to_z), found

    sources = []
    for p in range(count):
        cond, found = incoming(p)
        sources += [(cond, at) for at in found]
    meet(sources, [(None, args(p)[4]) for p in range(count)], me)
    for p in range(count):
        push(*args(p))
    for p in range(count):
        kind = plan[p][2]
        cond, found = incoming(p)

        @pl.when(cond)
        def _(kind=kind, found=found):
            for h in range(2):
                for g in range(4):
                    for ee in range(2):
                        first = ee * (half // 2) + g * tile
                        if kind == "turn":
                            dst, sem = turned.at[pl.ds(first, tile), pl.ds(h * half, half)], u_recv.at[h, g, ee]
                        else:
                            dst = (extra if kind == "add" else flat).at[pl.ds(h * half + first, tile), :]
                            sem = (a_recv if kind == "add" else f_recv).at[h, g, ee]
                        arrived(dst, f_send.at[0], sem, found[h * 8 + g * 2 + ee], me)

    adds = {(p[0], p[1]) for p in plan if p[2] == "add"}
    turns = {(p[1], p[0]) for p in plan if p[2] == "turn"}
    keeps = {(p[0], p[1]) for p in plan if p[2] == "keep"}
    for b_row in range(4):
        for b_col in range(4):
            @pl.when((x == b_row) & (z == b_col))
            def _(at=(b_row, b_col)):
                total = None
                if at in keeps:
                    total = flat[...]
                if at in adds:
                    total = extra[...] if total is None else total + extra[...]
                if at in turns:
                    moved = turned[...].T
                    total = moved if total is None else total + moved
                out[...] = total
    for p in range(count):
        sent(*args(p))


def final(n, items):
    tile, half, big = n // 128, n // 16, n // 8
    dma = pltpu.SemaphoreType.DMA
    arrays = [i[0] for i in items]
    plan = [i[1:] for i in items]
    scratch = [pltpu.VMEM((big, half), F32), pltpu.VMEM((big, half), F32), pltpu.VMEM((half, big), F32),
               dma((len(items),)), dma((2, 4, 2)), dma((2, 4, 2)), dma((2, 4, 2))]
    call = vmem_call(functools.partial(final_kernel, n, plan), [(big, half)], scratch, len(arrays), 10 ** 7, "final")
    return call(*arrays)[0]


def solution(mesh):
    def local_fn(l_blk):
        n = l_blk.shape[0] * 8
        half = n // 16
        ct, d, g, dt = stage0(l_blk, l_blk.T, n)
        dt = dt[0]
        ct = {(r, c): ct[(r * (r - 1)) // 2 + c] for r in range(4) for c in range(r)}
        ax, ay, az = ALONG["x"], ALONG["y"], ALONG["z"]

        def piece(array, op, how, down=0, across=0):
            return array, op, how, down, across

        def part(array, r, c):
            return array[r][:, c * half:(c + 1) * half]

        one, two, minus = (1, 1), (2, 2), (True,) * 3
        (w0,), (w1,) = product(
            n, [piece(ct[1, 0], 0, ax), piece(d[0], 1, az), piece(ct[3, 2], 2, ax), piece(d[2], 3, az)],
            [one] * 4, [(0, 1, 1), (2, 3, 1)], "y", (False,) * 2, "w_half")
        (y0, x21), (y1,), (yt1,) = product(
            n, [piece(g[1], 0, ax), piece(dt, 0, ax, 0, 1), piece(w0, 1, ay), piece(g[3], 2, ax), piece(w1, 3, ay)],
            [(1, 2), one, one, one], [(0, 1, 2), (2, 3, 1), (3, 2, 1)], "z", minus, "y_half")
        (h0,), (h1,) = product(
            n, [piece(w0, 0, W_TURN), piece(y0, 1, az), piece(w1, 2, W_TURN), piece(y1, 3, az)],
            [one] * 4, [(0, 1, 1), (2, 3, 1)], "y", minus, "h_half")
        g0, g2 = g[0] + h0, g[2] + h1
        whole = [(0, 1, 2)]
        (w,) = product(
            n, [piece(ct[2 + r, c], 0, ax, c, r) for r in range(2) for c in range(2)]
            + [piece(d[0], 1, az), piece(jnp.concatenate([x21, d[1]], axis=1), 1, az, 1)],
            [two] * 2, whole, "y", (False,), "w_full")
        (yy,) = product(
            n, [piece(g2, 0, H_TURN), piece(yt1, 0, YT_TURN, 0, 1), piece(y1, 0, Y_TURN, 1), piece(g[3], 0, ax, 1, 1)]
            + [piece(w[r], 1, ay, r) for r in range(2)],
            [two] * 2, whole, "z", minus, "y_full")
        (h,) = product(
            n, [piece(w[r], 0, W_TURN, r) for r in range(2)] + [piece(yy[r], 1, az, r) for r in range(2)],
            [two] * 2, whole, "y", minus, "h_full")
        items = []
        for r in range(2):
            for c in range(2):
                items.append((part(h, r, c), r, c, "keep", *"zxy"))
                items += [(part(yy, r, c), 2 + r, c, kind, *"yxz") for kind in ("keep", "turn")]
        items += [(g0, 0, 0, "add", *"zxy"), (g[1], 1, 1, "add", *"zyx"), (g2, 2, 2, "keep", *"zxy"),
                  (g[3], 3, 3, "keep", *"zyx")]
        for array, r, keep in ((y0, 1, "add"), (y1, 3, "keep")):
            items += [(array, r, r - 1, kind, *"yxz") for kind in (keep, "turn")]
        return final(n, items)

    spec = P(("batch", "row"), "col")
    return jax.shard_map(local_fn, mesh=mesh, in_specs=(spec,), out_specs=spec, check_vma=False)
```

```python
import functools

import jax
import jax.numpy as jnp
from jax import lax
from jax.experimental import pallas as pl
from jax.experimental.pallas import tpu as pltpu
from jax.sharding import PartitionSpec as P

MESH = pl.DeviceIdType.MESH
HIGHEST = lax.Precision.HIGHEST
F32 = jnp.float32
VMEM_LIMIT = 67043328


def coords():
    col = lax.axis_index("col")
    row = lax.axis_index("row")
    return {"x": row // 2, "y": col % 4, "z": col // 4, "e": row % 2}


def device(at):
    return (0, 4 * at["z"] + at["y"], 2 * at["x"] + at["e"])


def same(p, q):
    return (p["x"] == q["x"]) & (p["y"] == q["y"]) & (p["z"] == q["z"]) & (p["e"] == q["e"])


def mm(a, b, dims=((1,), (0,))):
    return lax.dot_general(a, b, (dims, ((), ())), precision=HIGHEST, preferred_element_type=F32)


def loop(count, body):
    def step(k, carry):
        body(k)
        return carry

    lax.fori_loop(0, count, step, jnp.int32(0))


def push(src, dst, send_sem, recv_sem, to, me):
    here = same(to, me)

    @pl.when(here)
    def _():
        dst[...] = src[...]

    @pl.when(jnp.logical_not(here))
    def _():
        pltpu.make_async_remote_copy(
            src_ref=src, dst_ref=dst, send_sem=send_sem, recv_sem=recv_sem, device_id=device(to), device_id_type=MESH
        ).start()


def sent(src, dst, send_sem, recv_sem, to, me):
    @pl.when(jnp.logical_not(same(to, me)))
    def _():
        pltpu.make_async_remote_copy(
            src_ref=src, dst_ref=dst, send_sem=send_sem, recv_sem=recv_sem, device_id=device(to), device_id_type=MESH
        ).wait_send()


def arrived(dst, send_sem, recv_sem, source, me):
    @pl.when(jnp.logical_not(same(source, me)))
    def _():
        pltpu.make_async_remote_copy(
            src_ref=dst, dst_ref=dst, send_sem=send_sem, recv_sem=recv_sem, device_id=device(source), device_id_type=MESH
        ).wait_recv()


def meet(sources, dests, me):
    barrier = pltpu.get_barrier_semaphore()

    def other(cond, at):
        apart = jnp.logical_not(same(at, me))
        return apart if cond is None else apart & cond

    total = jnp.int32(0)
    for cond, count, which in sources:
        def tell(k, cond=cond, which=which):
            @pl.when(other(cond, which(k)))
            def _():
                pl.semaphore_signal(barrier, inc=1, device_id=device(which(k)), device_id_type=MESH)

        loop(count, tell)
    for cond, count, which in dests:
        def add(k, carry, cond=cond, which=which):
            return carry + other(cond, which(k)).astype(jnp.int32)

        total = lax.fori_loop(0, count, add, total)

    @pl.when(total > 0)
    def _():
        pl.semaphore_wait(barrier, total)


def invert_block(left, corner, inv, base):
    half = 3 * base
    rows = lax.broadcasted_iota(jnp.int32, (base, base), 0)
    cols = lax.broadcasted_iota(jnp.int32, (base, base), 1)
    eye = rows == cols

    def block(i, j):
        if j < 3:
            return left[i * base:(i + 1) * base, j * base:(j + 1) * base]
        return corner[(i - 3) * base:(i - 2) * base, (j - 3) * base:(j - 2) * base]

    tri = [block(i, i) for i in range(6)]
    found = []
    for i in range(6):
        diag = jnp.sum(jnp.where(eye, tri[i], 0.0), axis=1, keepdims=True)
        found.append(jnp.where(eye, 1.0 / diag, 0.0))
    size = 1
    while size < base:
        below = ((rows // size) % 2 == 1) & (cols // size == rows // size - 1)
        half_way = [mm(jnp.where(below, tri[i], 0.0), found[i]) for i in range(6)]
        found = [found[i] - mm(found[i], half_way[i]) for i in range(6)]
        size = size * 2
    inv[...] = jnp.zeros(inv.shape, F32)
    for k in (0, 3):
        x0, x1, x2 = found[k:k + 3]
        x10 = -mm(x1, mm(block(k + 1, k), x0))
        x21 = -mm(x2, mm(block(k + 2, k + 1), x1))
        x20 = -mm(x2, mm(block(k + 2, k), x0) + mm(block(k + 2, k + 1), x10))
        for i, j, val in ((0, 0, x0), (1, 1, x1), (2, 2, x2), (1, 0, x10), (2, 1, x21), (2, 0, x20)):
            inv[(k + i) * base:(k + i + 1) * base, (k + j) * base:(k + j + 1) * base] = val
    low = mm(left[half:, :], inv[:half, :half])
    inv[half:, :half] = -mm(inv[half:, half:], low)


def stage0(n, me, sources, dests, l_ref, lt_ref, ct_out, d_out, g_out, dt_out,
           left, corner, cmat, inv_a, inv_b, inv_t, slab_d, slab_t, slab_g,
           ct_send, ct_recv, ab_send, ab_recv, c_send, c_recv, x_send, x_recv, t_send, t_recv):
    x, y, z, e = me["x"], me["y"], me["z"], me["e"]
    big = n // 8
    half = n // 16
    quarter = n // 32
    tile = n // 128
    sib = dict(me, e=1 - e)
    diag = x == z

    slot = (x * (x - 1)) // 2 + z
    def ct_args(i):
        g, k, h, ee = i // 16, i // 4 % 4, i // 2 % 2, i % 2
        rows = pl.ds(pl.multiple_of(quarter * ee + tile * g, 8), tile)
        src = lt_ref.at[rows, pl.ds(pl.multiple_of(half * h, half), half)]
        to = {"x": k, "y": y, "z": 2 * e + h, "e": ee}
        return src, ct_out.at[slot, g], ct_send.at[i], ct_recv.at[slot, g], to, me

    source = diag & (y // 2 == e)
    c_source = diag & (e == 1) & (y < 2)

    def at(b, along_y):
        b = jnp.int32(b)
        return {"x": b, "y": along_y, "z": b, "e": e}

    odd = x % 2

    def dest(kind, i):
        g, j = i // 4, i % 4
        if kind == 0:
            return {"x": j, "y": y, "z": g, "e": e}
        if kind == 1:
            return {"x": odd * g + (1 - odd) * j, "y": odd * j + (1 - odd) * g, "z": y, "e": e}
        return {"x": g, "y": j, "z": y, "e": e}

    pairs = [(b_row, b_col) for b_row in range(4) for b_col in range(b_row)]

    def ct_source(b_row, b_col):
        return {"x": jnp.int32(b_row), "y": y, "z": jnp.int32(b_col), "e": z // 2}

    def one(cond, where):
        return cond, 1, lambda k: where

    sources = sources + [one(None, ct_source(*pair)) for pair in pairs] + [one(diag, sib)]
    sources += [(diag, 2, lambda k: dict(me, y=2 * e + k)), (diag & (e == 1), 2, lambda k: dict(me, y=k))]
    sources += [(None, 4, lambda b: at(b, y)), (None, 4, lambda b: at(b, z)), one(None, at(1, z))]
    dests = dests + [(x > z, 16, lambda i: ct_args(i)[4]), one(diag, sib)]
    dests += [(cond, 3, lambda k: dict(me, y=(y + k + 1) % 4)) for cond in (source, c_source)]
    dests += [(diag, 16, lambda i: dest(0, i)), (diag, 16, lambda i: dest(1, i)), (diag & (x == 1), 16, lambda i: dest(2, i))]
    meet(sources, dests, me)

    def ab_args(k, part):
        to = dict(me, y=(y + k) % 4)
        if part == 0:
            return l_ref, left, ab_send.at[k - 1], ab_recv.at[0], to, me
        return l_ref.at[pl.ds(half, half), :], corner, ab_send.at[k - 1], ab_recv.at[1], to, me

    for part in range(2):
        @pl.when(source & (y % 2 == part))
        def _(part=part):
            for k in (1, 3, 2):
                push(*ab_args(k, part))

    def c_args(k):
        to = dict(me, y=(y + k) % 4)
        return l_ref, cmat.at[y % 2], c_send.at[k - 1], c_recv.at[y % 2], to, me

    @pl.when(c_source)
    def _():
        for k in (1, 3, 2):
            push(*c_args(k))

    @pl.when(x > z)
    def _():
        loop(64, lambda i: push(*ct_args(i)))

    def swap_args(k):
        mine = [inv_a, inv_b, cmat.at[0], cmat.at[1]][k]
        return mine, mine, x_send.at[k], x_recv.at[k], sib, me

    @pl.when(diag)
    def _():
        for part, (dst, src_rows) in enumerate(((left, 0), (corner, half))):
            @pl.when(source & (y % 2 == part))
            def _(dst=dst, src_rows=src_rows):
                dst[...] = l_ref[src_rows:, :]

            arrived(dst, ab_send.at[0], ab_recv.at[part], dict(me, y=2 * e + part), me)

        invert_block(left, corner, inv_t, n // 48)
        for core, inv in ((0, inv_a), (1, inv_b)):
            @pl.when(e == core)
            def _(inv=inv):
                inv[...] = inv_t[...]

        @pl.when(e == 0)
        def _():
            push(*swap_args(0))
            for k in (1, 2, 3):
                arrived(swap_args(k)[1], x_send.at[k], x_recv.at[k], sib, me)
            sent(*swap_args(0))

        @pl.when(e == 1)
        def _():
            push(*swap_args(1))
            for part in range(2):
                @pl.when(y == part)
                def _(part=part):
                    cmat[part] = l_ref[...]

                arrived(cmat.at[part], c_send.at[0], c_recv.at[part], dict(me, y=jnp.int32(part)), me)
                push(*swap_args(2 + part))
            arrived(inv_a, x_send.at[0], x_recv.at[0], sib, me)
            for k in (1, 2, 3):
                sent(*swap_args(k))

        first = pl.multiple_of((y % 2) * half + e * quarter, 8)
        mine = pl.ds(first, quarter)

        def times_c(v):
            return jnp.concatenate([mm(v, cmat[0]), mm(v, cmat[1])], axis=1)

        @pl.when(y < 2)
        def _():
            slab_d[:, :big] = inv_a[mine, :]
            slab_d[:, big:] = jnp.zeros((quarter, big), F32)
            inv_t[...] = inv_a[...].T
            u_a = inv_t[mine, :]
            slab_t[:, :big] = u_a
            w = mm(u_a[:, :half], cmat[0], ((1,), (1,))) + mm(u_a[:, half:], cmat[1], ((1,), (1,)))
            slab_t[:, big:] = -mm(w, inv_b[...], ((1,), (1,)))
            q = mm(slab_t[:, big:], inv_b[...])
            slab_g[:, big:] = q
            slab_g[:, :big] = mm(slab_t[:, :big] - times_c(q), inv_a[...])

        @pl.when(y >= 2)
        def _():
            v_b = inv_b[mine, :]
            slab_d[:, big:] = v_b
            slab_d[:, :big] = -mm(times_c(v_b), inv_a[...])
            inv_t[...] = inv_b[...].T
            u_b = inv_t[mine, :]
            slab_t[:, :big] = jnp.zeros((quarter, big), F32)
            slab_t[:, big:] = u_b
            q = mm(u_b, inv_b[...])
            slab_g[:, big:] = q
            slab_g[:, :big] = -mm(times_c(q), inv_a[...])

        def spread(kind, i):
            rows = pl.ds(pl.multiple_of(tile * (i // 4), 8), tile)
            src = (slab_d, slab_g, slab_t)[kind].at[rows, pl.ds(pl.multiple_of(half * (i % 4), half), half)]
            dst = (d_out, g_out)[kind].at[x] if kind < 2 else dt_out.at[0]
            recv = t_recv.at[kind, x] if kind < 2 else t_recv.at[2, 0]
            return src, dst, t_send.at[kind * 16 + i], recv, dest(kind, i), me

        for use in (push, sent):
            for kind in range(2):
                loop(16, lambda i, kind=kind, use=use: use(*spread(kind, i)))

            @pl.when(x == 1)
            def _(use=use):
                loop(16, lambda i: use(*spread(2, i)))

        for part in range(2):
            @pl.when(source & (y % 2 == part))
            def _(part=part):
                for k in (1, 2, 3):
                    sent(*ab_args(k, part))

        @pl.when(c_source)
        def _():
            for k in (1, 2, 3):
                sent(*c_args(k))

    loop(4, lambda b: arrived(d_out.at[b], t_send.at[0], t_recv.at[0, b], at(b, y), me))
    loop(4, lambda b: arrived(g_out.at[b], t_send.at[0], t_recv.at[1, b], at(b, z), me))
    arrived(dt_out.at[0], t_send.at[0], t_recv.at[2, 0], at(1, z), me)
    for k, pair in enumerate(pairs):
        loop(4, lambda g, k=k, pair=pair: arrived(ct_out.at[k, g], ct_send.at[0], ct_recv.at[k, g], ct_source(*pair), me))

    def finish():
        @pl.when(x > z)
        def _():
            loop(64, lambda i: sent(*ct_args(i)))

    return finish


def along(axis):
    def to(me, k):
        return dict(me, **{axis: jnp.int32(k)})

    return to, to, lambda me: me[axis]


ALONG = {axis: along(axis) for axis in ("x", "y", "z")}


def mapped(to, source, slot):
    return (lambda me, k: dict(to(me, k), e=me["e"]), lambda me, k: dict(source(me, k), e=me["e"]), slot)


W_TURN = mapped(
    lambda m, k: {"x": jnp.int32(k), "y": m["z"], "z": m["x"]},
    lambda m, k: {"x": m["z"], "y": jnp.int32(k), "z": m["y"]}, lambda m: m["y"])
H_TURN = mapped(
    lambda m, k: {"x": jnp.int32(k), "y": m["x"], "z": m["z"]},
    lambda m, k: {"x": m["y"], "y": jnp.int32(k), "z": m["z"]}, lambda m: m["y"])
Y_TURN = mapped(
    lambda m, k: {"x": jnp.int32(k), "y": m["x"], "z": m["y"]},
    lambda m, k: {"x": m["y"], "y": m["z"], "z": jnp.int32(k)}, lambda m: m["z"])
YT_TURN = mapped(
    lambda m, k: {"x": jnp.int32(k), "y": m["y"], "z": m["x"]},
    lambda m, k: {"x": m["z"], "y": m["y"], "z": jnp.int32(k)}, lambda m: m["z"])


class Gather:
    def __init__(self, how, me, buf, send, recv):
        self.to, self.source, self.slot = how
        self.me, self.buf, self.send, self.recv = me, buf, send, recv

    def args(self, k):
        at = self.slot(self.me)
        return self.src, self.buf.at[at], self.send.at[k], self.recv.at[at], self.to(self.me, k), self.me

    def start(self, src):
        self.src = src
        loop(4, lambda k: push(*self.args(k)))

    def wait(self):
        loop(4, lambda k: arrived(
            self.buf.at[k], self.send.at[0], self.recv.at[k], self.source(self.me, k), self.me))

    def finish(self):
        loop(4, lambda k: sent(*self.args(k)))

    def rows(self, block=None):
        tiles = [self.buf[k] if block is None else self.buf[k, block] for k in range(4)]
        return jnp.concatenate(tiles, axis=0)


class Reduce:
    def __init__(self, axis, me, part, sib, land, out, s_send, s_recv, r_send, r_recv):
        self.axis, self.me, self.part, self.sib, self.land, self.out = axis, me, part, sib, land, out
        self.sems = s_send, s_recv, r_send, r_recv
        self.other = dict(me, e=1 - me["e"])
        self.down = out.shape[0]
        self.tile = out.shape[1]

    def swap_args(self, d):
        rows = pl.ds(((1 - self.me["e"]) + 2 * d) * (4 * self.tile), 4 * self.tile)
        return self.part.at[rows, :], self.sib.at[d], self.sems[0].at[d], self.sems[1].at[d], self.other, self.me

    def args(self, k):
        at = self.me[self.axis]
        to = dict(self.me, **{self.axis: jnp.int32(k)})
        src = self.sib.at[:, pl.ds(pl.multiple_of(k * self.tile, 8), self.tile), :]
        return src, self.land.at[at], self.sems[2].at[k], self.sems[3].at[at], to, self.me

    def put(self, d, value):
        self.part[d * 8 * self.tile:(d + 1) * 8 * self.tile, :] = value
        push(*self.swap_args(d))

    def start(self):
        tile = self.tile
        for d in range(self.down):
            arrived(self.sib.at[d], self.sems[0].at[d], self.sems[1].at[d], self.other, self.me)
            first = pl.multiple_of((self.me["e"] + 2 * d) * (4 * tile), 8)
            self.sib[d] = self.part[pl.ds(first, 4 * tile), :] + self.sib[d]
        loop(4, lambda k: push(*self.args(k)))

    def wait(self, sign=1, more=None):
        loop(4, lambda k: arrived(
            self.land.at[k], self.sems[2].at[k], self.sems[3].at[k], dict(self.me, **{self.axis: k}), self.me))
        total = (self.land[0] + self.land[1]) + (self.land[2] + self.land[3])
        total = total if sign > 0 else -total
        self.out[...] = total if more is None else total + more

    def swapped(self):
        for d in range(self.down):
            sent(*self.swap_args(d))

    def finish(self):
        loop(4, lambda k: sent(*self.args(k)))


def turn(a, b):
    return mm(a, b, ((0,), (0,)))


class Output:
    def __init__(self, n, me, flat, extra, turned, send, f_recv, a_recv, u_recv):
        self.half, self.tile, self.me, self.send = n // 16, n // 128, me, send
        self.into = {"keep": (flat, f_recv), "add": (extra, a_recv), "turn": (turned, u_recv)}
        self.started = []

    def place(self, kind, h, g, ee):
        buf, recv = self.into[kind]
        first = ee * (4 * self.tile) + g * self.tile
        if kind == "turn":
            cols = pl.ds(pl.multiple_of(h * self.half, self.half), self.half)
            return buf.at[pl.ds(pl.multiple_of(first, 8), self.tile), cols], recv.at[h, g, ee]
        return buf.at[pl.ds(pl.multiple_of(first + h * self.half, 8), self.tile), :], recv.at[h, g, ee]

    def to(self, plan):
        b_row, b_col, kind, rax, cax, gax = plan
        a_r, a_c = self.me[rax], self.me[cax]
        if kind == "turn":
            return {"x": jnp.int32(b_col), "y": a_r, "z": jnp.int32(b_row), "e": a_c // 2}, a_c % 2
        return {"x": jnp.int32(b_row), "y": a_c, "z": jnp.int32(b_col), "e": a_r // 2}, a_r % 2

    def args(self, index):
        plan, src = self.started[index]
        to, h = self.to(plan)
        dst, recv = self.place(plan[2], h, self.me[plan[5]], self.me["e"])
        return src, dst, self.send.at[index], recv, to, self.me

    def start(self, src, *plan):
        self.started.append((plan, src))
        push(*self.args(len(self.started) - 1))

    def incoming(self, plan):
        b_row, b_col, kind, rax, cax, gax = plan
        to_x, to_z = (b_col, b_row) if kind == "turn" else (b_row, b_col)
        y, e = self.me["y"], self.me["e"]

        def find(i):
            h, g, ee = i // 8, i // 2 % 4, i % 2
            a_r, a_c = (y, 2 * e + h) if kind == "turn" else (2 * e + h, y)
            return h, g, ee, {rax: a_r, cax: a_c, gax: g, "e": ee}

        return (self.me["x"] == to_x) & (self.me["z"] == to_z), find

    def finish(self, out):
        for plan, _ in self.started:
            cond, find = self.incoming(plan)

            @pl.when(cond)
            def _(plan=plan, find=find):
                def take(i):
                    h, g, ee, at = find(i)
                    dst, recv = self.place(plan[2], h, g, ee)
                    arrived(dst, self.send.at[0], recv, at, self.me)

                loop(16, take)

        kinds = {}
        for plan, _ in self.started:
            where = (plan[1], plan[0]) if plan[2] == "turn" else plan[:2]
            kinds.setdefault(where, set()).add(plan[2])
        for (b_row, b_col), has in kinds.items():
            @pl.when((self.me["x"] == b_row) & (self.me["z"] == b_col))
            def _(has=has):
                terms = [self.into[kind][0][...] for kind in ("keep", "add") if kind in has]
                if "turn" in has:
                    terms.append(self.into["turn"][0][...].T)
                out[...] = sum(terms[1:], terms[0])
        for index in range(len(self.started)):
            sent(*self.args(index))


ZXY, YXZ, ZYX = tuple("zxy"), tuple("yxz"), tuple("zyx")
PLANS = [(r, c, "keep", *ZXY) for r in range(2) for c in range(2)]
PLANS += [(2 + r, c, kind, *YXZ) for r in range(2) for c in range(2) for kind in ("keep", "turn")]
PLANS += [(0, 0, "add", *ZXY), (1, 1, "add", *ZYX), (2, 2, "keep", *ZXY), (3, 3, "keep", *ZYX)]
PLANS += [(r, r - 1, kind, *YXZ) for r, keep in ((1, "add"), (3, "keep")) for kind in (keep, "turn")]
X, Y, Z = ALONG["x"], ALONG["y"], ALONG["z"]
GATHERS = [("d0", Z, 0), ("d1", Z, 0), ("d2", Z, 0), ("g1", X, 0), ("dt", X, 0), ("g3", X, 0), ("w0", Y, 0), ("w1", Y, 0),
           ("y0", Z, 0), ("y1", Z, 0), ("x21", Z, 0), ("w0t", W_TURN, 0), ("w1t", W_TURN, 0), ("g2t", H_TURN, 0),
           ("yt1t", YT_TURN, 0), ("y1t", Y_TURN, 0), ("w", Y, 1), ("wt", W_TURN, 1), ("y", Z, 1)]
REDUCES = [("w0", "y", 0), ("w1", "y", 0), ("x21", "z", 0), ("y0", "z", 0), ("y1", "z", 0), ("yt1", "z", 0), ("h0", "y", 0),
           ("h1", "y", 0), ("w", "y", 1), ("y", "z", 1), ("h", "y", 1)]


def scratch_plan(n):
    big, half, quarter, tile = n // 8, n // 16, n // 32, n // 128
    dma, vmem = pltpu.SemaphoreType.DMA, lambda *shape: pltpu.VMEM(shape, F32)
    pairs, four = 6, 4
    groups = [[vmem(pairs, four, tile, half), vmem(four, tile, half), vmem(four, tile, half), vmem(1, tile, half),
               vmem(big, half), vmem(half, half), vmem(2, big, half)]
              + [vmem(big, big)] * 3 + [vmem(quarter, 2 * big)] * 3
              + [dma((64,)), dma((pairs, four)), dma((3,)), dma((2,)), dma((3,)), dma((2,)), dma((four,)), dma((four,)),
                 dma((48,)), dma((3, four))]]
    for _, _, wide in GATHERS:
        shape = (2, tile, 2 * half) if wide else (tile, half)
        groups.append([vmem(four, *shape), dma((four,)), dma((four,))])
    for _, _, wide in REDUCES:
        down, width = (2, 2 * half) if wide else (1, half)
        part = [] if wide else [vmem(half, width)]
        groups.append(part + [vmem(down, quarter, width), vmem(four, down, tile, width), vmem(down, tile, width),
                       dma((down,)), dma((down,)), dma((four,)), dma((four,))])
    hubs = dma((2, four, 2))
    groups.append([vmem(big, half), vmem(big, half), vmem(half, big), dma((len(PLANS),)), hubs, hubs, hubs])
    return groups


def whole_kernel(n, sizes, l_ref, lt_ref, out, *refs):
    half = n // 16
    me = coords()
    groups = []
    for size in sizes:
        groups.append(refs[:size])
        refs = refs[size:]
    first, groups = groups[0], groups[1:]
    ga = {name: Gather(how, me, *group) for (name, how, _), group in zip(GATHERS, groups)}
    groups = groups[len(GATHERS):]
    re = {name: Reduce(axis, me, *((first[9],) if wide else ()), *group)
          for (name, axis, wide), group in zip(REDUCES, groups)}
    res = Output(n, me, *groups[-1])

    maps = [X, Y, Z, W_TURN, H_TURN, Y_TURN, YT_TURN]
    sources = [(None, 4, lambda k, how=how: how[1](me, k)) for how in maps]
    dests = [(None, 4, lambda k, how=how: how[0](me, k)) for how in maps]
    for plan in PLANS:
        cond, find = res.incoming(plan)
        sources.append((cond, 16, lambda i, find=find: find(i)[-1]))
        dests.append((None, 1, lambda k, plan=plan: res.to(plan)[0]))
    ct, d, g, dt = first[:4]
    ending = stage0(n, me, sources, dests, l_ref, lt_ref, *first)

    def ctr(r, c):
        slot = (r * (r - 1)) // 2 + c
        return jnp.concatenate([ct[slot, k] for k in range(4)], axis=0)

    def cols(array, r, c):
        return array.at[r, :, pl.ds(c * half, half)]

    for name, src in (("d0", d.at[0]), ("d2", d.at[2]), ("g1", g.at[1]), ("dt", dt.at[0]), ("g3", g.at[3]), ("d1", d.at[1])):
        ga[name].start(src)
    for name, pair, right in (("w0", (1, 0), "d0"), ("w1", (3, 2), "d2")):
        ga[right].wait()
        re[name].put(0, turn(ctr(*pair), ga[right].rows()))
    for name in ("w0", "w1"):
        re[name].start()
    for name in ("w0", "w1"):
        re[name].wait()
        ga[name].start(re[name].out.at[0])
    for name in ("w0", "w1"):
        ga[name + "t"].start(re[name].out.at[0])
    res.start(g.at[1], 1, 1, "add", *ZYX)
    res.start(g.at[3], 3, 3, "keep", *ZYX)
    for name in ("dt", "g1", "g3", "w0", "w1"):
        ga[name].wait()
    made = ("x21", "y0", "y1", "yt1")
    for name, left, right in zip(made, ("dt", "g1", "g3", "w1"), ("w0", "w0", "w1", "g3")):
        re[name].put(0, turn(ga[left].rows(), ga[right].rows()))
    for name in made:
        re[name].start()
    re["x21"].wait(-1)
    ga["x21"].start(re["x21"].out.at[0])
    for name in made[1:]:
        re[name].wait(-1)
    for name in ("y0", "y1"):
        ga[name].start(re[name].out.at[0])
    ga["d1"].wait()
    ga["x21"].wait()
    zero, one = ga["d0"].rows(), jnp.concatenate([ga["x21"].rows(), ga["d1"].rows()], axis=1)
    for r in range(2):
        top = turn(ctr(2 + r, 1), one)
        re["w"].put(r, jnp.concatenate([top[:, :half] + turn(ctr(2 + r, 0), zero), top[:, half:]], axis=1))
    re["w"].start()
    for name in ("yt1", "y1"):
        ga[name + "t"].start(re[name].out.at[0])
    for name, left, right in (("h0", "w0t", "y0"), ("h1", "w1t", "y1")):
        ga[left].wait()
        ga[right].wait()
        re[name].put(0, turn(ga[left].rows(), ga[right].rows()))
    for name in ("h1", "h0"):
        re[name].start()
    re["w"].wait()
    re["w"].swapped()
    ga["w"].start(re["w"].out)
    re["h1"].wait(-1, g[2:3])
    ga["g2t"].start(re["h1"].out.at[0])
    re["h0"].wait(-1, g[0:1])
    ga["wt"].start(re["w"].out)
    for name in ("yt1t", "y1t", "g2t", "w"):
        ga[name].wait()
    for r, names in enumerate((("g2t", "y1t"), ("yt1t", "g3"))):
        re["y"].put(r, sum(turn(ga[name].rows(), ga["w"].rows(c)) for c, name in enumerate(names)))
    re["y"].start()
    for name, r, keep in (("y0", 1, "add"), ("y1", 3, "keep")):
        for kind in (keep, "turn"):
            res.start(re[name].out.at[0], r, r - 1, kind, *YXZ)
    res.start(re["h0"].out.at[0], 0, 0, "add", *ZXY)
    res.start(re["h1"].out.at[0], 2, 2, "keep", *ZXY)
    re["y"].wait(-1)
    re["y"].swapped()
    ga["y"].start(re["y"].out)
    for r in range(2):
        for c in range(2):
            for kind in ("keep", "turn"):
                res.start(cols(re["y"].out, r, c), 2 + r, c, kind, *YXZ)
    ga["wt"].wait()
    ga["y"].wait()
    for r in range(2):
        left = [ga["wt"].rows(c)[:, r * half:(r + 1) * half] for c in range(2)]
        re["h"].put(r, sum(turn(left[c], ga["y"].rows(c)) for c in range(2)))
    re["h"].start()
    re["h"].wait(-1)
    for r in range(2):
        for c in range(2):
            res.start(cols(re["h"].out, r, c), r, c, "keep", *ZXY)
    res.finish(out)
    ending()
    for part in [*ga.values(), *re.values()]:
        part.finish()
    for name in ("w0", "w1", *made, "h0", "h1", "h"):
        re[name].swapped()


def solution(mesh):
    def local_fn(l_blk):
        n = l_blk.shape[0] * 8
        groups = scratch_plan(n)
        spec = pl.BlockSpec(memory_space=pltpu.VMEM)
        call = pl.pallas_call(
            functools.partial(whole_kernel, n, [len(group) for group in groups]),
            out_shape=jax.ShapeDtypeStruct(l_blk.shape, F32),
            in_specs=[spec, spec],
            out_specs=spec,
            scratch_shapes=sum(groups, []),
            compiler_params=pltpu.CompilerParams(
                has_side_effects=True, vmem_limit_bytes=VMEM_LIMIT, collective_id=0),
            name="whole",
        )
        return call(l_blk, l_blk.T)

    spec = P(("batch", "row"), "col")
    return jax.shard_map(local_fn, mesh=mesh, in_specs=(spec,), out_specs=spec, check_vma=False)
```

```python
import functools

import jax
import jax.numpy as jnp
from jax import lax
from jax.experimental import pallas as pl
from jax.experimental.pallas import tpu as pltpu
from jax.sharding import PartitionSpec as P

MESH = pl.DeviceIdType.MESH
HIGHEST = lax.Precision.HIGHEST
F32 = jnp.float32
VMEM_LIMIT = 67043328


def coords():
    col = lax.axis_index("col")
    row = lax.axis_index("row")
    return {"x": row // 2, "y": col % 4, "z": col // 4, "e": row % 2}


def device(at):
    return (0, 4 * at["z"] + at["y"], 2 * at["x"] + at["e"])


def same(p, q):
    return (p["x"] == q["x"]) & (p["y"] == q["y"]) & (p["z"] == q["z"]) & (p["e"] == q["e"])


def mm(a, b, dims=((1,), (0,))):
    return lax.dot_general(a, b, (dims, ((), ())), precision=HIGHEST, preferred_element_type=F32)


def loop(count, body):
    def step(k, carry):
        body(k)
        return carry

    lax.fori_loop(0, count, step, jnp.int32(0))


def push(src, dst, send_sem, recv_sem, to, me):
    here = same(to, me)

    @pl.when(here)
    def _():
        dst[...] = src[...]

    @pl.when(jnp.logical_not(here))
    def _():
        pltpu.make_async_remote_copy(
            src_ref=src, dst_ref=dst, send_sem=send_sem, recv_sem=recv_sem, device_id=device(to), device_id_type=MESH
        ).start()


def sent(src, dst, send_sem, recv_sem, to, me):
    @pl.when(jnp.logical_not(same(to, me)))
    def _():
        pltpu.make_async_remote_copy(
            src_ref=src, dst_ref=dst, send_sem=send_sem, recv_sem=recv_sem, device_id=device(to), device_id_type=MESH
        ).wait_send()


def arrived(dst, send_sem, recv_sem, source, me):
    @pl.when(jnp.logical_not(same(source, me)))
    def _():
        pltpu.make_async_remote_copy(
            src_ref=dst, dst_ref=dst, send_sem=send_sem, recv_sem=recv_sem, device_id=device(source), device_id_type=MESH
        ).wait_recv()


def meet(sources, dests, me):
    barrier = pltpu.get_barrier_semaphore()

    def other(cond, at):
        apart = jnp.logical_not(same(at, me))
        return apart if cond is None else apart & cond

    total = jnp.int32(0)
    for cond, count, which in sources:
        def tell(k, which=which):
            @pl.when(other(None, which(k)))
            def _():
                pl.semaphore_signal(barrier, inc=1, device_id=device(which(k)), device_id_type=MESH)

        if cond is None:
            loop(count, tell)
        else:
            @pl.when(cond)
            def _(count=count, tell=tell):
                loop(count, tell)

    for cond, count, which in dests:
        def add(k, carry, cond=cond, which=which):
            return carry + other(cond, which(k)).astype(jnp.int32)

        total = lax.fori_loop(0, count, add, total)

    @pl.when(total > 0)
    def _():
        pl.semaphore_wait(barrier, total)


def remote(src, dst, send_sem, recv_sem, to):
    return pltpu.make_async_remote_copy(
        src_ref=src, dst_ref=dst, send_sem=send_sem, recv_sem=recv_sem, device_id=device(to), device_id_type=MESH)


def invert_block(left, corner, inv, base):
    half = 3 * base
    rows = lax.broadcasted_iota(jnp.int32, (base, base), 0)
    cols = lax.broadcasted_iota(jnp.int32, (base, base), 1)
    eye = rows == cols

    def block(i, j):
        if j < 3:
            return left[i * base:(i + 1) * base, j * base:(j + 1) * base]
        return corner[(i - 3) * base:(i - 2) * base, (j - 3) * base:(j - 2) * base]

    tri = [block(i, i) for i in range(6)]
    found = []
    for i in range(6):
        diag = jnp.sum(jnp.where(eye, tri[i], 0.0), axis=1, keepdims=True)
        found.append(jnp.where(eye, 1.0 / diag, 0.0))
    size = 1
    while size < base:
        below = ((rows // size) % 2 == 1) & (cols // size == rows // size - 1)
        half_way = [mm(jnp.where(below, tri[i], 0.0), found[i]) for i in range(6)]
        found = [found[i] - mm(found[i], half_way[i]) for i in range(6)]
        size = size * 2
    inv[...] = jnp.zeros(inv.shape, F32)
    for k in (0, 3):
        x0, x1, x2 = found[k:k + 3]
        x10 = -mm(x1, mm(block(k + 1, k), x0))
        x21 = -mm(x2, mm(block(k + 2, k + 1), x1))
        x20 = -mm(x2, mm(block(k + 2, k), x0) + mm(block(k + 2, k + 1), x10))
        for i, j, val in ((0, 0, x0), (1, 1, x1), (2, 2, x2), (1, 0, x10), (2, 1, x21), (2, 0, x20)):
            inv[(k + i) * base:(k + i + 1) * base, (k + j) * base:(k + j + 1) * base] = val
    low = mm(left[half:, :], inv[:half, :half])
    inv[half:, :half] = -mm(inv[half:, half:], low)


def stage0(n, me, sources, dests, l_ref, lt_ref, ct_out, d_out, g_out, dt_out,
           left, corner, cmat, inv_a, inv_b, inv_t, slab_d, slab_t, slab_g,
           ct_send, ct_recv, ab_send, ab_recv, c_send, c_recv, x_send, x_recv, t_send, t_recv):
    x, y, z, e = me["x"], me["y"], me["z"], me["e"]
    big = n // 8
    half = n // 16
    quarter = n // 32
    tile = n // 128
    sib = dict(me, e=1 - e)
    diag = x == z

    slot = (x * (x - 1)) // 2 + z
    def ct_args(i):
        g, k, h, ee = i // 16, i // 4 % 4, i // 2 % 2, i % 2
        rows = pl.ds(pl.multiple_of(quarter * ee + tile * g, 8), tile)
        src = lt_ref.at[rows, pl.ds(pl.multiple_of(half * h, half), half)]
        to = {"x": k, "y": y, "z": 2 * e + h, "e": ee}
        return src, ct_out.at[slot, g], ct_send.at[i], ct_recv.at[slot, g], to, me

    source = diag & (y // 2 == e)
    c_source = diag & (e == 1) & (y < 2)

    def at(b, along_y):
        b = jnp.int32(b)
        return {"x": b, "y": along_y, "z": b, "e": e}

    odd = x % 2

    def dest(kind, i):
        g, j = i // 4, i % 4
        if kind == 0:
            return {"x": j, "y": y, "z": g, "e": e}
        if kind == 1:
            return {"x": odd * g + (1 - odd) * j, "y": odd * j + (1 - odd) * g, "z": y, "e": e}
        return {"x": g, "y": j, "z": y, "e": e}

    def full(kind, i):
        return i % 4 <= y if kind == 0 else i % 4 >= y

    pairs = [(b_row, b_col) for b_row in range(4) for b_col in range(b_row)]

    def ct_source(b_row, b_col):
        return {"x": jnp.int32(b_row), "y": y, "z": jnp.int32(b_col), "e": z // 2}

    def one(cond, where):
        return cond, 1, lambda k: where

    sources = sources + [one(None, ct_source(*pair)) for pair in pairs] + [one(diag, sib)]
    sources += [(diag, 2, lambda k: dict(me, y=2 * e + k)), (diag & (e == 1), 2, lambda k: dict(me, y=k))]
    sources += [(x <= y, 3, lambda b: at(b, y)), (None, 4, lambda b: at(b, z)), one(y >= z, at(1, z))]
    dests = dests + [(x > z, 16, lambda i: ct_args(i)[4]), one(diag, sib)]
    dests += [(cond, 3, lambda k: dict(me, y=(y + k + 1) % 4)) for cond in (source, c_source)]
    dests += [(diag, 16, lambda i: dest(1, i))]
    for kind, cond in ((0, diag & (x < 3)), (2, diag & (x == 1))):
        dests += [(cond & full(kind, i), 1, lambda k, kind=kind, i=i: dest(kind, jnp.int32(i))) for i in range(16)]
    meet(sources, dests, me)

    def ab_args(k, part):
        to = dict(me, y=(y + k) % 4)
        if part == 0:
            return l_ref, left, ab_send.at[k - 1], ab_recv.at[0], to, me
        return l_ref.at[pl.ds(half, half), :], corner, ab_send.at[k - 1], ab_recv.at[1], to, me

    for part in range(2):
        @pl.when(source & (y % 2 == part))
        def _(part=part):
            for k in (1, 3, 2):
                push(*ab_args(k, part))

    def c_args(k):
        to = dict(me, y=(y + k) % 4)
        return l_ref, cmat.at[y % 2], c_send.at[k - 1], c_recv.at[y % 2], to, me

    @pl.when(x > z)
    def _():
        loop(64, lambda i: push(*ct_args(i)))

    def swap_args(k):
        mine = [inv_a, inv_b, cmat.at[0], cmat.at[1]][k]
        return mine, mine, x_send.at[k], x_recv.at[k], sib, me

    @pl.when(diag)
    def _():
        for part, (dst, src_rows) in enumerate(((left, 0), (corner, half))):
            @pl.when(source & (y % 2 == part))
            def _(dst=dst, src_rows=src_rows):
                dst[...] = l_ref[src_rows:, :]

            arrived(dst, ab_send.at[0], ab_recv.at[part], dict(me, y=2 * e + part), me)

        @pl.when(c_source)
        def _():
            for k in (1, 3, 2):
                push(*c_args(k))

        invert_block(left, corner, inv_t, n // 48)
        for core, inv in ((0, inv_a), (1, inv_b)):
            @pl.when(e == core)
            def _(inv=inv):
                inv[...] = inv_t[...]

        @pl.when(e == 0)
        def _():
            push(*swap_args(0))
            for k in (1, 2, 3):
                arrived(swap_args(k)[1], x_send.at[k], x_recv.at[k], sib, me)
            sent(*swap_args(0))

        @pl.when(e == 1)
        def _():
            push(*swap_args(1))
            for part in range(2):
                @pl.when(y == part)
                def _(part=part):
                    cmat[part] = l_ref[...]

                arrived(cmat.at[part], c_send.at[0], c_recv.at[part], dict(me, y=jnp.int32(part)), me)
                push(*swap_args(2 + part))
            arrived(inv_a, x_send.at[0], x_recv.at[0], sib, me)
            for k in (1, 2, 3):
                sent(*swap_args(k))

        first = pl.multiple_of((y % 2) * half + e * quarter, 8)
        mine = pl.ds(first, quarter)

        def times_c(v):
            return jnp.concatenate([mm(v, cmat[0]), mm(v, cmat[1])], axis=1)

        def spread(kind, i):
            rows = pl.ds(pl.multiple_of(tile * (i // 4), 8), tile)
            src = (slab_d, slab_g, slab_t)[kind].at[rows, pl.ds(pl.multiple_of(half * (i % 4), half), half)]
            dst = (d_out, g_out)[kind].at[x] if kind < 2 else dt_out.at[0]
            recv = t_recv.at[kind, x] if kind < 2 else t_recv.at[2, 0]
            return src, dst, t_send.at[kind * 16 + i], recv, dest(kind, i), me

        def spread_all(use, kind):
            def step(i):
                if kind == 1:
                    use(*spread(kind, i))
                else:
                    @pl.when(full(kind, i))
                    def _():
                        use(*spread(kind, i))

            loop(16, step)

        lower = y >= 2

        @pl.when(jnp.logical_not(lower))
        def _():
            slab_d[:, :big] = inv_a[mine, :]

        @pl.when(lower)
        def _():
            v_b = inv_b[mine, :]
            slab_d[:, big:] = v_b
            slab_d[:, :big] = -mm(times_c(v_b), inv_a[...])

        @pl.when(x < 3)
        def _():
            spread_all(push, 0)

        @pl.when(jnp.logical_not(lower))
        def _():
            inv_t[...] = inv_a[...].T
            u_a = inv_t[mine, :]
            slab_t[:, :big] = u_a
            w = mm(u_a[:, :half], cmat[0], ((1,), (1,))) + mm(u_a[:, half:], cmat[1], ((1,), (1,)))
            slab_t[:, big:] = -mm(w, inv_b[...], ((1,), (1,)))

        @pl.when(lower)
        def _():
            inv_t[...] = inv_b[...].T
            slab_t[:, big:] = inv_t[mine, :]

        @pl.when(x == 1)
        def _():
            spread_all(push, 2)

        slab_g[:, big:] = mm(slab_t[:, big:], inv_b[...])

        @pl.when(jnp.logical_not(lower))
        def _():
            slab_g[:, :big] = mm(slab_t[:, :big] - times_c(slab_g[:, big:]), inv_a[...])

        @pl.when(lower)
        def _():
            slab_g[:, :big] = -mm(times_c(slab_g[:, big:]), inv_a[...])

        spread_all(push, 1)

        @pl.when(x < 3)
        def _():
            spread_all(sent, 0)

        @pl.when(x == 1)
        def _():
            spread_all(sent, 2)

        spread_all(sent, 1)

        for part in range(2):
            @pl.when(source & (y % 2 == part))
            def _(part=part):
                for k in (1, 2, 3):
                    sent(*ab_args(k, part))

        @pl.when(c_source)
        def _():
            for k in (1, 2, 3):
                sent(*c_args(k))

    @pl.when(x <= y)
    def _():
        loop(3, lambda b: arrived(d_out.at[b], t_send.at[0], t_recv.at[0, b], at(b, y), me))

    @pl.when(x > y)
    def _():
        d_out[...] = jnp.zeros(d_out.shape, F32)

    loop(4, lambda b: arrived(g_out.at[b], t_send.at[0], t_recv.at[1, b], at(b, z), me))

    @pl.when(y >= z)
    def _():
        arrived(dt_out.at[0], t_send.at[0], t_recv.at[2, 0], at(1, z), me)

    @pl.when(y < z)
    def _():
        dt_out[...] = jnp.zeros(dt_out.shape, F32)

    for k, pair in enumerate(pairs):
        loop(4, lambda g, k=k, pair=pair: arrived(ct_out.at[k, g], ct_send.at[0], ct_recv.at[k, g], ct_source(*pair), me))

    def finish():
        @pl.when(x > z)
        def _():
            loop(64, lambda i: sent(*ct_args(i)))

    return finish


def moved(to, source):
    return tuple(lambda me, way=way: dict(zip("xyz", (me[w] for w in way)), e=me["e"]) for way in (to, source))


W_TURN = moved("yzx", "zxy")
H_TURN = moved("yxz", "yxz")
Y_TURN = moved("zxy", "yzx")
YT_TURN = moved("zyx", "zyx")


class Move:
    def __init__(self, way, me, buf, send, recv):
        (self.to, self.source), self.me, self.buf, self.send, self.recv = way, me, buf, send, recv

    def args(self):
        return self.src, self.buf, self.send.at[0], self.recv.at[0], self.to(self.me), self.me

    def start(self, src):
        self.src = src
        push(*self.args())

    def wait(self):
        arrived(self.buf, self.send.at[0], self.recv.at[0], self.source(self.me), self.me)

    def finish(self):
        sent(*self.args())


class Line:
    def __init__(self, axis, me):
        self.at = me[axis]
        self.up, self.across, self.down = ((self.at + k) % 4 for k in (1, 2, 3))
        self.above, self.below = dict(me, **{axis: self.up}), dict(me, **{axis: self.down})


class Gather:
    def __init__(self, axis, me, buf, send, recv):
        self.line, self.buf, self.send, self.recv = Line(axis, me), buf, send, recv

    def piece(self, slot, half):
        if len(self.buf.shape) > 3:
            return self.buf.at[slot, pl.ds(half, 1)]
        rows = self.buf.shape[1] // 2
        return self.buf.at[slot, pl.ds(half * rows, rows)]

    def copies(self):
        line, buf = self.line, self.buf
        return [
            remote(self.src, buf.at[line.at], self.send.at[0], self.recv.at[0], line.above),
            remote(self.src, buf.at[line.at], self.send.at[1], self.recv.at[1], line.below),
            remote(self.piece(line.down, 0), self.piece(line.down, 0), self.send.at[2], self.recv.at[2], line.above),
            remote(self.piece(line.up, 1), self.piece(line.up, 1), self.send.at[3], self.recv.at[3], line.below)]

    def start(self, src):
        self.src = src
        for copy in self.copies()[:2]:
            copy.start()
        self.buf[self.line.at] = src[...]

    def relay(self):
        line, buf = self.line, self.buf
        onward = self.copies()[2:]
        remote(buf.at[line.down], buf.at[line.down], self.send.at[0], self.recv.at[0], line.below).wait_recv()
        onward[0].start()
        remote(buf.at[line.up], buf.at[line.up], self.send.at[1], self.recv.at[1], line.above).wait_recv()
        onward[1].start()

    def wait(self):
        for half, whom in ((0, self.line.below), (1, self.line.above)):
            piece = self.piece(self.line.across, half)
            remote(piece, piece, self.send.at[2 + half], self.recv.at[2 + half], whom).wait_recv()

    def finish(self):
        for copy in self.copies():
            copy.wait_send()

    def rows(self, block=None):
        tiles = [self.buf[k] if block is None else self.buf[k, block] for k in range(4)]
        return jnp.concatenate(tiles, axis=0)


class Reduce:
    def __init__(self, axis, me, part, sib, half, land, out, s_send, s_recv, r_send, r_recv):
        self.line, self.me, self.part, self.sib, self.half, self.land, self.out = Line(axis, me), me, part, sib, half, land, out
        self.s_send, self.s_recv, self.send, self.recv = s_send, s_recv, r_send, r_recv
        self.other = dict(me, e=1 - me["e"])
        self.down, self.tile = out.shape[:2]

    def swap_args(self, d):
        rows = pl.ds(((1 - self.me["e"]) + 2 * d) * (4 * self.tile), 4 * self.tile)
        return self.part.at[rows, :], self.sib.at[d], self.s_send.at[d], self.s_recv.at[d], self.other, self.me

    def put(self, d, value):
        self.part[d * 8 * self.tile:(d + 1) * 8 * self.tile, :] = value
        push(*self.swap_args(d))

    def where(self, k, half=None):
        first = pl.multiple_of(k * self.tile, 8)
        if half is None:
            return slice(None), pl.ds(first, self.tile)
        if self.down > 1:
            return pl.ds(half, 1), pl.ds(first, self.tile)
        rows = self.tile // 2
        return slice(None), pl.ds(pl.multiple_of(first + half * rows, 8), rows)

    def copies(self):
        line, sib = self.line, self.sib
        return [
            remote(sib.at[self.where(line.across, 0)], self.half.at[0], self.send.at[0], self.recv.at[0], line.above),
            remote(sib.at[self.where(line.across, 1)], self.half.at[1], self.send.at[1], self.recv.at[1], line.below),
            remote(sib.at[self.where(line.up)], self.land.at[0], self.send.at[2], self.recv.at[2], line.above),
            remote(sib.at[self.where(line.down)], self.land.at[1], self.send.at[3], self.recv.at[3], line.below)]

    def start(self):
        tile = self.tile
        for d in range(self.down):
            arrived(self.sib.at[d], self.s_send.at[d], self.s_recv.at[d], self.other, self.me)
            first = pl.multiple_of((self.me["e"] + 2 * d) * (4 * tile), 8)
            self.sib[d] = self.part[pl.ds(first, 4 * tile), :] + self.sib[d]
        for copy in self.copies()[:2]:
            copy.start()

    def relay(self):
        line, copies = self.line, self.copies()
        for half, whom, k in ((0, line.below, line.up), (1, line.above, line.down)):
            got = self.half.at[half]
            remote(got, got, self.send.at[half], self.recv.at[half], whom).wait_recv()
            at = self.where(k, half)
            self.sib[at] = self.sib[at] + self.half[half]
            copies[2 + half].start()

    def wait(self, sign=1, more=None):
        for side, whom in ((0, self.line.below), (1, self.line.above)):
            got = self.land.at[side]
            remote(got, got, self.send.at[2 + side], self.recv.at[2 + side], whom).wait_recv()
        total = (self.land[0] + self.land[1]) + self.sib[self.where(self.line.at)]
        total = total if sign > 0 else -total
        self.out[...] = total if more is None else total + more

    def swapped(self):
        for d in range(self.down):
            sent(*self.swap_args(d))

    def finish(self):
        for copy in self.copies():
            copy.wait_send()


def turn(a, b):
    return mm(a, b, ((0,), (0,)))


class Output:
    def __init__(self, n, me, flat, extra, turned, send, f_recv, a_recv, u_recv):
        self.half, self.tile, self.me, self.send = n // 16, n // 128, me, send
        self.into = {"keep": (flat, f_recv), "add": (extra, a_recv), "turn": (turned, u_recv)}
        self.started = []

    def place(self, kind, h, g, ee):
        buf, recv = self.into[kind]
        first = ee * (4 * self.tile) + g * self.tile
        if kind == "turn":
            cols = pl.ds(pl.multiple_of(h * self.half, self.half), self.half)
            return buf.at[pl.ds(pl.multiple_of(first, 8), self.tile), cols], recv.at[h, g, ee]
        return buf.at[pl.ds(pl.multiple_of(first + h * self.half, 8), self.tile), :], recv.at[h, g, ee]

    def to(self, plan):
        b_row, b_col, kind, rax, cax, gax = plan
        a_r, a_c = self.me[rax], self.me[cax]
        if kind == "turn":
            return {"x": jnp.int32(b_col), "y": a_r, "z": jnp.int32(b_row), "e": a_c // 2}, a_c % 2
        return {"x": jnp.int32(b_row), "y": a_c, "z": jnp.int32(b_col), "e": a_r // 2}, a_r % 2

    def args(self, index):
        plan, src = self.started[index]
        to, h = self.to(plan)
        dst, recv = self.place(plan[2], h, self.me[plan[5]], self.me["e"])
        return src, dst, self.send.at[index], recv, to, self.me

    def start(self, src, *plan):
        self.started.append((plan, src))
        push(*self.args(len(self.started) - 1))

    def incoming(self, plan):
        b_row, b_col, kind, rax, cax, gax = plan
        to_x, to_z = (b_col, b_row) if kind == "turn" else (b_row, b_col)
        y, e = self.me["y"], self.me["e"]

        def find(i):
            h, g, ee = i // 8, i // 2 % 4, i % 2
            a_r, a_c = (y, 2 * e + h) if kind == "turn" else (2 * e + h, y)
            return h, g, ee, {rax: a_r, cax: a_c, gax: g, "e": ee}

        return (self.me["x"] == to_x) & (self.me["z"] == to_z), find

    def finish(self, out):
        for plan, _ in self.started:
            cond, find = self.incoming(plan)

            @pl.when(cond)
            def _(plan=plan, find=find):
                def take(i):
                    h, g, ee, at = find(i)
                    dst, recv = self.place(plan[2], h, g, ee)
                    arrived(dst, self.send.at[0], recv, at, self.me)

                loop(16, take)

        kinds = {}
        for plan, _ in self.started:
            where = (plan[1], plan[0]) if plan[2] == "turn" else plan[:2]
            kinds.setdefault(where, set()).add(plan[2])
        for (b_row, b_col), has in kinds.items():
            @pl.when((self.me["x"] == b_row) & (self.me["z"] == b_col))
            def _(has=has):
                terms = [self.into[kind][0][...] for kind in ("keep", "add") if kind in has]
                if "turn" in has:
                    terms.append(self.into["turn"][0][...].T)
                out[...] = sum(terms[1:], terms[0])
        for index in range(len(self.started)):
            sent(*self.args(index))


ZXY, YXZ, ZYX = tuple("zxy"), tuple("yxz"), tuple("zyx")
PLANS = [(r, c, "keep", *ZXY) for r in range(2) for c in range(2)]
PLANS += [(2 + r, c, kind, *YXZ) for r in range(2) for c in range(2) for kind in ("keep", "turn")]
PLANS += [(0, 0, "add", *ZXY), (1, 1, "add", *ZYX), (2, 2, "keep", *ZXY), (3, 3, "keep", *ZYX)]
PLANS += [(r, r - 1, kind, *YXZ) for r, keep in ((1, "add"), (3, "keep")) for kind in (keep, "turn")]
WIDE = ("w", "wt", "y", "h")
GATHERS = [("d0", "z"), ("d1", "z"), ("d2", "z"), ("g1", "x"), ("dt", "x"), ("g3", "x"), ("w0", "y"), ("w1", "y"), ("y0", "z"),
           ("y1", "z"), ("x21", "z"), ("w0t", "x"), ("w1t", "x"), ("g2t", "x"), ("yt1t", "x"), ("y1t", "x"), ("w", "y"),
           ("wt", "x"), ("y", "z")]
MOVES = [("w0t", W_TURN), ("w1t", W_TURN), ("g2t", H_TURN), ("yt1t", YT_TURN), ("y1t", Y_TURN), ("wt", W_TURN)]
REDUCES = [("w0", "y"), ("w1", "y"), ("x21", "z"), ("y0", "z"), ("y1", "z"), ("yt1", "z"), ("h0", "y"), ("h1", "y"),
           ("w", "y"), ("y", "z"), ("h", "y")]


def scratch_plan(n):
    big, half, quarter, tile = n // 8, n // 16, n // 32, n // 128
    dma, vmem = pltpu.SemaphoreType.DMA, lambda *shape: pltpu.VMEM(shape, F32)
    pairs, four = 6, 4
    groups = [[vmem(pairs, four, tile, half), vmem(four, tile, half), vmem(four, tile, half), vmem(1, tile, half),
               vmem(big, half), vmem(half, half), vmem(2, big, half)]
              + [vmem(big, big)] * 3 + [vmem(quarter, 2 * big)] * 3
              + [dma((64,)), dma((pairs, four)), dma((3,)), dma((2,)), dma((3,)), dma((2,)), dma((four,)), dma((four,)),
                 dma((48,)), dma((3, four))]]
    for name, _ in GATHERS:
        wide = name in WIDE
        shape = (2, tile, 2 * half) if wide else (tile, half)
        groups.append([vmem(four, *shape), dma((four,)), dma((four,))])
    for name, _ in MOVES:
        wide = name in WIDE
        groups.append([vmem(2, tile, 2 * half) if wide else vmem(tile, half), dma((1,)), dma((1,))])
    for name, _ in REDUCES:
        wide = name in WIDE
        down, width = (2, 2 * half) if wide else (1, half)
        part = [] if wide else [vmem(half, width)]
        piece = vmem(2, 1, tile if wide else tile // 2, width)
        groups.append(part + [vmem(down, quarter, width), piece, vmem(2, down, tile, width), vmem(down, tile, width),
                       dma((down,)), dma((down,)), dma((four,)), dma((four,))])
    hubs = dma((2, four, 2))
    groups.append([vmem(big, half), vmem(big, half), vmem(half, big), dma((len(PLANS),)), hubs, hubs, hubs])
    return groups


def whole_kernel(n, sizes, l_ref, lt_ref, out, *refs):
    half = n // 16
    me = coords()
    groups = []
    for size in sizes:
        groups.append(refs[:size])
        refs = refs[size:]
    first, groups = groups[0], groups[1:]
    ga = {name: Gather(axis, me, *group) for (name, axis), group in zip(GATHERS, groups)}
    groups = groups[len(GATHERS):]
    mv = {name: Move(way, me, *group) for (name, way), group in zip(MOVES, groups)}
    groups = groups[len(MOVES):]
    re = {name: Reduce(axis, me, *((first[9],) if name in WIDE else ()), *group)
          for (name, axis), group in zip(REDUCES, groups)}
    res = Output(n, me, *groups[-1])

    lines = [(None, 4, lambda k, axis=axis: dict(me, **{axis: k})) for axis in "xyz"]
    turns = [W_TURN, H_TURN, Y_TURN, YT_TURN]
    sources = lines + [(None, 1, lambda k, way=way: way[1](me)) for way in turns]
    dests = lines + [(None, 1, lambda k, way=way: way[0](me)) for way in turns]
    for plan in PLANS:
        cond, find = res.incoming(plan)
        sources.append((cond, 16, lambda i, find=find: find(i)[-1]))
        dests.append((None, 1, lambda k, plan=plan: res.to(plan)[0]))
    ct, d, g, dt = first[:4]
    ending = stage0(n, me, sources, dests, l_ref, lt_ref, *first)

    def ctr(r, c):
        slot = (r * (r - 1)) // 2 + c
        return jnp.concatenate([ct[slot, k] for k in range(4)], axis=0)

    def cols(array, r, c):
        return array.at[r, :, pl.ds(c * half, half)]

    for name, src in (("d0", d.at[0]), ("d2", d.at[2]), ("dt", dt.at[0]), ("g1", g.at[1]), ("g3", g.at[3]), ("d1", d.at[1])):
        ga[name].start(src)

    def each(names, *steps):
        for step in steps:
            for name in names:
                step(name)

    def gathered(name):
        ga[name].relay()

    def ready(name):
        ga[name].wait()

    def begin(name):
        re[name].start()

    def passed(name):
        re[name].relay()

    def turned(name):
        mv[name].wait()
        ga[name].start(mv[name].buf)

    each(("d0", "d2"), gathered, ready)
    for name, pair, right in (("w0", (1, 0), "d0"), ("w1", (3, 2), "d2")):
        re[name].put(0, turn(ctr(*pair), ga[right].rows()))
    each(("w0", "w1"), begin)
    each(("dt", "g1", "g3", "d1"), gathered)
    each(("w0", "w1"), passed)
    for name in ("w0", "w1"):
        re[name].wait()
        ga[name].start(re[name].out.at[0])
    for name in ("w0", "w1"):
        mv[name + "t"].start(re[name].out.at[0])
    each(("w0", "w1"), gathered, ready)
    each(("dt", "g1", "g3"), ready)
    made = ("x21", "y0", "y1", "yt1")
    for name, left, right in zip(made, ("dt", "g1", "g3", "w1"), ("w0", "w0", "w1", "g3")):
        re[name].put(0, turn(ga[left].rows(), ga[right].rows()))
    each(made, begin)
    each(("w0t", "w1t"), turned)
    each(made, passed)
    re["x21"].wait(-1)
    ga["x21"].start(re["x21"].out.at[0])
    for name in made[1:]:
        re[name].wait(-1)
    for name in ("y0", "y1"):
        ga[name].start(re[name].out.at[0])
    for name in ("yt1", "y1"):
        mv[name + "t"].start(re[name].out.at[0])
    each(("x21",), gathered, ready)
    ready("d1")
    zero, one = ga["d0"].rows(), jnp.concatenate([ga["x21"].rows(), ga["d1"].rows()], axis=1)
    for r in range(2):
        top = turn(ctr(2 + r, 1), one)
        re["w"].put(r, jnp.concatenate([top[:, :half] + turn(ctr(2 + r, 0), zero), top[:, half:]], axis=1))
    begin("w")
    each(("w0t", "w1t", "y0", "y1"), gathered, ready)
    passed("w")
    each(("yt1t", "y1t"), turned)
    for name, left, right in (("h1", "w1t", "y1"), ("h0", "w0t", "y0")):
        re[name].put(0, turn(ga[left].rows(), ga[right].rows()))
    each(("h1", "h0"), begin)
    re["w"].wait()
    re["w"].swapped()
    ga["w"].start(re["w"].out)
    each(("h1", "h0"), passed)
    re["h1"].wait(-1, g[2:3])
    mv["g2t"].start(re["h1"].out.at[0])
    re["h0"].wait(-1, g[0:1])
    each(("yt1t", "y1t"), gathered)
    turned("g2t")
    each(("w", "g2t"), gathered)
    each(("w", "g2t", "yt1t", "y1t"), ready)
    for r, names in enumerate((("g2t", "y1t"), ("yt1t", "g3"))):
        re["y"].put(r, sum(turn(ga[name].rows(), ga["w"].rows(c)) for c, name in enumerate(names)))
    begin("y")
    mv["wt"].start(re["w"].out)
    passed("y")
    turned("wt")
    re["y"].wait(-1)
    re["y"].swapped()
    ga["y"].start(re["y"].out)
    each(("y", "wt"), gathered, ready)
    for r in range(2):
        left = [ga["wt"].rows(c)[:, r * half:(r + 1) * half] for c in range(2)]
        re["h"].put(r, sum(turn(left[c], ga["y"].rows(c)) for c in range(2)))
    begin("h")
    res.start(g.at[1], 1, 1, "add", *ZYX)
    res.start(g.at[3], 3, 3, "keep", *ZYX)
    for name, r, keep in (("y0", 1, "add"), ("y1", 3, "keep")):
        for kind in (keep, "turn"):
            res.start(re[name].out.at[0], r, r - 1, kind, *YXZ)
    res.start(re["h0"].out.at[0], 0, 0, "add", *ZXY)
    res.start(re["h1"].out.at[0], 2, 2, "keep", *ZXY)
    passed("h")
    for r in range(2):
        for c in range(2):
            for kind in ("keep", "turn"):
                res.start(cols(re["y"].out, r, c), 2 + r, c, kind, *YXZ)
    re["h"].wait(-1)
    for r in range(2):
        for c in range(2):
            res.start(cols(re["h"].out, r, c), r, c, "keep", *ZXY)
    res.finish(out)
    ending()
    for part in [*ga.values(), *mv.values(), *re.values()]:
        part.finish()
    for name in ("w0", "w1", *made, "h0", "h1", "h"):
        re[name].swapped()


def solution(mesh):
    def local_fn(l_blk):
        n = l_blk.shape[0] * 8
        groups = scratch_plan(n)
        spec = pl.BlockSpec(memory_space=pltpu.VMEM)
        call = pl.pallas_call(
            functools.partial(whole_kernel, n, [len(group) for group in groups]),
            out_shape=jax.ShapeDtypeStruct(l_blk.shape, F32),
            in_specs=[spec, spec],
            out_specs=spec,
            scratch_shapes=sum(groups, []),
            compiler_params=pltpu.CompilerParams(
                has_side_effects=True, vmem_limit_bytes=VMEM_LIMIT, collective_id=0),
            name="whole",
        )
        return call(l_blk, l_blk.T)

    spec = P(("batch", "row"), "col")
    return jax.shard_map(local_fn, mesh=mesh, in_specs=(spec,), out_specs=spec, check_vma=False)
```

```python
import functools

import jax
import jax.numpy as jnp
from jax import lax
from jax.experimental import pallas as pl
from jax.experimental.pallas import tpu as pltpu
from jax.sharding import PartitionSpec as P

MESH = pl.DeviceIdType.MESH
HIGHEST = lax.Precision.HIGHEST
F32 = jnp.float32
VMEM_LIMIT = 67043328


def coords():
    col = lax.axis_index("col")
    row = lax.axis_index("row")
    return {"x": row // 2, "y": col % 4, "z": col // 4, "e": row % 2}


def device(at):
    return (0, 4 * at["z"] + at["y"], 2 * at["x"] + at["e"])


def same(p, q):
    return (p["x"] == q["x"]) & (p["y"] == q["y"]) & (p["z"] == q["z"]) & (p["e"] == q["e"])


def mm(a, b, dims=((1,), (0,))):
    return lax.dot_general(a, b, (dims, ((), ())), precision=HIGHEST, preferred_element_type=F32)


def loop(count, body):
    def step(k, carry):
        body(k)
        return carry

    lax.fori_loop(0, count, step, jnp.int32(0))


def push(src, dst, send_sem, recv_sem, to, me):
    here = same(to, me)

    @pl.when(here)
    def _():
        dst[...] = src[...]

    @pl.when(jnp.logical_not(here))
    def _():
        pltpu.make_async_remote_copy(
            src_ref=src, dst_ref=dst, send_sem=send_sem, recv_sem=recv_sem, device_id=device(to), device_id_type=MESH
        ).start()


def sent(src, dst, send_sem, recv_sem, to, me):
    @pl.when(jnp.logical_not(same(to, me)))
    def _():
        pltpu.make_async_remote_copy(
            src_ref=src, dst_ref=dst, send_sem=send_sem, recv_sem=recv_sem, device_id=device(to), device_id_type=MESH
        ).wait_send()


def arrived(dst, send_sem, recv_sem, source, me):
    @pl.when(jnp.logical_not(same(source, me)))
    def _():
        pltpu.make_async_remote_copy(
            src_ref=dst, dst_ref=dst, send_sem=send_sem, recv_sem=recv_sem, device_id=device(source), device_id_type=MESH
        ).wait_recv()


def meet(sources, dests, me):
    barrier = pltpu.get_barrier_semaphore()

    def other(cond, at):
        apart = jnp.logical_not(same(at, me))
        return apart if cond is None else apart & cond

    total = jnp.int32(0)
    for cond, count, which in sources:
        def tell(k, which=which):
            @pl.when(other(None, which(k)))
            def _():
                pl.semaphore_signal(barrier, inc=1, device_id=device(which(k)), device_id_type=MESH)

        if cond is None:
            loop(count, tell)
        else:
            @pl.when(cond)
            def _(count=count, tell=tell):
                loop(count, tell)

    for cond, count, which in dests:
        def add(k, carry, cond=cond, which=which):
            return carry + other(cond, which(k)).astype(jnp.int32)

        total = lax.fori_loop(0, count, add, total)

    @pl.when(total > 0)
    def _():
        pl.semaphore_wait(barrier, total)


def remote(src, dst, send_sem, recv_sem, to):
    return pltpu.make_async_remote_copy(
        src_ref=src, dst_ref=dst, send_sem=send_sem, recv_sem=recv_sem, device_id=device(to), device_id_type=MESH)


def invert_block(left, corner, inv, base):
    half = 3 * base
    rows = lax.broadcasted_iota(jnp.int32, (base, base), 0)
    cols = lax.broadcasted_iota(jnp.int32, (base, base), 1)
    eye = rows == cols

    def block(i, j):
        if j < 3:
            return left[i * base:(i + 1) * base, j * base:(j + 1) * base]
        return corner[(i - 3) * base:(i - 2) * base, (j - 3) * base:(j - 2) * base]

    tri = [block(i, i) for i in range(6)]
    found = []
    for i in range(6):
        diag = jnp.sum(jnp.where(eye, tri[i], 0.0), axis=1, keepdims=True)
        found.append(jnp.where(eye, 1.0 / diag, 0.0))
    size = 1
    while size < base:
        below = ((rows // size) % 2 == 1) & (cols // size == rows // size - 1)
        half_way = [mm(jnp.where(below, tri[i], 0.0), found[i]) for i in range(6)]
        found = [found[i] - mm(found[i], half_way[i]) for i in range(6)]
        size = size * 2
    inv[...] = jnp.zeros(inv.shape, F32)
    for k in (0, 3):
        x0, x1, x2 = found[k:k + 3]
        x10 = -mm(x1, mm(block(k + 1, k), x0))
        x21 = -mm(x2, mm(block(k + 2, k + 1), x1))
        x20 = -mm(x2, mm(block(k + 2, k), x0) + mm(block(k + 2, k + 1), x10))
        for i, j, val in ((0, 0, x0), (1, 1, x1), (2, 2, x2), (1, 0, x10), (2, 1, x21), (2, 0, x20)):
            inv[(k + i) * base:(k + i + 1) * base, (k + j) * base:(k + j + 1) * base] = val
    low = mm(left[half:, :], inv[:half, :half])
    inv[half:, :half] = -mm(inv[half:, half:], low)


def stage0(n, me, sources, dests, l_ref, ct_out, d_out, g_out, dt_out,
           left, corner, cmat, inv_a, inv_b, inv_t, slab_d, slab_t, slab_g, lt_ref,
           ct_send, ct_recv, ab_send, ab_recv, c_send, c_recv, x_send, x_recv, t_send, t_recv):
    x, y, z, e = me["x"], me["y"], me["z"], me["e"]
    big = n // 8
    half = n // 16
    quarter = n // 32
    tile = n // 128
    sib = dict(me, e=1 - e)
    diag = x == z

    slot = (x * (x - 1)) // 2 + z
    def ct_args(i):
        g, k, h, ee = i // 16, i // 4 % 4, i // 2 % 2, i % 2
        rows = pl.ds(pl.multiple_of(quarter * ee + tile * g, 8), tile)
        src = lt_ref.at[rows, pl.ds(pl.multiple_of(half * h, half), half)]
        to = {"x": k, "y": y, "z": 2 * e + h, "e": ee}
        return src, ct_out.at[slot, g], ct_send.at[i], ct_recv.at[slot, g], to, me

    up, down = dict(me, y=(y + 1) % 4), dict(me, y=(y + 3) % 4)

    def at(b, along_y):
        b = jnp.int32(b)
        return {"x": b, "y": along_y, "z": b, "e": e}

    odd = x % 2

    def dest(kind, i):
        g, j = i // 4, i % 4
        if kind == 0:
            return {"x": j, "y": y, "z": g, "e": e}
        if kind == 1:
            return {"x": odd * g + (1 - odd) * j, "y": odd * j + (1 - odd) * g, "z": y, "e": e}
        return {"x": g, "y": j, "z": y, "e": e}

    def full(kind, i):
        return i % 4 <= y if kind == 0 else i % 4 >= y

    pairs = [(b_row, b_col) for b_row in range(4) for b_col in range(b_row)]

    def ct_source(b_row, b_col):
        return {"x": jnp.int32(b_row), "y": y, "z": jnp.int32(b_col), "e": z // 2}

    def one(cond, where):
        return cond, 1, lambda k: where

    sources = sources + [one(None, ct_source(*pair)) for pair in pairs] + [one(diag, sib)]
    sources += [one(diag, up), one(diag, down)]
    sources += [(x <= y, 3, lambda b: at(b, y)), (None, 4, lambda b: at(b, z)), one(y >= z, at(1, z))]
    dests = dests + [(x > z, 16, lambda i: ct_args(i)[4]), one(diag, sib)]
    dests += [one(diag, up), one(diag, down)]
    dests += [(diag, 16, lambda i: dest(1, i))]
    for kind, cond in ((0, diag & (x < 3)), (2, diag & (x == 1))):
        dests += [(cond & full(kind, i), 1, lambda k, kind=kind, i=i: dest(kind, jnp.int32(i))) for i in range(16)]

    @pl.when(x > z)
    def _():
        lt_ref[...] = l_ref[...].T

    meet(sources, dests, me)

    place = (y + 4 - 2 * e) % 4
    upper, under = left.at[pl.ds(0, half), :], left.at[pl.ds(half, half), :]

    def ab_copy(chunk, way, own):
        dst = (upper, under, corner)[chunk]
        src = l_ref.at[pl.ds(half * min(chunk, 1), half), :] if own else dst
        return remote(src, dst, ab_send.at[chunk + 3 * way], ab_recv.at[chunk], (up, down)[way])

    def ab_came(chunk):
        dst = (upper, under, corner)[chunk]
        remote(dst, dst, ab_send.at[chunk], ab_recv.at[chunk], up).wait_recv()

    ab_sends = [("001", "111", "101", "011"), ("211", "201", "000"), ("200",), ("110",)]

    def c_copy(part, chunk, way, own):
        rows = pl.ds(half * chunk, half)
        dst = cmat.at[part, rows, :]
        src = l_ref.at[rows, :] if own else dst
        return remote(src, dst, c_send.at[chunk + 2 * way], c_recv.at[2 * part + chunk], (up, down)[way])

    def c_came(part, chunk):
        c_copy(part, chunk, 0, 0).wait_recv()

    c_sends = [("0001", "0011", "0101", "0111"), ("1001", "1011", "1101", "1111"), ("1000", "1100"), ("0010", "0110")]

    for part in range(2):
        @pl.when(diag & (place == part))
        def _(part=part):
            for code in ab_sends[part]:
                if int(code[2]):
                    ab_copy(*map(int, code)).start()

    @pl.when(x > z)
    def _():
        loop(64, lambda i: push(*ct_args(i)))

    def swap_args(k):
        mine = [inv_a, inv_b, cmat.at[0], cmat.at[1]][k]
        return mine, mine, x_send.at[k], x_recv.at[k], sib, me

    def swap_came(k):
        arrived(swap_args(k)[1], x_send.at[k], x_recv.at[k], sib, me)

    closing = []

    @pl.when(diag)
    def _():
        for part, order in enumerate(("2", "01", "201", "102")):
            @pl.when(place == part)
            def _(part=part, order=order):
                if part == 0:
                    left[...] = l_ref[...]
                elif part == 1:
                    corner[...] = l_ref[half:, :]
                for chunk in order:
                    ab_came(int(chunk))
                    if part > 0 and chunk == order[0]:
                        ab_copy(*map(int, ab_sends[part][-1])).start()

        for part in range(2):
            @pl.when((e == 1) & (y == part))
            def _(part=part):
                for code in c_sends[part]:
                    c_copy(*map(int, code)).start()

        invert_block(left, corner, inv_t, n // 48)
        for core, inv in ((0, inv_a), (1, inv_b)):
            @pl.when(e == core)
            def _(inv=inv):
                inv[...] = inv_t[...]

        lower, across = y >= 2, ((1,), (1,))
        first = pl.multiple_of((y % 2) * half + e * quarter, 8)
        mine = pl.ds(first, quarter)

        for core in range(2):
            @pl.when(e == core)
            def _(core=core):
                push(*swap_args(core))
                swap_came(1 - core)

        @pl.when(jnp.logical_not(lower))
        def _():
            inv_t[...] = inv_a[...].T
            slab_t[:, :big] = inv_t[mine, :]
            slab_d[:, :big] = inv_a[mine, :]

        @pl.when(lower)
        def _():
            inv_t[...] = inv_b[...].T
            slab_t[:, big:] = inv_t[mine, :]
            slab_g[:, big:] = mm(slab_t[:, big:], inv_b[...])
            slab_d[:, big:] = inv_b[mine, :]

        @pl.when(e == 1)
        def _():
            for part in range(2):
                @pl.when(y == part)
                def _(part=part):
                    cmat[part] = l_ref[...]
                    c_came(1 - part, 0)
                    c_came(1 - part, 1)

                @pl.when(y == part + 2)
                def _(part=part):
                    for code in c_sends[part + 2]:
                        c_came(1 - part, int(code[1]))
                        c_copy(*map(int, code)).start()
                    c_came(part, 0)
                    c_came(part, 1)

            for part in range(2):
                push(*swap_args(2 + part))

        @pl.when(e == 0)
        def _():
            swap_came(2)
            swap_came(3)

        def times_c(v):
            return jnp.concatenate([mm(v, cmat[0]), mm(v, cmat[1])], axis=1)

        def spread(kind, i):
            rows = pl.ds(pl.multiple_of(tile * (i // 4), 8), tile)
            src = (slab_d, slab_g, slab_t)[kind].at[rows, pl.ds(pl.multiple_of(half * (i % 4), half), half)]
            dst = (d_out, g_out)[kind].at[x] if kind < 2 else dt_out.at[0]
            recv = t_recv.at[kind, x] if kind < 2 else t_recv.at[2, 0]
            return src, dst, t_send.at[kind * 16 + i], recv, dest(kind, i), me

        def spread_all(use, kind):
            def step(i):
                if kind == 1:
                    use(*spread(kind, i))
                else:
                    @pl.when(full(kind, i))
                    def _():
                        use(*spread(kind, i))

            loop(16, step)

        @pl.when(lower)
        def _():
            slab_d[:, :big] = -mm(times_c(slab_d[:, big:]), inv_a[...])

        @pl.when(x < 3)
        def _():
            spread_all(push, 0)

        @pl.when(jnp.logical_not(lower))
        def _():
            w = mm(slab_t[:, :half], cmat[0], across) + mm(slab_t[:, half:big], cmat[1], across)
            slab_t[:, big:] = -mm(w, inv_b[...], across)

        @pl.when(x == 1)
        def _():
            spread_all(push, 2)

        @pl.when(jnp.logical_not(lower))
        def _():
            slab_g[:, big:] = mm(slab_t[:, big:], inv_b[...])
            slab_g[:, :big] = mm(slab_t[:, :big] - times_c(slab_g[:, big:]), inv_a[...])

        @pl.when(lower)
        def _():
            slab_g[:, :big] = -mm(times_c(slab_g[:, big:]), inv_a[...])

        spread_all(push, 1)

        def close():
            @pl.when(x < 3)
            def _():
                spread_all(sent, 0)

            @pl.when(x == 1)
            def _():
                spread_all(sent, 2)

            spread_all(sent, 1)
            for part in range(4):
                @pl.when(place == part)
                def _(part=part):
                    for code in ab_sends[part]:
                        ab_copy(*map(int, code)).wait_send()

                @pl.when((e == 1) & (y == part))
                def _(part=part):
                    for code in c_sends[part]:
                        c_copy(*map(int, code)).wait_send()

            for core in range(2):
                @pl.when(e == core)
                def _(core=core):
                    for k in (0,) if core == 0 else (1, 2, 3):
                        sent(*swap_args(k))

        closing.append(close)

    @pl.when(x <= y)
    def _():
        loop(3, lambda b: arrived(d_out.at[b], t_send.at[0], t_recv.at[0, b], at(b, y), me))

    @pl.when(x > y)
    def _():
        d_out[...] = jnp.zeros(d_out.shape, F32)

    for k, pair in enumerate(pairs):
        loop(4, lambda g, k=k, pair=pair: arrived(ct_out.at[k, g], ct_send.at[0], ct_recv.at[k, g], ct_source(*pair), me))

    def late():
        loop(4, lambda b: arrived(g_out.at[b], t_send.at[0], t_recv.at[1, b], at(b, z), me))

        @pl.when(y >= z)
        def _():
            arrived(dt_out.at[0], t_send.at[0], t_recv.at[2, 0], at(1, z), me)

        @pl.when(y < z)
        def _():
            dt_out[...] = jnp.zeros(dt_out.shape, F32)

    def finish():
        @pl.when(diag)
        def _():
            closing[0]()

        @pl.when(x > z)
        def _():
            loop(64, lambda i: sent(*ct_args(i)))

    return late, finish


def moved(to, source):
    return tuple(lambda me, way=way: dict(zip("xyz", (me[w] for w in way)), e=me["e"]) for way in (to, source))


W_TURN = moved("yzx", "zxy")
H_TURN = moved("yxz", "yxz")
Y_TURN = moved("zxy", "yzx")
YT_TURN = moved("zyx", "zyx")


class Move:
    def __init__(self, way, me, buf, send, recv):
        (self.to, self.source), self.me, self.buf, self.send, self.recv = way, me, buf, send, recv

    def args(self):
        return self.src, self.buf, self.send.at[0], self.recv.at[0], self.to(self.me), self.me

    def start(self, src):
        self.src = src
        push(*self.args())

    def wait(self):
        arrived(self.buf, self.send.at[0], self.recv.at[0], self.source(self.me), self.me)

    def finish(self):
        sent(*self.args())


class Line:
    def __init__(self, axis, me):
        self.at = me[axis]
        self.up, self.across, self.down = ((self.at + k) % 4 for k in (1, 2, 3))
        self.above, self.below = dict(me, **{axis: self.up}), dict(me, **{axis: self.down})


class Gather:
    def __init__(self, axis, me, buf, send, recv):
        self.line, self.buf, self.send, self.recv = Line(axis, me), buf, send, recv

    def piece(self, slot, half):
        if len(self.buf.shape) > 3:
            return self.buf.at[slot, pl.ds(half, 1)]
        rows = self.buf.shape[1] // 2
        return self.buf.at[slot, pl.ds(half * rows, rows)]

    def copies(self):
        line, buf = self.line, self.buf
        return [
            remote(self.src, buf.at[line.at], self.send.at[0], self.recv.at[0], line.above),
            remote(self.src, buf.at[line.at], self.send.at[1], self.recv.at[1], line.below),
            remote(self.piece(line.down, 0), self.piece(line.down, 0), self.send.at[2], self.recv.at[2], line.above),
            remote(self.piece(line.up, 1), self.piece(line.up, 1), self.send.at[3], self.recv.at[3], line.below)]

    def start(self, src):
        self.src = src
        for copy in self.copies()[:2]:
            copy.start()
        self.buf[self.line.at] = src[...]

    def relay(self):
        line, buf = self.line, self.buf
        onward = self.copies()[2:]
        remote(buf.at[line.down], buf.at[line.down], self.send.at[0], self.recv.at[0], line.below).wait_recv()
        onward[0].start()
        remote(buf.at[line.up], buf.at[line.up], self.send.at[1], self.recv.at[1], line.above).wait_recv()
        onward[1].start()

    def wait(self):
        for half, whom in ((0, self.line.below), (1, self.line.above)):
            piece = self.piece(self.line.across, half)
            remote(piece, piece, self.send.at[2 + half], self.recv.at[2 + half], whom).wait_recv()

    def finish(self):
        for copy in self.copies():
            copy.wait_send()

    def rows(self, block=None):
        tiles = [self.buf[k] if block is None else self.buf[k, block] for k in range(4)]
        return jnp.concatenate(tiles, axis=0)


class Reduce:
    def __init__(self, axis, me, part, sib, half, land, out, s_send, s_recv, r_send, r_recv):
        self.line, self.me, self.part, self.sib, self.half, self.land, self.out = Line(axis, me), me, part, sib, half, land, out
        self.s_send, self.s_recv, self.send, self.recv = s_send, s_recv, r_send, r_recv
        self.other = dict(me, e=1 - me["e"])
        self.down, self.tile = out.shape[:2]

    def swap_args(self, d):
        rows = pl.ds(((1 - self.me["e"]) + 2 * d) * (4 * self.tile), 4 * self.tile)
        return self.part.at[rows, :], self.sib.at[d], self.s_send.at[d], self.s_recv.at[d], self.other, self.me

    def put(self, d, value):
        self.part[d * 8 * self.tile:(d + 1) * 8 * self.tile, :] = value
        push(*self.swap_args(d))

    def where(self, k, half=None):
        first = pl.multiple_of(k * self.tile, 8)
        if half is None:
            return slice(None), pl.ds(first, self.tile)
        if self.down > 1:
            return pl.ds(half, 1), pl.ds(first, self.tile)
        rows = self.tile // 2
        return slice(None), pl.ds(pl.multiple_of(first + half * rows, 8), rows)

    def copies(self):
        line, sib = self.line, self.sib
        return [
            remote(sib.at[self.where(line.across, 0)], self.half.at[0], self.send.at[0], self.recv.at[0], line.above),
            remote(sib.at[self.where(line.across, 1)], self.half.at[1], self.send.at[1], self.recv.at[1], line.below),
            remote(sib.at[self.where(line.up)], self.land.at[0], self.send.at[2], self.recv.at[2], line.above),
            remote(sib.at[self.where(line.down)], self.land.at[1], self.send.at[3], self.recv.at[3], line.below)]

    def start(self):
        tile = self.tile
        for d in range(self.down):
            arrived(self.sib.at[d], self.s_send.at[d], self.s_recv.at[d], self.other, self.me)
            first = pl.multiple_of((self.me["e"] + 2 * d) * (4 * tile), 8)
            self.sib[d] = self.part[pl.ds(first, 4 * tile), :] + self.sib[d]
        for copy in self.copies()[:2]:
            copy.start()

    def relay(self):
        line, copies = self.line, self.copies()
        for half, whom, k in ((0, line.below, line.up), (1, line.above, line.down)):
            got = self.half.at[half]
            remote(got, got, self.send.at[half], self.recv.at[half], whom).wait_recv()
            at = self.where(k, half)
            self.sib[at] = self.sib[at] + self.half[half]
            copies[2 + half].start()

    def wait(self, sign=1, more=None):
        for side, whom in ((0, self.line.below), (1, self.line.above)):
            got = self.land.at[side]
            remote(got, got, self.send.at[2 + side], self.recv.at[2 + side], whom).wait_recv()
        total = (self.land[0] + self.land[1]) + self.sib[self.where(self.line.at)]
        total = total if sign > 0 else -total
        self.out[...] = total if more is None else total + more

    def swapped(self):
        for d in range(self.down):
            sent(*self.swap_args(d))

    def finish(self):
        for copy in self.copies():
            copy.wait_send()


def turn(a, b):
    return mm(a, b, ((0,), (0,)))


class Output:
    def __init__(self, n, me, flat, extra, turned, send, f_recv, a_recv, u_recv):
        self.half, self.tile, self.me, self.send = n // 16, n // 128, me, send
        self.into = {"keep": (flat, f_recv), "add": (extra, a_recv), "turn": (turned, u_recv)}
        self.started = []

    def place(self, kind, h, g, ee):
        buf, recv = self.into[kind]
        first = ee * (4 * self.tile) + g * self.tile
        if kind == "turn":
            cols = pl.ds(pl.multiple_of(h * self.half, self.half), self.half)
            return buf.at[pl.ds(pl.multiple_of(first, 8), self.tile), cols], recv.at[h, g, ee]
        return buf.at[pl.ds(pl.multiple_of(first + h * self.half, 8), self.tile), :], recv.at[h, g, ee]

    def to(self, plan):
        b_row, b_col, kind, rax, cax, gax = plan
        a_r, a_c = self.me[rax], self.me[cax]
        if kind == "turn":
            return {"x": jnp.int32(b_col), "y": a_r, "z": jnp.int32(b_row), "e": a_c // 2}, a_c % 2
        return {"x": jnp.int32(b_row), "y": a_c, "z": jnp.int32(b_col), "e": a_r // 2}, a_r % 2

    def args(self, index):
        plan, src = self.started[index]
        to, h = self.to(plan)
        dst, recv = self.place(plan[2], h, self.me[plan[5]], self.me["e"])
        return src, dst, self.send.at[index], recv, to, self.me

    def start(self, src, *plan):
        self.started.append((plan, src))
        push(*self.args(len(self.started) - 1))

    def incoming(self, plan):
        b_row, b_col, kind, rax, cax, gax = plan
        to_x, to_z = (b_col, b_row) if kind == "turn" else (b_row, b_col)
        y, e = self.me["y"], self.me["e"]

        def find(i):
            h, g, ee = i // 8, i // 2 % 4, i % 2
            a_r, a_c = (y, 2 * e + h) if kind == "turn" else (2 * e + h, y)
            return h, g, ee, {rax: a_r, cax: a_c, gax: g, "e": ee}

        return (self.me["x"] == to_x) & (self.me["z"] == to_z), find

    def finish(self, out):
        for plan, _ in self.started:
            cond, find = self.incoming(plan)

            @pl.when(cond)
            def _(plan=plan, find=find):
                def take(i):
                    h, g, ee, at = find(i)
                    dst, recv = self.place(plan[2], h, g, ee)
                    arrived(dst, self.send.at[0], recv, at, self.me)

                loop(16, take)

        kinds = {}
        for plan, _ in self.started:
            where = (plan[1], plan[0]) if plan[2] == "turn" else plan[:2]
            kinds.setdefault(where, set()).add(plan[2])
        for (b_row, b_col), has in kinds.items():
            @pl.when((self.me["x"] == b_row) & (self.me["z"] == b_col))
            def _(has=has):
                terms = [self.into[kind][0][...] for kind in ("keep", "add") if kind in has]
                if "turn" in has:
                    terms.append(self.into["turn"][0][...].T)
                out[...] = sum(terms[1:], terms[0])
        for index in range(len(self.started)):
            sent(*self.args(index))


ZXY, YXZ, ZYX = tuple("zxy"), tuple("yxz"), tuple("zyx")
PLANS = [(r, c, "keep", *ZXY) for r in range(2) for c in range(2)]
PLANS += [(2 + r, c, kind, *YXZ) for r in range(2) for c in range(2) for kind in ("keep", "turn")]
PLANS += [(0, 0, "add", *ZXY), (1, 1, "add", *ZYX), (2, 2, "keep", *ZXY), (3, 3, "keep", *ZYX)]
PLANS += [(r, r - 1, kind, *YXZ) for r, keep in ((1, "add"), (3, "keep")) for kind in (keep, "turn")]
WIDE = ("w", "wt", "y", "h")
GATHERS = [("d0", "z"), ("d1", "z"), ("d2", "z"), ("g1", "x"), ("dt", "x"), ("g3", "x"), ("w0", "y"), ("w1", "y"), ("y0", "z"),
           ("y1", "z"), ("x21", "z"), ("w0t", "x"), ("w1t", "x"), ("g2t", "x"), ("yt1t", "x"), ("y1t", "x"), ("w", "y"),
           ("wt", "x"), ("y", "z")]
MOVES = [("w0t", W_TURN), ("w1t", W_TURN), ("g2t", H_TURN), ("yt1t", YT_TURN), ("y1t", Y_TURN), ("wt", W_TURN)]
REDUCES = [("w0", "y"), ("w1", "y"), ("x21", "z"), ("y0", "z"), ("y1", "z"), ("yt1", "z"), ("h0", "y"), ("h1", "y"),
           ("w", "y"), ("y", "z"), ("h", "y")]


def scratch_plan(n):
    big, half, quarter, tile = n // 8, n // 16, n // 32, n // 128
    dma, vmem = pltpu.SemaphoreType.DMA, lambda *shape: pltpu.VMEM(shape, F32)
    pairs, four = 6, 4
    groups = [[vmem(pairs, four, tile, half), vmem(four, tile, half), vmem(four, tile, half), vmem(1, tile, half),
               vmem(big, half), vmem(half, half), vmem(2, big, half)]
              + [vmem(big, big)] * 3 + [vmem(quarter, 2 * big)] * 3 + [vmem(half, big)]
              + [dma((64,)), dma((pairs, four)), dma((6,)), dma((3,)), dma((four,)), dma((four,)), dma((four,)), dma((four,)),
                 dma((48,)), dma((3, four))]]
    for name, _ in GATHERS:
        wide = name in WIDE
        shape = (2, tile, 2 * half) if wide else (tile, half)
        groups.append([vmem(four, *shape), dma((four,)), dma((four,))])
    for name, _ in MOVES:
        wide = name in WIDE
        groups.append([vmem(2, tile, 2 * half) if wide else vmem(tile, half), dma((1,)), dma((1,))])
    for name, _ in REDUCES:
        wide = name in WIDE
        down, width = (2, 2 * half) if wide else (1, half)
        part = [] if wide else [vmem(half, width)]
        piece = vmem(2, 1, tile if wide else tile // 2, width)
        groups.append(part + [vmem(down, quarter, width), piece, vmem(2, down, tile, width), vmem(down, tile, width),
                       dma((down,)), dma((down,)), dma((four,)), dma((four,))])
    hubs = dma((2, four, 2))
    groups.append([vmem(big, half), vmem(big, half), vmem(half, big), dma((len(PLANS),)), hubs, hubs, hubs])
    return groups


def whole_kernel(n, sizes, l_ref, out, *refs):
    half = n // 16
    me = coords()
    groups = []
    for size in sizes:
        groups.append(refs[:size])
        refs = refs[size:]
    first, groups = groups[0], groups[1:]
    ga = {name: Gather(axis, me, *group) for (name, axis), group in zip(GATHERS, groups)}
    groups = groups[len(GATHERS):]
    mv = {name: Move(way, me, *group) for (name, way), group in zip(MOVES, groups)}
    groups = groups[len(MOVES):]
    re = {name: Reduce(axis, me, *((first[9],) if name in WIDE else ()), *group)
          for (name, axis), group in zip(REDUCES, groups)}
    res = Output(n, me, *groups[-1])

    lines = [(None, 4, lambda k, axis=axis: dict(me, **{axis: k})) for axis in "xyz"]
    turns = [W_TURN, H_TURN, Y_TURN, YT_TURN]
    sources = lines + [(None, 1, lambda k, way=way: way[1](me)) for way in turns]
    dests = lines + [(None, 1, lambda k, way=way: way[0](me)) for way in turns]
    for plan in PLANS:
        cond, find = res.incoming(plan)
        sources.append((cond, 16, lambda i, find=find: find(i)[-1]))
        dests.append((None, 1, lambda k, plan=plan: res.to(plan)[0]))
    ct, d, g, dt = first[:4]
    late, ending = stage0(n, me, sources, dests, l_ref, *first)

    def ctr(r, c):
        slot = (r * (r - 1)) // 2 + c
        return jnp.concatenate([ct[slot, k] for k in range(4)], axis=0)

    def cols(array, r, c):
        return array.at[r, :, pl.ds(c * half, half)]

    for name, src in (("d0", d.at[0]), ("d2", d.at[2]), ("d1", d.at[1])):
        ga[name].start(src)

    def each(names, *steps):
        for step in steps:
            for name in names:
                step(name)

    def gathered(name):
        ga[name].relay()

    def ready(name):
        ga[name].wait()

    def begin(name):
        re[name].start()

    def passed(name):
        re[name].relay()

    def turned(name):
        mv[name].wait()
        ga[name].start(mv[name].buf)

    each(("d0", "d2"), gathered, ready)
    for name, pair, right in (("w0", (1, 0), "d0"), ("w1", (3, 2), "d2")):
        re[name].put(0, turn(ctr(*pair), ga[right].rows()))
    each(("w0", "w1"), begin, passed)
    for name in ("w0", "w1"):
        re[name].wait()
        ga[name].start(re[name].out.at[0])
    late()
    for name, src in (("dt", dt.at[0]), ("g1", g.at[1]), ("g3", g.at[3])):
        ga[name].start(src)
    for name in ("w1", "w0"):
        mv[name + "t"].start(re[name].out.at[0])
    each(("w0", "w1", "dt", "g1", "g3"), gathered)
    each(("w0", "w1", "dt", "g1", "g3"), ready)
    made = ("x21", "y1", "y0", "yt1")
    for name, left, right in zip(made, ("dt", "g3", "g1", "w1"), ("w0", "w1", "w0", "g3")):
        re[name].put(0, turn(ga[left].rows(), ga[right].rows()))
    each(made, begin)
    each(("w1t", "w0t"), turned)
    each(made, passed)
    for name in ("x21", "y1"):
        re[name].wait(-1)
        ga[name].start(re[name].out.at[0])
    for name in ("y0", "yt1"):
        re[name].wait(-1)
    for name in ("yt1", "y1"):
        mv[name + "t"].start(re[name].out.at[0])

    def half_h(name, left, right):
        re[name].put(0, turn(ga[left].rows(), ga[right].rows()))

    each(("x21", "y1", "w1t", "d1"), gathered)
    each(("y1", "w1t"), ready)
    half_h("h1", "w1t", "y1")
    each(("x21", "d1"), ready)
    zero, one = ga["d0"].rows(), jnp.concatenate([ga["x21"].rows(), ga["d1"].rows()], axis=1)
    for r in range(2):
        if r == 1:
            begin("h1")
        top = turn(ctr(2 + r, 1), one)
        re["w"].put(r, jnp.concatenate([top[:, :half] + turn(ctr(2 + r, 0), zero), top[:, half:]], axis=1))
    passed("h1")
    begin("w")
    ga["y0"].start(re["y0"].out.at[0])
    each(("yt1t", "y1t"), turned)
    passed("w")
    re["h1"].wait(-1, g[2:3])
    mv["g2t"].start(re["h1"].out.at[0])
    each(("w0t", "y0"), gathered, ready)
    half_h("h0", "w0t", "y0")
    turned("g2t")
    re["w"].wait()
    re["w"].swapped()
    ga["w"].start(re["w"].out)
    begin("h0")
    mv["wt"].start(re["w"].out)
    each(("yt1t", "y1t", "g2t"), gathered)
    each(("w",), gathered)
    each(("w", "g2t", "yt1t", "y1t"), ready)
    for r, names in enumerate((("g2t", "y1t"), ("yt1t", "g3"))):
        re["y"].put(r, sum(turn(ga[name].rows(), ga["w"].rows(c)) for c, name in enumerate(names)))
    begin("y")
    turned("wt")
    passed("y")
    passed("h0")
    re["h0"].wait(-1, g[0:1])
    ending()
    early = [*made, "w0", "w1", "h1", "h0"]
    for name in early:
        re[name].finish()
        re[name].swapped()
    for name in ga:
        if name not in ("w", "wt", "y"):
            ga[name].finish()
    re["y"].wait(-1)
    re["y"].swapped()
    ga["y"].start(re["y"].out)
    each(("y", "wt"), gathered, ready)
    for r in range(2):
        left = [ga["wt"].rows(c)[:, r * half:(r + 1) * half] for c in range(2)]
        re["h"].put(r, sum(turn(left[c], ga["y"].rows(c)) for c in range(2)))
    begin("h")
    res.start(g.at[1], 1, 1, "add", *ZYX)
    res.start(g.at[3], 3, 3, "keep", *ZYX)
    for name, r, keep in (("y0", 1, "add"), ("y1", 3, "keep")):
        for kind in (keep, "turn"):
            res.start(re[name].out.at[0], r, r - 1, kind, *YXZ)
    res.start(re["h0"].out.at[0], 0, 0, "add", *ZXY)
    res.start(re["h1"].out.at[0], 2, 2, "keep", *ZXY)
    passed("h")
    for r in range(2):
        for c in range(2):
            for kind in ("keep", "turn"):
                res.start(cols(re["y"].out, r, c), 2 + r, c, kind, *YXZ)
    re["h"].wait(-1)
    for r in range(2):
        for c in range(2):
            res.start(cols(re["h"].out, r, c), r, c, "keep", *ZXY)
    for part in [*mv.values(), *(ga[name] for name in ("w", "wt", "y")), re["w"], re["y"]]:
        part.finish()
    res.finish(out)
    re["h"].finish()
    re["h"].swapped()


def solution(mesh):
    def local_fn(l_blk):
        n = l_blk.shape[0] * 8
        groups = scratch_plan(n)
        spec = pl.BlockSpec(memory_space=pltpu.VMEM)
        call = pl.pallas_call(
            functools.partial(whole_kernel, n, [len(group) for group in groups]),
            out_shape=jax.ShapeDtypeStruct(l_blk.shape, F32),
            in_specs=[spec],
            out_specs=spec,
            scratch_shapes=sum(groups, []),
            compiler_params=pltpu.CompilerParams(
                has_side_effects=True, vmem_limit_bytes=VMEM_LIMIT, collective_id=0),
            name="whole",
        )
        return call(l_blk)

    spec = P(("batch", "row"), "col")
    return jax.shard_map(local_fn, mesh=mesh, in_specs=(spec,), out_specs=spec, check_vma=False)
```

```python
import functools

import jax
import jax.numpy as jnp
from jax import lax
from jax.experimental import pallas as pl
from jax.experimental.pallas import tpu as pltpu
from jax.sharding import PartitionSpec as P

MESH = pl.DeviceIdType.MESH
HIGHEST = lax.Precision.HIGHEST
F32 = jnp.float32
VMEM_LIMIT = 67043328
SIDE, PAIR, SUBLANES = 4, 2, 8


def coords():
    col = lax.axis_index("col")
    row = lax.axis_index("row")
    return {"x": row // 2, "y": col % SIDE, "z": col // 4, "e": row % 2}


def device(at):
    return (0, 4 * at["z"] + at["y"], 2 * at["x"] + at["e"])


def same(p, q):
    return (p["x"] == q["x"]) & (p["y"] == q["y"]) & (p["z"] == q["z"]) & (p["e"] == q["e"])


def mm(a, b, dims=((1,), (0,))):
    return lax.dot_general(a, b, (dims, ((), ())), precision=HIGHEST, preferred_element_type=F32)


def loop(count, body):
    def step(k, carry):
        body(k)
        return carry

    lax.fori_loop(0, count, step, jnp.int32(0))


def push(src, dst, send_sem, recv_sem, to, me):
    here = same(to, me)

    @pl.when(here)
    def _():
        dst[...] = src[...]

    @pl.when(jnp.logical_not(here))
    def _():
        pltpu.make_async_remote_copy(
            src_ref=src, dst_ref=dst, send_sem=send_sem, recv_sem=recv_sem, device_id=device(to), device_id_type=MESH
        ).start()


def sent(src, dst, send_sem, recv_sem, to, me):
    @pl.when(jnp.logical_not(same(to, me)))
    def _():
        pltpu.make_async_remote_copy(
            src_ref=src, dst_ref=dst, send_sem=send_sem, recv_sem=recv_sem, device_id=device(to), device_id_type=MESH
        ).wait_send()


def arrived(dst, send_sem, recv_sem, source, me):
    @pl.when(jnp.logical_not(same(source, me)))
    def _():
        pltpu.make_async_remote_copy(
            src_ref=dst, dst_ref=dst, send_sem=send_sem, recv_sem=recv_sem, device_id=device(source), device_id_type=MESH
        ).wait_recv()


def meet(sources, dests, me):
    barrier = pltpu.get_barrier_semaphore()

    def other(cond, at):
        apart = jnp.logical_not(same(at, me))
        return apart if cond is None else apart & cond

    total = jnp.int32(0)
    for cond, count, which in sources:
        def tell(k, which=which):
            @pl.when(other(None, which(k)))
            def _():
                pl.semaphore_signal(barrier, inc=1, device_id=device(which(k)), device_id_type=MESH)

        if cond is None:
            loop(count, tell)
        else:
            @pl.when(cond)
            def _(count=count, tell=tell):
                loop(count, tell)

    for cond, count, which in dests:
        def add(k, carry, cond=cond, which=which):
            return carry + other(cond, which(k)).astype(jnp.int32)

        total = lax.fori_loop(0, count, add, total)

    @pl.when(total > 0)
    def _():
        pl.semaphore_wait(barrier, total)


def remote(src, dst, send_sem, recv_sem, to):
    return pltpu.make_async_remote_copy(
        src_ref=src, dst_ref=dst, send_sem=send_sem, recv_sem=recv_sem, device_id=device(to), device_id_type=MESH)


def invert_block(left, corner, inv, base):
    half = 3 * base
    rows = lax.broadcasted_iota(jnp.int32, (base, base), 0)
    cols = lax.broadcasted_iota(jnp.int32, (base, base), 1)
    eye = rows == cols

    def block(i, j):
        if j < 3:
            return left[i * base:(i + 1) * base, j * base:(j + 1) * base]
        return corner[(i - 3) * base:(i - 2) * base, (j - 3) * base:(j - 2) * base]

    tri = [block(i, i) for i in range(6)]
    found = []
    for i in range(6):
        diag = jnp.sum(jnp.where(eye, tri[i], 0.0), axis=1, keepdims=True)
        found.append(jnp.where(eye, 1.0 / diag, 0.0))
    size = 1
    while size < base:
        below = ((rows // size) % 2 == 1) & (cols // size == rows // size - 1)
        half_way = [mm(jnp.where(below, tri[i], 0.0), found[i]) for i in range(6)]
        found = [found[i] - mm(found[i], half_way[i]) for i in range(6)]
        size = size * 2
    inv[...] = jnp.zeros(inv.shape, F32)
    for k in (0, 3):
        x0, x1, x2 = found[k:k + 3]
        x10 = -mm(x1, mm(block(k + 1, k), x0))
        x21 = -mm(x2, mm(block(k + 2, k + 1), x1))
        x20 = -mm(x2, mm(block(k + 2, k), x0) + mm(block(k + 2, k + 1), x10))
        for i, j, val in ((0, 0, x0), (1, 1, x1), (2, 2, x2), (1, 0, x10), (2, 1, x21), (2, 0, x20)):
            inv[(k + i) * base:(k + i + 1) * base, (k + j) * base:(k + j + 1) * base] = val
    low = mm(left[half:, :], inv[:half, :half])
    inv[half:, :half] = -mm(inv[half:, half:], low)


def stage0(n, me, sources, dests, l_ref, ct_out, d_out, g_out, dt_out,
           left, corner, cmat, inv_a, inv_b, inv_t, slab_d, slab_t, slab_g, lt_ref,
           ct_send, ct_recv, ab_send, ab_recv, c_send, c_recv, x_send, x_recv, t_send, t_recv):
    x, y, z, e = me["x"], me["y"], me["z"], me["e"]
    big = n // 8
    half = n // 16
    quarter = n // 32
    tile = n // 128
    sib = dict(me, e=1 - e)
    diag = x == z

    slot = (x * (x - 1)) // 2 + z
    def ct_args(i):
        g, k, h, ee = i // 16, i // 4 % SIDE, i // 2 % 2, i % 2
        rows = pl.ds(pl.multiple_of(quarter * ee + tile * g, SUBLANES), tile)
        src = lt_ref.at[rows, pl.ds(pl.multiple_of(half * h, half), half)]
        to = {"x": k, "y": y, "z": 2 * e + h, "e": ee}
        return src, ct_out.at[slot, g], ct_send.at[i], ct_recv.at[slot, g], to, me

    up, down = dict(me, y=(y + 1) % SIDE), dict(me, y=(y + 3) % SIDE)

    def at(b, along_y):
        b = jnp.int32(b)
        return {"x": b, "y": along_y, "z": b, "e": e}

    odd = x % 2

    def dest(kind, i):
        g, j = i // 4, i % SIDE
        if kind == 0:
            return {"x": j, "y": y, "z": g, "e": e}
        if kind == 1:
            return {"x": odd * g + (1 - odd) * j, "y": odd * j + (1 - odd) * g, "z": y, "e": e}
        return {"x": g, "y": j, "z": y, "e": e}

    def full(kind, i):
        return i % SIDE <= y if kind == 0 else i % SIDE >= y

    pairs = [(b_row, b_col) for b_row in range(SIDE) for b_col in range(b_row)]

    def ct_source(b_row, b_col):
        return {"x": jnp.int32(b_row), "y": y, "z": jnp.int32(b_col), "e": z // 2}

    def one(cond, where):
        return cond, 1, lambda k: where

    sources = sources + [one(None, ct_source(*pair)) for pair in pairs] + [one(diag, sib)]
    sources += [one(diag, up), one(diag, down)]
    sources += [(x <= y, 3, lambda b: at(b, y)), (None, 4, lambda b: at(b, z)), one(y >= z, at(1, z))]
    dests = dests + [(x > z, 16, lambda i: ct_args(i)[4]), one(diag, sib)]
    dests += [one(diag, up), one(diag, down)]
    dests += [(diag, 16, lambda i: dest(1, i))]
    for kind, cond in ((0, diag & (x < 3)), (2, diag & (x == 1))):
        dests += [(cond & full(kind, i), 1, lambda k, kind=kind, i=i: dest(kind, jnp.int32(i))) for i in range(16)]

    @pl.when(x > z)
    def _():
        lt_ref[...] = l_ref[...].T

    meet(sources, dests, me)

    place = (y + SIDE - 2 * e) % SIDE
    upper, under = left.at[pl.ds(0, half), :], left.at[pl.ds(half, half), :]

    def ab_copy(chunk, way, own):
        dst = (upper, under, corner)[chunk]
        src = l_ref.at[pl.ds(half * min(chunk, 1), half), :] if own else dst
        return remote(src, dst, ab_send.at[chunk + 3 * way], ab_recv.at[chunk], (up, down)[way])

    def ab_came(chunk):
        dst = (upper, under, corner)[chunk]
        remote(dst, dst, ab_send.at[chunk], ab_recv.at[chunk], up).wait_recv()

    ab_sends = [("001", "111", "101", "011"), ("211", "201", "000"), ("200",), ("110",)]

    def c_copy(part, chunk, way, own):
        rows = pl.ds(half * chunk, half)
        dst = cmat.at[part, rows, :]
        src = l_ref.at[rows, :] if own else dst
        return remote(src, dst, c_send.at[chunk + 2 * way], c_recv.at[2 * part + chunk], (up, down)[way])

    def c_came(part, chunk):
        c_copy(part, chunk, 0, 0).wait_recv()

    c_sends = [("0001", "0011", "0101", "0111"), ("1001", "1011", "1101", "1111"), ("1000", "1100"), ("0010", "0110")]

    for part in range(PAIR):
        @pl.when(diag & (place == part))
        def _(part=part):
            for code in ab_sends[part]:
                if int(code[2]):
                    ab_copy(*map(int, code)).start()

    @pl.when(x > z)
    def _():
        loop(64, lambda i: push(*ct_args(i)))

    def swap_args(k):
        mine = [inv_a, inv_b, cmat.at[0], cmat.at[1]][k]
        return mine, mine, x_send.at[k], x_recv.at[k], sib, me

    def swap_came(k):
        arrived(swap_args(k)[1], x_send.at[k], x_recv.at[k], sib, me)

    closing = []

    @pl.when(diag)
    def _():
        for part, order in enumerate(("2", "01", "201", "102")):
            @pl.when(place == part)
            def _(part=part, order=order):
                if part == 0:
                    left[...] = l_ref[...]
                elif part == 1:
                    corner[...] = l_ref[half:, :]
                for chunk in order:
                    ab_came(int(chunk))
                    if part > 0 and chunk == order[0]:
                        ab_copy(*map(int, ab_sends[part][-1])).start()

        for part in range(PAIR):
            @pl.when((e == 1) & (y == part))
            def _(part=part):
                for code in c_sends[part]:
                    c_copy(*map(int, code)).start()
                cmat[part] = l_ref[...]

        invert_block(left, corner, inv_t, n // 48)
        for part in range(PAIR):
            @pl.when((e == 1) & (y == part))
            def _(part=part):
                push(*swap_args(2 + part))

            @pl.when((e == 1) & (y == part + 2))
            def _(part=part):
                c_came(1 - part, 0)
                c_copy(*map(int, c_sends[part + 2][0])).start()

        for core, inv in ((0, inv_a), (1, inv_b)):
            @pl.when(e == core)
            def _(inv=inv):
                inv[...] = inv_t[...]

        lower, across = y >= 2, ((1,), (1,))
        first = pl.multiple_of((y % 2) * half + e * quarter, SUBLANES)
        mine = pl.ds(first, quarter)

        for core in range(PAIR):
            @pl.when(e == core)
            def _(core=core):
                push(*swap_args(core))
                swap_came(1 - core)

        @pl.when(jnp.logical_not(lower))
        def _():
            inv_t[...] = inv_a[...].T
            slab_t[:, :big] = inv_t[mine, :]
            slab_d[:, :big] = inv_a[mine, :]

        @pl.when(lower)
        def _():
            inv_t[...] = inv_b[...].T
            slab_t[:, big:] = inv_t[mine, :]
            slab_g[:, big:] = mm(slab_t[:, big:], inv_b[...])
            slab_d[:, big:] = inv_b[mine, :]

        @pl.when(e == 1)
        def _():
            for part in range(PAIR):
                @pl.when(y == part)
                def _(part=part):
                    c_came(1 - part, 0)
                    c_came(1 - part, 1)
                    push(*swap_args(3 - part))

                @pl.when(y == part + 2)
                def _(part=part):
                    c_came(1 - part, 1)
                    c_copy(*map(int, c_sends[part + 2][1])).start()
                    push(*swap_args(3 - part))
                    c_came(part, 0)
                    c_came(part, 1)
                    push(*swap_args(2 + part))

        @pl.when(e == 0)
        def _():
            swap_came(2)
            swap_came(3)

        def times_c(v):
            return jnp.concatenate([mm(v, cmat[0]), mm(v, cmat[1])], axis=1)

        def spread(kind, i):
            rows = pl.ds(pl.multiple_of(tile * (i // 4), SUBLANES), tile)
            src = (slab_d, slab_g, slab_t)[kind].at[rows, pl.ds(pl.multiple_of(half * (i % SIDE), half), half)]
            dst = (d_out, g_out)[kind].at[x] if kind < 2 else dt_out.at[0]
            recv = t_recv.at[kind, x] if kind < 2 else t_recv.at[2, 0]
            return src, dst, t_send.at[kind * 16 + i], recv, dest(kind, i), me

        def spread_all(use, kind):
            def step(i):
                if kind == 1:
                    use(*spread(kind, i))
                else:
                    @pl.when(full(kind, i))
                    def _():
                        use(*spread(kind, i))

            loop(16, step)

        @pl.when(lower)
        def _():
            slab_d[:, :big] = -mm(times_c(slab_d[:, big:]), inv_a[...])

        @pl.when(x < 3)
        def _():
            spread_all(push, 0)

        @pl.when(jnp.logical_not(lower))
        def _():
            w = mm(slab_t[:, :half], cmat[0], across) + mm(slab_t[:, half:big], cmat[1], across)
            slab_t[:, big:] = -mm(w, inv_b[...], across)

        @pl.when(x == 1)
        def _():
            spread_all(push, 2)

        @pl.when(jnp.logical_not(lower))
        def _():
            slab_g[:, big:] = mm(slab_t[:, big:], inv_b[...])
            slab_g[:, :big] = mm(slab_t[:, :big] - times_c(slab_g[:, big:]), inv_a[...])

        @pl.when(lower)
        def _():
            slab_g[:, :big] = -mm(times_c(slab_g[:, big:]), inv_a[...])

        spread_all(push, 1)

        def close():
            @pl.when(x < 3)
            def _():
                spread_all(sent, 0)

            @pl.when(x == 1)
            def _():
                spread_all(sent, 2)

            spread_all(sent, 1)
            for part in range(SIDE):
                @pl.when(place == part)
                def _(part=part):
                    for code in ab_sends[part]:
                        ab_copy(*map(int, code)).wait_send()

                @pl.when((e == 1) & (y == part))
                def _(part=part):
                    for code in c_sends[part]:
                        c_copy(*map(int, code)).wait_send()

            for core in range(PAIR):
                @pl.when(e == core)
                def _(core=core):
                    for k in (0,) if core == 0 else (1, 2, 3):
                        sent(*swap_args(k))

        closing.append(close)

    @pl.when(x <= y)
    def _():
        loop(3, lambda b: arrived(d_out.at[b], t_send.at[0], t_recv.at[0, b], at(b, y), me))

    @pl.when(x > y)
    def _():
        d_out[...] = jnp.zeros(d_out.shape, F32)

    for k, pair in enumerate(pairs):
        loop(SIDE, lambda g, k=k, pair=pair: arrived(ct_out.at[k, g], ct_send.at[0], ct_recv.at[k, g], ct_source(*pair), me))

    def late():
        loop(SIDE, lambda b: arrived(g_out.at[b], t_send.at[0], t_recv.at[1, b], at(b, z), me))

        @pl.when(y >= z)
        def _():
            arrived(dt_out.at[0], t_send.at[0], t_recv.at[2, 0], at(1, z), me)

        @pl.when(y < z)
        def _():
            dt_out[...] = jnp.zeros(dt_out.shape, F32)

    def finish():
        @pl.when(diag)
        def _():
            closing[0]()

        @pl.when(x > z)
        def _():
            loop(64, lambda i: sent(*ct_args(i)))

    return late, finish


def moved(turn, digit, back):
    def to(me):
        return {"x": (me["x"] + me[digit]) % SIDE, "y": me[turn[0]], "z": me[turn[1]], "e": me["e"]}

    def source(me):
        found = dict(me, x=me[back])
        found.update(zip(turn, (me["y"], me["z"])))
        found[digit] = (me["x"] + SIDE - me[back]) % SIDE
        return found

    return to, source, back


W_TURN = moved("zx", "y", "z")
H_TURN = moved("xz", "y", "y")
Y_TURN = moved("xy", "z", "y")
YT_TURN = moved("yx", "z", "z")


class Move:
    def __init__(self, way, me, buf, send, recv):
        (self.to, self.source, self.back), self.me, self.buf, self.send, self.recv = way, me, buf, send, recv

    def args(self):
        return self.src, self.buf, self.send.at[0], self.recv.at[0], self.to(self.me), self.me

    def start(self, src):
        self.src = src
        push(*self.args())

    def wait(self):
        arrived(self.buf, self.send.at[0], self.recv.at[0], self.source(self.me), self.me)

    def finish(self):
        sent(*self.args())


class Line:
    def __init__(self, axis, me):
        self.at = me[axis]
        self.up, self.across, self.down = ((self.at + k) % SIDE for k in (1, 2, 3))
        self.above, self.below = dict(me, **{axis: self.up}), dict(me, **{axis: self.down})


class Gather:
    def __init__(self, axis, me, buf, send, recv):
        self.line, self.buf, self.send, self.recv = Line(axis, me), buf, send, recv
        self.shift = None

    def piece(self, slot, half):
        if len(self.buf.shape) > 3:
            return self.buf.at[slot, pl.ds(half, 1)]
        rows = self.buf.shape[1] // 2
        return self.buf.at[slot, pl.ds(half * rows, rows)]

    def copies(self):
        line, buf = self.line, self.buf
        return [
            remote(self.src, buf.at[line.at], self.send.at[0], self.recv.at[0], line.above),
            remote(self.src, buf.at[line.at], self.send.at[1], self.recv.at[1], line.below),
            remote(self.piece(line.down, 0), self.piece(line.down, 0), self.send.at[2], self.recv.at[2], line.above),
            remote(self.piece(line.up, 1), self.piece(line.up, 1), self.send.at[3], self.recv.at[3], line.below)]

    def start(self, src):
        self.src = src
        for copy in self.copies()[:2]:
            copy.start()
        self.buf[self.line.at] = src[...]

    def relay(self):
        line, buf = self.line, self.buf
        onward = self.copies()[2:]
        remote(buf.at[line.down], buf.at[line.down], self.send.at[0], self.recv.at[0], line.below).wait_recv()
        onward[0].start()
        remote(buf.at[line.up], buf.at[line.up], self.send.at[1], self.recv.at[1], line.above).wait_recv()
        onward[1].start()

    def wait(self):
        for half, whom in ((0, self.line.below), (1, self.line.above)):
            piece = self.piece(self.line.across, half)
            remote(piece, piece, self.send.at[2 + half], self.recv.at[2 + half], whom).wait_recv()

    def finish(self):
        for copy in self.copies():
            copy.wait_send()

    def rows(self, block=None):
        places = [k if self.shift is None else (k + self.shift) % SIDE for k in range(SIDE)]
        tiles = [self.buf[k] if block is None else self.buf[k, block] for k in places]
        return jnp.concatenate(tiles, axis=0)


class Reduce:
    def __init__(self, axis, me, part, sib, half, land, out, s_send, s_recv, r_send, r_recv):
        self.line, self.me, self.part, self.sib, self.half, self.land, self.out = Line(axis, me), me, part, sib, half, land, out
        self.s_send, self.s_recv, self.send, self.recv = s_send, s_recv, r_send, r_recv
        self.other = dict(me, e=1 - me["e"])
        self.down, self.tile = out.shape[:2]

    def swap_args(self, d):
        rows = pl.ds(((1 - self.me["e"]) + 2 * d) * (SIDE * self.tile), SIDE * self.tile)
        return self.part.at[rows, :], self.sib.at[d], self.s_send.at[d], self.s_recv.at[d], self.other, self.me

    def put(self, d, value):
        self.part[d * 8 * self.tile:(d + 1) * 8 * self.tile, :] = value
        push(*self.swap_args(d))

    def where(self, k, half=None):
        first = pl.multiple_of(k * self.tile, SUBLANES)
        if half is None:
            return slice(None), pl.ds(first, self.tile)
        if self.down > 1:
            return pl.ds(half, 1), pl.ds(first, self.tile)
        rows = self.tile // 2
        return slice(None), pl.ds(pl.multiple_of(first + half * rows, SUBLANES), rows)

    def copies(self):
        line, sib = self.line, self.sib
        return [
            remote(sib.at[self.where(line.across, 0)], self.half.at[0], self.send.at[0], self.recv.at[0], line.above),
            remote(sib.at[self.where(line.across, 1)], self.half.at[1], self.send.at[1], self.recv.at[1], line.below),
            remote(sib.at[self.where(line.up)], self.land.at[0], self.send.at[2], self.recv.at[2], line.above),
            remote(sib.at[self.where(line.down)], self.land.at[1], self.send.at[3], self.recv.at[3], line.below)]

    def start(self):
        tile = self.tile
        for d in range(self.down):
            arrived(self.sib.at[d], self.s_send.at[d], self.s_recv.at[d], self.other, self.me)
            first = pl.multiple_of((self.me["e"] + 2 * d) * (4 * tile), SUBLANES)
            self.sib[d] = self.part[pl.ds(first, 4 * tile), :] + self.sib[d]
        for copy in self.copies()[:2]:
            copy.start()

    def relay(self):
        line, copies = self.line, self.copies()
        for half, whom, k in ((0, line.below, line.up), (1, line.above, line.down)):
            got = self.half.at[half]
            remote(got, got, self.send.at[half], self.recv.at[half], whom).wait_recv()
            at = self.where(k, half)
            self.sib[at] = self.sib[at] + self.half[half]
            copies[2 + half].start()

    def wait(self, sign=1, more=None):
        for side, whom in ((0, self.line.below), (1, self.line.above)):
            got = self.land.at[side]
            remote(got, got, self.send.at[2 + side], self.recv.at[2 + side], whom).wait_recv()
        total = (self.land[0] + self.land[1]) + self.sib[self.where(self.line.at)]
        total = total if sign > 0 else -total
        self.out[...] = total if more is None else total + more

    def swapped(self):
        for d in range(self.down):
            sent(*self.swap_args(d))

    def finish(self):
        for copy in self.copies():
            copy.wait_send()


def turn(a, b):
    return mm(a, b, ((0,), (0,)))


class Output:
    def __init__(self, n, me, flat, extra, turned, send, f_recv, a_recv, u_recv):
        self.half, self.tile, self.me, self.send = n // 16, n // 128, me, send
        self.into = {"keep": (flat, f_recv), "add": (extra, a_recv), "turn": (turned, u_recv)}
        self.started = []

    def place(self, kind, h, g, ee):
        buf, recv = self.into[kind]
        first = ee * (SIDE * self.tile) + g * self.tile
        if kind == "turn":
            cols = pl.ds(pl.multiple_of(h * self.half, self.half), self.half)
            return buf.at[pl.ds(pl.multiple_of(first, SUBLANES), self.tile), cols], recv.at[h, g, ee]
        return buf.at[pl.ds(pl.multiple_of(first + h * self.half, SUBLANES), self.tile), :], recv.at[h, g, ee]

    def to(self, plan):
        b_row, b_col, kind, rax, cax, gax = plan
        a_r, a_c = self.me[rax], self.me[cax]
        if kind == "turn":
            return {"x": jnp.int32(b_col), "y": a_r, "z": jnp.int32(b_row), "e": a_c // 2}, a_c % 2
        return {"x": jnp.int32(b_row), "y": a_c, "z": jnp.int32(b_col), "e": a_r // 2}, a_r % 2

    def args(self, index):
        plan, src = self.started[index]
        to, h = self.to(plan)
        dst, recv = self.place(plan[2], h, self.me[plan[5]], self.me["e"])
        return src, dst, self.send.at[index], recv, to, self.me

    def start(self, src, *plan):
        self.started.append((plan, src))
        push(*self.args(len(self.started) - 1))

    def incoming(self, plan):
        b_row, b_col, kind, rax, cax, gax = plan
        to_x, to_z = (b_col, b_row) if kind == "turn" else (b_row, b_col)
        y, e = self.me["y"], self.me["e"]

        def find(i):
            h, g, ee = i // 8, i // 2 % SIDE, i % 2
            a_r, a_c = (y, 2 * e + h) if kind == "turn" else (2 * e + h, y)
            return h, g, ee, {rax: a_r, cax: a_c, gax: g, "e": ee}

        return (self.me["x"] == to_x) & (self.me["z"] == to_z), find

    def finish(self, out):
        for plan, _ in self.started:
            cond, find = self.incoming(plan)

            @pl.when(cond)
            def _(plan=plan, find=find):
                def take(i):
                    h, g, ee, at = find(i)
                    dst, recv = self.place(plan[2], h, g, ee)
                    arrived(dst, self.send.at[0], recv, at, self.me)

                loop(16, take)

        kinds = {}
        for plan, _ in self.started:
            where = (plan[1], plan[0]) if plan[2] == "turn" else plan[:2]
            kinds.setdefault(where, set()).add(plan[2])
        for (b_row, b_col), has in kinds.items():
            @pl.when((self.me["x"] == b_row) & (self.me["z"] == b_col))
            def _(has=has):
                terms = [self.into[kind][0][...] for kind in ("keep", "add") if kind in has]
                if "turn" in has:
                    terms.append(self.into["turn"][0][...].T)
                out[...] = sum(terms[1:], terms[0])
        for index in range(len(self.started)):
            sent(*self.args(index))


ZXY, YXZ, ZYX = tuple("zxy"), tuple("yxz"), tuple("zyx")
PLANS = [(r, c, "keep", *ZXY) for r in range(PAIR) for c in range(PAIR)]
PLANS += [(2 + r, c, kind, *YXZ) for r in range(PAIR) for c in range(PAIR) for kind in ("keep", "turn")]
PLANS += [(0, 0, "add", *ZXY), (1, 1, "add", *ZYX), (2, 2, "keep", *ZXY), (3, 3, "keep", *ZYX)]
PLANS += [(r, r - 1, kind, *YXZ) for r, keep in ((1, "add"), (3, "keep")) for kind in (keep, "turn")]
WIDE = ("w", "wt", "y", "h")
GATHERS = [("d0", "z"), ("d1", "z"), ("d2", "z"), ("g1", "x"), ("dt", "x"), ("g3", "x"), ("w0", "y"), ("w1", "y"), ("y0", "z"),
           ("y1", "z"), ("x21", "z"), ("w0t", "x"), ("w1t", "x"), ("g2t", "x"), ("yt1t", "x"), ("y1t", "x"), ("w", "y"),
           ("wt", "x"), ("y", "z")]
MOVES = [("w0t", W_TURN), ("w1t", W_TURN), ("g2t", H_TURN), ("yt1t", YT_TURN), ("y1t", Y_TURN), ("wt", W_TURN)]
REDUCES = [("w0", "y"), ("w1", "y"), ("x21", "z"), ("y0", "z"), ("y1", "z"), ("yt1", "z"), ("h0", "y"), ("h1", "y"),
           ("w", "y"), ("y", "z"), ("h", "y")]


def scratch_plan(n):
    big, half, quarter, tile = n // 8, n // 16, n // 32, n // 128
    dma, vmem = pltpu.SemaphoreType.DMA, lambda *shape: pltpu.VMEM(shape, F32)
    pairs, four = 6, 4
    groups = [[vmem(pairs, four, tile, half), vmem(four, tile, half), vmem(four, tile, half), vmem(1, tile, half),
               vmem(big, half), vmem(half, half), vmem(2, big, half)]
              + [vmem(big, big)] * 3 + [vmem(quarter, 2 * big)] * 3 + [vmem(half, big)]
              + [dma((64,)), dma((pairs, four)), dma((6,)), dma((3,)), dma((four,)), dma((four,)), dma((four,)), dma((four,)),
                 dma((48,)), dma((3, four))]]
    for name, _ in GATHERS:
        wide = name in WIDE
        shape = (2, tile, 2 * half) if wide else (tile, half)
        groups.append([vmem(four, *shape), dma((four,)), dma((four,))])
    for name, _ in MOVES:
        wide = name in WIDE
        groups.append([vmem(2, tile, 2 * half) if wide else vmem(tile, half), dma((1,)), dma((1,))])
    for name, _ in REDUCES:
        wide = name in WIDE
        down, width = (2, 2 * half) if wide else (1, half)
        part = [] if wide else [vmem(half, width)]
        piece = vmem(2, 1, tile if wide else tile // 2, width)
        groups.append(part + [vmem(down, quarter, width), piece, vmem(2, down, tile, width), vmem(down, tile, width),
                       dma((down,)), dma((down,)), dma((four,)), dma((four,))])
    hubs = dma((2, four, 2))
    groups.append([vmem(big, half), vmem(big, half), vmem(half, big), dma((len(PLANS),)), hubs, hubs, hubs])
    return groups


def whole_kernel(n, sizes, l_ref, out, *refs):
    half = n // 16
    me = coords()
    groups = []
    for size in sizes:
        groups.append(refs[:size])
        refs = refs[size:]
    first, groups = groups[0], groups[1:]
    ga = {name: Gather(axis, me, *group) for (name, axis), group in zip(GATHERS, groups)}
    groups = groups[len(GATHERS):]
    mv = {name: Move(way, me, *group) for (name, way), group in zip(MOVES, groups)}
    groups = groups[len(MOVES):]
    re = {name: Reduce(axis, me, *((first[9],) if name in WIDE else ()), *group)
          for (name, axis), group in zip(REDUCES, groups)}
    res = Output(n, me, *groups[-1])

    lines = [(None, 4, lambda k, axis=axis: dict(me, **{axis: k})) for axis in "xyz"]
    turns = [W_TURN, H_TURN, Y_TURN, YT_TURN]
    sources = lines + [(None, 1, lambda k, way=way: way[1](me)) for way in turns]
    dests = lines + [(None, 1, lambda k, way=way: way[0](me)) for way in turns]
    for plan in PLANS:
        cond, find = res.incoming(plan)
        sources.append((cond, 16, lambda i, find=find: find(i)[-1]))
        dests.append((None, 1, lambda k, plan=plan: res.to(plan)[0]))
    ct, d, g, dt = first[:4]
    late, ending = stage0(n, me, sources, dests, l_ref, *first)

    def ctr(r, c):
        slot = (r * (r - 1)) // 2 + c
        return jnp.concatenate([ct[slot, k] for k in range(SIDE)], axis=0)

    def cols(array, r, c):
        return array.at[r, :, pl.ds(c * half, half)]

    for name, src in (("d0", d.at[0]), ("d2", d.at[2]), ("d1", d.at[1])):
        ga[name].start(src)

    def each(names, *steps):
        for step in steps:
            for name in names:
                step(name)

    def gathered(name):
        ga[name].relay()

    def ready(name):
        ga[name].wait()

    def begin(name):
        re[name].start()

    def passed(name):
        re[name].relay()

    def turned(name):
        mv[name].wait()
        ga[name].shift = me[mv[name].back]
        ga[name].start(mv[name].buf)

    each(("d0", "d2"), gathered, ready)
    for name, pair, right in (("w0", (1, 0), "d0"), ("w1", (3, 2), "d2")):
        re[name].put(0, turn(ctr(*pair), ga[right].rows()))
    each(("w0", "w1"), begin, passed)
    late()
    for name, src in (("dt", dt.at[0]), ("g3", g.at[3]), ("g1", g.at[1])):
        ga[name].start(src)
    for name in ("w0", "w1"):
        re[name].wait()
        ga[name].start(re[name].out.at[0])
    for name in ("w1", "w0"):
        mv[name + "t"].start(re[name].out.at[0])
    each(("w0", "w1", "dt", "g3", "g1"), gathered)
    each(("w0", "w1", "dt", "g1", "g3"), ready)
    made = ("x21", "y1", "y0", "yt1")
    for name, left, right in zip(made, ("dt", "g3", "g1", "w1"), ("w0", "w1", "w0", "g3")):
        re[name].put(0, turn(ga[left].rows(), ga[right].rows()))
    each(made, begin)
    each(("w1t", "w0t"), turned)
    each(made, passed)
    for name in ("x21", "y1"):
        re[name].wait(-1)
        ga[name].start(re[name].out.at[0])

    def half_h(name, left, right):
        re[name].put(0, turn(ga[left].rows(), ga[right].rows()))

    each(("x21", "y1", "w1t", "d1"), gathered)
    each(("y1", "w1t"), ready)
    half_h("h1", "w1t", "y1")
    each(("x21", "d1"), ready)
    res.start(g.at[1], 1, 1, "add", *ZYX)
    res.start(g.at[3], 3, 3, "keep", *ZYX)
    for kind in ("keep", "turn"):
        res.start(re["y1"].out.at[0], 3, 2, kind, *YXZ)
    zero, one = ga["d0"].rows(), jnp.concatenate([ga["x21"].rows(), ga["d1"].rows()], axis=1)
    for r in range(PAIR):
        if r == 1:
            begin("h1")
        top = turn(ctr(2 + r, 1), one)
        re["w"].put(r, jnp.concatenate([top[:, :half] + turn(ctr(2 + r, 0), zero), top[:, half:]], axis=1))
    passed("h1")
    begin("w")
    for name in ("y0", "yt1"):
        re[name].wait(-1)
    ga["y0"].start(re["y0"].out.at[0])
    for name in ("yt1", "y1"):
        mv[name + "t"].start(re[name].out.at[0])
    passed("w")
    re["h1"].wait(-1, g[2:3])
    mv["g2t"].start(re["h1"].out.at[0])
    each(("yt1t", "y1t"), turned)
    each(("w0t", "y0"), gathered)
    turned("g2t")
    re["w"].wait()
    re["w"].swapped()
    ga["w"].start(re["w"].out)
    each(("yt1t", "y1t", "g2t"), gathered)
    each(("w",), gathered)
    each(("w", "g2t", "yt1t", "y1t"), ready)
    mv["wt"].start(re["w"].out)
    for r, names in enumerate((("g2t", "y1t"), ("yt1t", "g3"))):
        re["y"].put(r, sum(turn(ga[name].rows(), ga["w"].rows(c)) for c, name in enumerate(names)))
    for kind in ("add", "turn"):
        res.start(re["y0"].out.at[0], 1, 0, kind, *YXZ)
    res.start(re["h1"].out.at[0], 2, 2, "keep", *ZXY)
    begin("y")
    each(("w0t", "y0"), ready)
    half_h("h0", "w0t", "y0")
    passed("y")
    begin("h0")
    re["y"].wait(-1)
    re["y"].swapped()
    ga["y"].start(re["y"].out)
    passed("h0")
    turned("wt")
    each(("y", "wt"), gathered, ready)
    for r in range(PAIR):
        for c in range(PAIR):
            for kind in ("keep", "turn"):
                res.start(cols(re["y"].out, r, c), 2 + r, c, kind, *YXZ)
    for r in range(PAIR):
        left = [ga["wt"].rows(c)[:, r * half:(r + 1) * half] for c in range(PAIR)]
        re["h"].put(r, sum(turn(left[c], ga["y"].rows(c)) for c in range(PAIR)))
    begin("h")
    re["h0"].wait(-1, g[0:1])
    res.start(re["h0"].out.at[0], 0, 0, "add", *ZXY)
    passed("h")
    ending()
    for name in (*made, "w0", "w1", "h1", "h0"):
        re[name].finish()
        re[name].swapped()
    for name in ga:
        if name not in ("w", "wt", "y"):
            ga[name].finish()
    re["h"].wait(-1)
    for r in range(PAIR):
        for c in range(PAIR):
            res.start(cols(re["h"].out, r, c), r, c, "keep", *ZXY)
    for part in [*mv.values(), *(ga[name] for name in ("w", "wt", "y")), re["w"], re["y"]]:
        part.finish()
    res.finish(out)
    re["h"].finish()
    re["h"].swapped()


def solution(mesh):
    def local_fn(l_blk):
        n = l_blk.shape[0] * 8
        groups = scratch_plan(n)
        spec = pl.BlockSpec(memory_space=pltpu.VMEM)
        call = pl.pallas_call(
            functools.partial(whole_kernel, n, [len(group) for group in groups]),
            out_shape=jax.ShapeDtypeStruct(l_blk.shape, F32),
            in_specs=[spec],
            out_specs=spec,
            scratch_shapes=sum(groups, []),
            compiler_params=pltpu.CompilerParams(
                has_side_effects=True, vmem_limit_bytes=VMEM_LIMIT, collective_id=0),
            name="whole",
        )
        return call(l_blk)

    spec = P(("batch", "row"), "col")
    return jax.shard_map(local_fn, mesh=mesh, in_specs=(spec,), out_specs=spec, check_vma=False)
```

```python
import functools

import jax
import jax.numpy as jnp
from jax import lax
from jax.experimental import pallas as pl
from jax.experimental.pallas import tpu as pltpu
from jax.sharding import PartitionSpec as P

MESH = pl.DeviceIdType.MESH
HIGHEST = lax.Precision.HIGHEST
F32 = jnp.float32
VMEM_LIMIT = 67043328
SIDE, PAIR, SUBLANES = 4, 2, 8


def coords():
    col = lax.axis_index("col")
    row = lax.axis_index("row")
    return {"x": row // 2, "y": col % SIDE, "z": col // 4, "e": row % 2}


def device(at):
    return (0, 4 * at["z"] + at["y"], 2 * at["x"] + at["e"])


def same(p, q):
    return (p["x"] == q["x"]) & (p["y"] == q["y"]) & (p["z"] == q["z"]) & (p["e"] == q["e"])


def mm(a, b, dims=((1,), (0,))):
    return lax.dot_general(a, b, (dims, ((), ())), precision=HIGHEST, preferred_element_type=F32)


def loop(count, body):
    def step(k, carry):
        body(k)
        return carry

    lax.fori_loop(0, count, step, jnp.int32(0))


def push(src, dst, send_sem, recv_sem, to, me):
    here = same(to, me)

    @pl.when(here)
    def _():
        dst[...] = src[...]

    @pl.when(jnp.logical_not(here))
    def _():
        pltpu.make_async_remote_copy(
            src_ref=src, dst_ref=dst, send_sem=send_sem, recv_sem=recv_sem, device_id=device(to), device_id_type=MESH
        ).start()


def sent(src, dst, send_sem, recv_sem, to, me):
    @pl.when(jnp.logical_not(same(to, me)))
    def _():
        pltpu.make_async_remote_copy(
            src_ref=src, dst_ref=dst, send_sem=send_sem, recv_sem=recv_sem, device_id=device(to), device_id_type=MESH
        ).wait_send()


def arrived(dst, send_sem, recv_sem, source, me):
    @pl.when(jnp.logical_not(same(source, me)))
    def _():
        pltpu.make_async_remote_copy(
            src_ref=dst, dst_ref=dst, send_sem=send_sem, recv_sem=recv_sem, device_id=device(source), device_id_type=MESH
        ).wait_recv()


def meet(sources, dests, me):
    barrier = pltpu.get_barrier_semaphore()

    def other(cond, at):
        apart = jnp.logical_not(same(at, me))
        return apart if cond is None else apart & cond

    total = jnp.int32(0)
    for cond, count, which in sources:
        def tell(k, which=which):
            @pl.when(other(None, which(k)))
            def _():
                pl.semaphore_signal(barrier, inc=1, device_id=device(which(k)), device_id_type=MESH)

        if cond is None:
            loop(count, tell)
        else:
            @pl.when(cond)
            def _(count=count, tell=tell):
                loop(count, tell)

    for cond, count, which in dests:
        def add(k, carry, cond=cond, which=which):
            return carry + other(cond, which(k)).astype(jnp.int32)

        total = lax.fori_loop(0, count, add, total)

    @pl.when(total > 0)
    def _():
        pl.semaphore_wait(barrier, total)


def remote(src, dst, send_sem, recv_sem, to):
    return pltpu.make_async_remote_copy(
        src_ref=src, dst_ref=dst, send_sem=send_sem, recv_sem=recv_sem, device_id=device(to), device_id_type=MESH)


def invert_block(left, corner, inv, base):
    half = 3 * base
    rows = lax.broadcasted_iota(jnp.int32, (base, base), 0)
    cols = lax.broadcasted_iota(jnp.int32, (base, base), 1)
    eye = rows == cols

    def block(i, j):
        if j < 3:
            return left[i * base:(i + 1) * base, j * base:(j + 1) * base]
        return corner[(i - 3) * base:(i - 2) * base, (j - 3) * base:(j - 2) * base]

    tri = [block(i, i) for i in range(6)]
    found = []
    for i in range(6):
        diag = jnp.sum(jnp.where(eye, tri[i], 0.0), axis=1, keepdims=True)
        found.append(jnp.where(eye, 1.0 / diag, 0.0))
    size = 1
    while size < base:
        below = ((rows // size) % 2 == 1) & (cols // size == rows // size - 1)
        half_way = [mm(jnp.where(below, tri[i], 0.0), found[i]) for i in range(6)]
        found = [found[i] - mm(found[i], half_way[i]) for i in range(6)]
        size = size * 2
    inv[...] = jnp.zeros(inv.shape, F32)
    for k in (0, 3):
        x0, x1, x2 = found[k:k + 3]
        x10 = -mm(x1, mm(block(k + 1, k), x0))
        x21 = -mm(x2, mm(block(k + 2, k + 1), x1))
        x20 = -mm(x2, mm(block(k + 2, k), x0) + mm(block(k + 2, k + 1), x10))
        for i, j, val in ((0, 0, x0), (1, 1, x1), (2, 2, x2), (1, 0, x10), (2, 1, x21), (2, 0, x20)):
            inv[(k + i) * base:(k + i + 1) * base, (k + j) * base:(k + j + 1) * base] = val
    low = mm(left[half:, :], inv[:half, :half])
    inv[half:, :half] = -mm(inv[half:, half:], low)


def stage0(n, me, sources, dests, l_ref, lt_ref, ct_out, d_out, g_out, dt_out,
           left, corner, cmat, inv_a, inv_b, inv_t, slab_d, slab_t, slab_g,
           ct_send, ct_recv, ab_send, ab_recv, c_send, c_recv, x_send, x_recv, t_send, t_recv):
    x, y, z, e = me["x"], me["y"], me["z"], me["e"]
    big = n // 8
    half = n // 16
    quarter = n // 32
    tile = n // 128
    sib = dict(me, e=1 - e)
    diag = x == z

    slot = (x * (x - 1)) // 2 + z
    def ct_args(i):
        g, k, h, ee = i // 16, i // 4 % SIDE, i // 2 % 2, i % 2
        rows = pl.ds(pl.multiple_of(quarter * ee + tile * g, SUBLANES), tile)
        src = lt_ref.at[rows, pl.ds(pl.multiple_of(half * h, half), half)]
        to = {"x": k, "y": y, "z": 2 * e + h, "e": ee}
        return src, ct_out.at[slot, g], ct_send.at[i], ct_recv.at[slot, g], to, me

    up, down = dict(me, y=(y + 1) % SIDE), dict(me, y=(y + 3) % SIDE)

    def at(b, along_y):
        b = jnp.int32(b)
        return {"x": b, "y": along_y, "z": b, "e": e}

    odd = x % 2

    def dest(kind, i):
        g, j = i // 4, i % SIDE
        if kind == 0:
            return {"x": j, "y": y, "z": g, "e": e}
        if kind == 1:
            return {"x": odd * g + (1 - odd) * j, "y": odd * j + (1 - odd) * g, "z": y, "e": e}
        return {"x": g, "y": j, "z": y, "e": e}

    def full(kind, i):
        return i % SIDE <= y if kind == 0 else i % SIDE >= y

    pairs = [(b_row, b_col) for b_row in range(SIDE) for b_col in range(b_row)]

    def ct_source(b_row, b_col):
        return {"x": jnp.int32(b_row), "y": y, "z": jnp.int32(b_col), "e": z // 2}

    def one(cond, where):
        return cond, 1, lambda k: where

    sources = sources + [one(None, ct_source(*pair)) for pair in pairs] + [one(diag, sib)]
    sources += [one(diag, up), one(diag, down)]
    sources += [(x <= y, 3, lambda b: at(b, y)), (None, 4, lambda b: at(b, z)), one(y >= z, at(1, z))]
    dests = dests + [(x > z, 16, lambda i: ct_args(i)[4]), one(diag, sib)]
    dests += [one(diag, up), one(diag, down)]
    dests += [(diag, 16, lambda i: dest(1, i))]
    for kind, cond in ((0, diag & (x < 3)), (2, diag & (x == 1))):
        dests += [(cond & full(kind, i), 1, lambda k, kind=kind, i=i: dest(kind, jnp.int32(i))) for i in range(16)]

    @pl.when(x > z)
    def _():
        lt_ref[...] = l_ref[...].T

    meet(sources, dests, me)

    place = (y + SIDE - 2 * e) % SIDE
    upper, under = left.at[pl.ds(0, half), :], left.at[pl.ds(half, half), :]

    def ab_copy(chunk, way, own):
        dst = (upper, under, corner)[chunk]
        src = l_ref.at[pl.ds(half * min(chunk, 1), half), :] if own else dst
        return remote(src, dst, ab_send.at[chunk + 3 * way], ab_recv.at[chunk], (up, down)[way])

    def ab_came(chunk):
        dst = (upper, under, corner)[chunk]
        remote(dst, dst, ab_send.at[chunk], ab_recv.at[chunk], up).wait_recv()

    ab_sends = [("001", "111", "101", "011"), ("211", "201", "000"), ("200",), ("110",)]

    def c_copy(part, chunk, way, own):
        rows = pl.ds(half * chunk, half)
        dst = cmat.at[part, rows, :]
        src = l_ref.at[rows, :] if own else dst
        return remote(src, dst, c_send.at[chunk + 2 * way], c_recv.at[2 * part + chunk], (up, down)[way])

    def c_came(part, chunk):
        c_copy(part, chunk, 0, 0).wait_recv()

    c_sends = [("0001", "0011", "0101", "0111"), ("1001", "1011", "1101", "1111"), ("1000", "1100"), ("0010", "0110")]

    for part in range(PAIR):
        @pl.when(diag & (place == part))
        def _(part=part):
            for code in ab_sends[part]:
                if int(code[2]):
                    ab_copy(*map(int, code)).start()

    @pl.when(x > z)
    def _():
        loop(64, lambda i: push(*ct_args(i)))

    def swap_args(k):
        mine = [inv_a, inv_b, cmat.at[0], cmat.at[1]][k]
        return mine, mine, x_send.at[k], x_recv.at[k], sib, me

    def swap_came(k):
        arrived(swap_args(k)[1], x_send.at[k], x_recv.at[k], sib, me)

    closing = []

    @pl.when(diag)
    def _():
        for part, order in enumerate(("2", "01", "201", "102")):
            @pl.when(place == part)
            def _(part=part, order=order):
                if part == 0:
                    left[...] = l_ref[...]
                elif part == 1:
                    corner[...] = l_ref[half:, :]
                for chunk in order:
                    ab_came(int(chunk))
                    if part > 0 and chunk == order[0]:
                        ab_copy(*map(int, ab_sends[part][-1])).start()

        for part in range(PAIR):
            @pl.when((e == 1) & (y == part))
            def _(part=part):
                for code in c_sends[part]:
                    c_copy(*map(int, code)).start()
                cmat[part] = l_ref[...]

        invert_block(left, corner, inv_t, n // 48)
        for part in range(PAIR):
            @pl.when((e == 1) & (y == part))
            def _(part=part):
                push(*swap_args(2 + part))

            @pl.when((e == 1) & (y == part + 2))
            def _(part=part):
                c_came(1 - part, 0)
                c_copy(*map(int, c_sends[part + 2][0])).start()

        for core, inv in ((0, inv_a), (1, inv_b)):
            @pl.when(e == core)
            def _(inv=inv):
                inv[...] = inv_t[...]

        lower, across = y >= 2, ((1,), (1,))
        first = pl.multiple_of((y % 2) * half + e * quarter, SUBLANES)
        mine = pl.ds(first, quarter)

        for core in range(PAIR):
            @pl.when(e == core)
            def _(core=core):
                push(*swap_args(core))
                swap_came(1 - core)

        @pl.when(jnp.logical_not(lower))
        def _():
            inv_t[...] = inv_a[...].T
            slab_t[:, :big] = inv_t[mine, :]
            slab_d[:, :big] = inv_a[mine, :]

        @pl.when(lower)
        def _():
            inv_t[...] = inv_b[...].T
            slab_t[:, big:] = inv_t[mine, :]
            slab_g[:, big:] = mm(slab_t[:, big:], inv_b[...])
            slab_d[:, big:] = inv_b[mine, :]

        @pl.when(e == 1)
        def _():
            for part in range(PAIR):
                @pl.when(y == part)
                def _(part=part):
                    c_came(1 - part, 0)
                    c_came(1 - part, 1)
                    push(*swap_args(3 - part))

                @pl.when(y == part + 2)
                def _(part=part):
                    c_came(1 - part, 1)
                    c_copy(*map(int, c_sends[part + 2][1])).start()
                    push(*swap_args(3 - part))
                    c_came(part, 0)
                    c_came(part, 1)
                    push(*swap_args(2 + part))

        @pl.when(e == 0)
        def _():
            swap_came(2)
            swap_came(3)

        def times_c(v):
            return jnp.concatenate([mm(v, cmat[0]), mm(v, cmat[1])], axis=1)

        def spread(kind, i):
            rows = pl.ds(pl.multiple_of(tile * (i // 4), SUBLANES), tile)
            src = (slab_d, slab_g, slab_t)[kind].at[rows, pl.ds(pl.multiple_of(half * (i % SIDE), half), half)]
            dst = (d_out, g_out)[kind].at[x] if kind < 2 else dt_out.at[0]
            recv = t_recv.at[kind, x] if kind < 2 else t_recv.at[2, 0]
            return src, dst, t_send.at[kind * 16 + i], recv, dest(kind, i), me

        def spread_all(use, kind):
            def step(i):
                if kind == 1:
                    use(*spread(kind, i))
                else:
                    @pl.when(full(kind, i))
                    def _():
                        use(*spread(kind, i))

            loop(16, step)

        @pl.when(lower)
        def _():
            slab_d[:, :big] = -mm(times_c(slab_d[:, big:]), inv_a[...])

        @pl.when(x < 3)
        def _():
            spread_all(push, 0)

        @pl.when(jnp.logical_not(lower))
        def _():
            w = mm(slab_t[:, :half], cmat[0], across) + mm(slab_t[:, half:big], cmat[1], across)
            slab_t[:, big:] = -mm(w, inv_b[...], across)

        @pl.when(x == 1)
        def _():
            spread_all(push, 2)

        @pl.when(jnp.logical_not(lower))
        def _():
            slab_g[:, big:] = mm(slab_t[:, big:], inv_b[...])
            slab_g[:, :big] = mm(slab_t[:, :big] - times_c(slab_g[:, big:]), inv_a[...])

        @pl.when(lower)
        def _():
            slab_g[:, :big] = -mm(times_c(slab_g[:, big:]), inv_a[...])

        spread_all(push, 1)

        def close():
            @pl.when(x < 3)
            def _():
                spread_all(sent, 0)

            @pl.when(x == 1)
            def _():
                spread_all(sent, 2)

            spread_all(sent, 1)
            for part in range(SIDE):
                @pl.when(place == part)
                def _(part=part):
                    for code in ab_sends[part]:
                        ab_copy(*map(int, code)).wait_send()

                @pl.when((e == 1) & (y == part))
                def _(part=part):
                    for code in c_sends[part]:
                        c_copy(*map(int, code)).wait_send()

            for core in range(PAIR):
                @pl.when(e == core)
                def _(core=core):
                    for k in (0,) if core == 0 else (1, 2, 3):
                        sent(*swap_args(k))

        closing.append(close)

    @pl.when(x <= y)
    def _():
        loop(3, lambda b: arrived(d_out.at[b], t_send.at[0], t_recv.at[0, b], at(b, y), me))

    @pl.when(x > y)
    def _():
        d_out[...] = jnp.zeros(d_out.shape, F32)

    for k, pair in enumerate(pairs):
        loop(SIDE, lambda g, k=k, pair=pair: arrived(ct_out.at[k, g], ct_send.at[0], ct_recv.at[k, g], ct_source(*pair), me))

    def late():
        loop(SIDE, lambda b: arrived(g_out.at[b], t_send.at[0], t_recv.at[1, b], at(b, z), me))

        @pl.when(y >= z)
        def _():
            arrived(dt_out.at[0], t_send.at[0], t_recv.at[2, 0], at(1, z), me)

        @pl.when(y < z)
        def _():
            dt_out[...] = jnp.zeros(dt_out.shape, F32)

    def finish():
        @pl.when(diag)
        def _():
            closing[0]()

        @pl.when(x > z)
        def _():
            loop(64, lambda i: sent(*ct_args(i)))

    return late, finish


def moved(turn, digit, back):
    def to(me):
        return {"x": (me["x"] + me[digit]) % SIDE, "y": me[turn[0]], "z": me[turn[1]], "e": me["e"]}

    def source(me):
        found = dict(me, x=me[back])
        found.update(zip(turn, (me["y"], me["z"])))
        found[digit] = (me["x"] + SIDE - me[back]) % SIDE
        return found

    return to, source, back


W_TURN = moved("zx", "y", "z")
H_TURN = moved("xz", "y", "y")
Y_TURN = moved("xy", "z", "y")
YT_TURN = moved("yx", "z", "z")


class Move:
    def __init__(self, way, me, buf, send, recv):
        (self.to, self.source, self.back), self.me, self.buf, self.send, self.recv = way, me, buf, send, recv

    def args(self):
        return self.src, self.buf, self.send.at[0], self.recv.at[0], self.to(self.me), self.me

    def start(self, src):
        self.src = src
        push(*self.args())

    def wait(self):
        arrived(self.buf, self.send.at[0], self.recv.at[0], self.source(self.me), self.me)

    def finish(self):
        sent(*self.args())


class Line:
    def __init__(self, axis, me):
        self.at = me[axis]
        self.up, self.across, self.down = ((self.at + k) % SIDE for k in (1, 2, 3))
        self.above, self.below = dict(me, **{axis: self.up}), dict(me, **{axis: self.down})


class Gather:
    def __init__(self, axis, me, buf, send, recv):
        self.line, self.buf, self.send, self.recv = Line(axis, me), buf, send, recv
        self.shift = None

    def piece(self, slot, half):
        if len(self.buf.shape) > 3:
            return self.buf.at[slot, pl.ds(half, 1)]
        rows = self.buf.shape[1] // 2
        return self.buf.at[slot, pl.ds(half * rows, rows)]

    def copies(self):
        line, buf = self.line, self.buf
        return [
            remote(self.src, buf.at[line.at], self.send.at[0], self.recv.at[0], line.above),
            remote(self.src, buf.at[line.at], self.send.at[1], self.recv.at[1], line.below),
            remote(self.piece(line.down, 0), self.piece(line.down, 0), self.send.at[2], self.recv.at[2], line.above),
            remote(self.piece(line.up, 1), self.piece(line.up, 1), self.send.at[3], self.recv.at[3], line.below)]

    def start(self, src):
        self.src = src
        for copy in self.copies()[:2]:
            copy.start()
        self.buf[self.line.at] = src[...]

    def relay(self):
        line, buf = self.line, self.buf
        onward = self.copies()[2:]
        remote(buf.at[line.down], buf.at[line.down], self.send.at[0], self.recv.at[0], line.below).wait_recv()
        onward[0].start()
        remote(buf.at[line.up], buf.at[line.up], self.send.at[1], self.recv.at[1], line.above).wait_recv()
        onward[1].start()

    def wait(self):
        for half, whom in ((0, self.line.below), (1, self.line.above)):
            piece = self.piece(self.line.across, half)
            remote(piece, piece, self.send.at[2 + half], self.recv.at[2 + half], whom).wait_recv()

    def finish(self):
        for copy in self.copies():
            copy.wait_send()

    def rows(self, block=None):
        places = [k if self.shift is None else (k + self.shift) % SIDE for k in range(SIDE)]
        tiles = [self.buf[k] if block is None else self.buf[k, block] for k in places]
        return jnp.concatenate(tiles, axis=0)


class Reduce:
    def __init__(self, axis, me, part, sib, half, land, out, s_send, s_recv, r_send, r_recv):
        self.line, self.me, self.part, self.sib, self.half, self.land, self.out = Line(axis, me), me, part, sib, half, land, out
        self.s_send, self.s_recv, self.send, self.recv = s_send, s_recv, r_send, r_recv
        self.other = dict(me, e=1 - me["e"])
        self.down, self.tile = out.shape[:2]

    def swap_args(self, d):
        rows = pl.ds(((1 - self.me["e"]) + 2 * d) * (SIDE * self.tile), SIDE * self.tile)
        return self.part.at[rows, :], self.sib.at[d], self.s_send.at[d], self.s_recv.at[d], self.other, self.me

    def put(self, d, value):
        self.part[d * 8 * self.tile:(d + 1) * 8 * self.tile, :] = value
        push(*self.swap_args(d))

    def where(self, k, half=None):
        first = pl.multiple_of(k * self.tile, SUBLANES)
        if half is None:
            return slice(None), pl.ds(first, self.tile)
        if self.down > 1:
            return pl.ds(half, 1), pl.ds(first, self.tile)
        rows = self.tile // 2
        return slice(None), pl.ds(pl.multiple_of(first + half * rows, SUBLANES), rows)

    def copies(self):
        line, sib = self.line, self.sib
        return [
            remote(sib.at[self.where(line.across, 0)], self.half.at[0], self.send.at[0], self.recv.at[0], line.above),
            remote(sib.at[self.where(line.across, 1)], self.half.at[1], self.send.at[1], self.recv.at[1], line.below),
            remote(sib.at[self.where(line.up)], self.land.at[0], self.send.at[2], self.recv.at[2], line.above),
            remote(sib.at[self.where(line.down)], self.land.at[1], self.send.at[3], self.recv.at[3], line.below)]

    def start(self):
        tile = self.tile
        for d in range(self.down):
            arrived(self.sib.at[d], self.s_send.at[d], self.s_recv.at[d], self.other, self.me)
            first = pl.multiple_of((self.me["e"] + 2 * d) * (4 * tile), SUBLANES)
            self.sib[d] = self.part[pl.ds(first, 4 * tile), :] + self.sib[d]
        for copy in self.copies()[:2]:
            copy.start()

    def relay(self):
        line, copies = self.line, self.copies()
        for half, whom, k in ((0, line.below, line.up), (1, line.above, line.down)):
            got = self.half.at[half]
            remote(got, got, self.send.at[half], self.recv.at[half], whom).wait_recv()
            at = self.where(k, half)
            self.sib[at] = self.sib[at] + self.half[half]
            copies[2 + half].start()

    def wait(self, sign=1, more=None):
        for side, whom in ((0, self.line.below), (1, self.line.above)):
            got = self.land.at[side]
            remote(got, got, self.send.at[2 + side], self.recv.at[2 + side], whom).wait_recv()
        total = (self.land[0] + self.land[1]) + self.sib[self.where(self.line.at)]
        total = total if sign > 0 else -total
        self.out[...] = total if more is None else total + more

    def swapped(self):
        for d in range(self.down):
            sent(*self.swap_args(d))

    def finish(self):
        for copy in self.copies():
            copy.wait_send()


def turn(a, b):
    return mm(a, b, ((0,), (0,)))


class Output:
    def __init__(self, n, me, flat, extra, turned, send, f_recv, a_recv, u_recv):
        self.half, self.tile, self.me, self.send = n // 16, n // 128, me, send
        self.into = {"keep": (flat, f_recv), "add": (extra, a_recv), "turn": (turned, u_recv)}
        self.started = []

    def place(self, kind, h, g, ee):
        buf, recv = self.into[kind]
        first = ee * (SIDE * self.tile) + g * self.tile
        if kind == "turn":
            cols = pl.ds(pl.multiple_of(h * self.half, self.half), self.half)
            return buf.at[pl.ds(pl.multiple_of(first, SUBLANES), self.tile), cols], recv.at[h, g, ee]
        return buf.at[pl.ds(pl.multiple_of(first + h * self.half, SUBLANES), self.tile), :], recv.at[h, g, ee]

    def to(self, plan):
        b_row, b_col, kind, rax, cax, gax = plan
        a_r, a_c = self.me[rax], self.me[cax]
        if kind == "turn":
            return {"x": jnp.int32(b_col), "y": a_r, "z": jnp.int32(b_row), "e": a_c // 2}, a_c % 2
        return {"x": jnp.int32(b_row), "y": a_c, "z": jnp.int32(b_col), "e": a_r // 2}, a_r % 2

    def args(self, index):
        plan, src = self.started[index]
        to, h = self.to(plan)
        dst, recv = self.place(plan[2], h, self.me[plan[5]], self.me["e"])
        return src, dst, self.send.at[index], recv, to, self.me

    def start(self, src, *plan):
        self.started.append((plan, src))
        push(*self.args(len(self.started) - 1))

    def incoming(self, plan):
        b_row, b_col, kind, rax, cax, gax = plan
        to_x, to_z = (b_col, b_row) if kind == "turn" else (b_row, b_col)
        y, e = self.me["y"], self.me["e"]

        def find(i):
            h, g, ee = i // 8, i // 2 % SIDE, i % 2
            a_r, a_c = (y, 2 * e + h) if kind == "turn" else (2 * e + h, y)
            return h, g, ee, {rax: a_r, cax: a_c, gax: g, "e": ee}

        return (self.me["x"] == to_x) & (self.me["z"] == to_z), find

    def finish(self, out):
        for plan, _ in self.started:
            cond, find = self.incoming(plan)

            @pl.when(cond)
            def _(plan=plan, find=find):
                def take(i):
                    h, g, ee, at = find(i)
                    dst, recv = self.place(plan[2], h, g, ee)
                    arrived(dst, self.send.at[0], recv, at, self.me)

                loop(16, take)

        kinds = {}
        for plan, _ in self.started:
            where = (plan[1], plan[0]) if plan[2] == "turn" else plan[:2]
            kinds.setdefault(where, set()).add(plan[2])
        for (b_row, b_col), has in kinds.items():
            @pl.when((self.me["x"] == b_row) & (self.me["z"] == b_col))
            def _(has=has):
                terms = [self.into[kind][0][...] for kind in ("keep", "add") if kind in has]
                if "turn" in has:
                    terms.append(self.into["turn"][0][...].T)
                out[...] = sum(terms[1:], terms[0])
        for index in range(len(self.started)):
            sent(*self.args(index))


ZXY, YXZ, ZYX = tuple("zxy"), tuple("yxz"), tuple("zyx")
PLANS = [(r, c, "keep", *ZXY) for r in range(PAIR) for c in range(PAIR)]
PLANS += [(2 + r, c, kind, *YXZ) for r in range(PAIR) for c in range(PAIR) for kind in ("keep", "turn")]
PLANS += [(0, 0, "add", *ZXY), (1, 1, "add", *ZYX), (2, 2, "keep", *ZXY), (3, 3, "keep", *ZYX)]
PLANS += [(r, r - 1, kind, *YXZ) for r, keep in ((1, "add"), (3, "keep")) for kind in (keep, "turn")]
WIDE = ("wa", "wb", "wat", "wbt", "ya", "yb", "ha", "hb")
GATHERS = [("d0", "z"), ("d1", "z"), ("d2", "z"), ("g1", "x"), ("dt", "x"), ("g3", "x"), ("w0", "y"), ("w1", "y"), ("y0", "z"),
           ("y1", "z"), ("x21", "z"), ("w0t", "x"), ("w1t", "x"), ("g2t", "x"), ("yt1t", "x"), ("y1t", "x"), ("wa", "y"),
           ("wb", "y"), ("wat", "x"), ("wbt", "x"), ("ya", "z"), ("yb", "z")]
MOVES = [("w0t", W_TURN), ("w1t", W_TURN), ("g2t", H_TURN), ("yt1t", YT_TURN), ("y1t", Y_TURN), ("wat", W_TURN), ("wbt", W_TURN)]
REDUCES = [("w0", "y"), ("w1", "y"), ("x21", "z"), ("y0", "z"), ("y1", "z"), ("yt1", "z"), ("h0", "y"), ("h1", "y"),
           ("wa", "y"), ("wb", "y"), ("ya", "z"), ("yb", "z"), ("ha", "y"), ("hb", "y")]


def scratch_plan(n):
    big, half, quarter, tile = n // 8, n // 16, n // 32, n // 128
    dma, vmem = pltpu.SemaphoreType.DMA, lambda *shape: pltpu.VMEM(shape, F32)
    pairs, four = 6, 4
    groups = [[vmem(pairs, four, tile, half), vmem(four, tile, half), vmem(four, tile, half), vmem(1, tile, half),
               vmem(big, half), vmem(half, half), vmem(2, big, half)]
              + [vmem(big, big)] * 3 + [vmem(quarter, 2 * big)] * 3
              + [dma((64,)), dma((pairs, four)), dma((6,)), dma((3,)), dma((four,)), dma((four,)), dma((four,)), dma((four,)),
                 dma((48,)), dma((3, four))]]
    def wide(name):
        return 2 * half if name in WIDE else half

    for name, _ in GATHERS:
        groups.append([vmem(four, tile, wide(name)), dma((four,)), dma((four,))])
    for name, _ in MOVES:
        groups.append([vmem(tile, wide(name)), dma((1,)), dma((1,))])
    for name, _ in REDUCES:
        width = wide(name)
        groups.append([vmem(half, width), vmem(1, quarter, width), vmem(2, 1, tile // 2, width), vmem(2, 1, tile, width),
                       vmem(1, tile, width), dma((1,)), dma((1,)), dma((four,)), dma((four,))])
    hubs = dma((2, four, 2))
    groups.append([vmem(big, half), vmem(big, half), vmem(half, big), dma((len(PLANS),)), hubs, hubs, hubs])
    return groups


def whole_kernel(n, sizes, l_ref, out, *refs):
    half = n // 16
    me = coords()
    groups = []
    for size in sizes:
        groups.append(refs[:size])
        refs = refs[size:]
    first, groups = groups[0], groups[1:]
    ga = {name: Gather(axis, me, *group) for (name, axis), group in zip(GATHERS, groups)}
    groups = groups[len(GATHERS):]
    mv = {name: Move(way, me, *group) for (name, way), group in zip(MOVES, groups)}
    groups = groups[len(MOVES):]
    re = {name: Reduce(axis, me, *group) for (name, axis), group in zip(REDUCES, groups)}
    res = Output(n, me, *groups[-1])

    lines = [(None, 4, lambda k, axis=axis: dict(me, **{axis: k})) for axis in "xyz"]
    turns = [W_TURN, H_TURN, Y_TURN, YT_TURN]
    sources = lines + [(None, 1, lambda k, way=way: way[1](me)) for way in turns]
    dests = lines + [(None, 1, lambda k, way=way: way[0](me)) for way in turns]
    for plan in PLANS:
        cond, find = res.incoming(plan)
        sources.append((cond, 16, lambda i, find=find: find(i)[-1]))
        dests.append((None, 1, lambda k, plan=plan: res.to(plan)[0]))
    ct, d, g, dt = first[:4]
    late, ending = stage0(n, me, sources, dests, l_ref, groups[-1][2], *first)

    def ctr(r, c):
        slot = (r * (r - 1)) // 2 + c
        return jnp.concatenate([ct[slot, k] for k in range(SIDE)], axis=0)

    def cols(array, c):
        return array.at[0, :, pl.ds(c * half, half)]

    for name, src in (("d0", d.at[0]), ("d2", d.at[2]), ("d1", d.at[1])):
        ga[name].start(src)

    def each(names, *steps):
        for step in steps:
            for name in names:
                step(name)

    def gathered(name):
        ga[name].relay()

    def ready(name):
        ga[name].wait()

    def begin(name):
        re[name].start()

    def passed(name):
        re[name].relay()

    def turned(name):
        mv[name].wait()
        ga[name].shift = me[mv[name].back]
        ga[name].start(mv[name].buf)

    each(("d0", "d2"), gathered, ready)
    for name, pair, right in (("w0", (1, 0), "d0"), ("w1", (3, 2), "d2")):
        re[name].put(0, turn(ctr(*pair), ga[right].rows()))
    each(("w0", "w1"), begin, passed)
    late()
    for name, src in (("dt", dt.at[0]), ("g3", g.at[3]), ("g1", g.at[1])):
        ga[name].start(src)
    for name in ("w0", "w1"):
        re[name].wait()
        ga[name].start(re[name].out.at[0])
    for name in ("w1", "w0"):
        mv[name + "t"].start(re[name].out.at[0])
    each(("w0", "w1", "dt", "g3", "g1"), gathered)
    each(("w0", "w1", "dt", "g1", "g3"), ready)
    made = ("x21", "y1", "y0", "yt1")
    for name, left, right in zip(made, ("dt", "g3", "g1", "w1"), ("w0", "w1", "w0", "g3")):
        re[name].put(0, turn(ga[left].rows(), ga[right].rows()))
    each(made, begin)
    each(("w1t", "w0t"), turned)
    each(made, passed)
    for name in ("x21", "y1"):
        re[name].wait(-1)
        ga[name].start(re[name].out.at[0])

    def half_h(name, left, right):
        re[name].put(0, turn(ga[left].rows(), ga[right].rows()))

    each(("x21", "y1", "w1t", "d1"), gathered)
    each(("y1", "w1t"), ready)
    half_h("h1", "w1t", "y1")
    each(("x21", "d1"), ready)
    res.start(g.at[1], 1, 1, "add", *ZYX)
    res.start(g.at[3], 3, 3, "keep", *ZYX)
    for kind in ("keep", "turn"):
        res.start(re["y1"].out.at[0], 3, 2, kind, *YXZ)
    zero, one = ga["d0"].rows(), jnp.concatenate([ga["x21"].rows(), ga["d1"].rows()], axis=1)
    for r, name in enumerate(("wa", "wb")):
        if r == 1:
            begin("h1")
        top = turn(ctr(2 + r, 1), one)
        re[name].put(0, jnp.concatenate([top[:, :half] + turn(ctr(2 + r, 0), zero), top[:, half:]], axis=1))
    passed("h1")
    each(("wa", "wb"), begin)
    for name in ("y0", "yt1"):
        re[name].wait(-1)
    ga["y0"].start(re["y0"].out.at[0])
    for name in ("yt1", "y1"):
        mv[name + "t"].start(re[name].out.at[0])
    each(("wa", "wb"), passed)
    re["h1"].wait(-1, g[2:3])
    mv["g2t"].start(re["h1"].out.at[0])
    each(("yt1t", "y1t"), turned)
    each(("w0t", "y0"), gathered)
    turned("g2t")
    for name in ("wa", "wb"):
        re[name].wait()
        ga[name].start(re[name].out.at[0])
    each(("yt1t", "y1t", "g2t"), gathered)

    def product(name, left, right, r=None, more=False):
        lhs = ga[left].rows()
        lhs = lhs if r is None else lhs[:, r * half:(r + 1) * half]
        value = turn(lhs, ga[right].rows())
        if more:
            re[name].put(0, re[name].part[...] + value)
        else:
            re[name].part[...] = value

    each(("wa", "wb"), gathered)
    each(("wa", "g2t", "yt1t"), ready)
    product("ya", "g2t", "wa")
    product("yb", "yt1t", "wa")
    each(("wb", "y1t"), ready)
    for name in ("wa", "wb"):
        mv[name + "t"].start(re[name].out.at[0])
    product("ya", "y1t", "wb", more=True)
    product("yb", "g3", "wb", more=True)
    for kind in ("add", "turn"):
        res.start(re["y0"].out.at[0], 1, 0, kind, *YXZ)
    res.start(re["h1"].out.at[0], 2, 2, "keep", *ZXY)
    each(("ya", "yb"), begin)
    each(("w0t", "y0"), ready)
    half_h("h0", "w0t", "y0")
    each(("ya", "yb"), passed)
    begin("h0")
    for name in ("ya", "yb"):
        re[name].wait(-1)
        ga[name].start(re[name].out.at[0])
    passed("h0")
    each(("wat", "wbt"), turned)
    each(("ya", "yb", "wat", "wbt"), gathered)
    each(("ya", "wat"), ready)
    for r, name in enumerate(("ha", "hb")):
        product(name, "wat", "ya", r)
    each(("yb", "wbt"), ready)
    for r in range(PAIR):
        for c in range(PAIR):
            for kind in ("keep", "turn"):
                res.start(cols(re["ya" if r == 0 else "yb"].out, c), 2 + r, c, kind, *YXZ)
    for r, name in enumerate(("ha", "hb")):
        product(name, "wbt", "yb", r, True)
    each(("ha", "hb"), begin)
    re["h0"].wait(-1, g[0:1])
    res.start(re["h0"].out.at[0], 0, 0, "add", *ZXY)
    each(("ha", "hb"), passed)
    ending()
    for name in (*made, "w0", "w1", "h1", "h0"):
        re[name].finish()
        re[name].swapped()
    for name in ga:
        if name not in WIDE:
            ga[name].finish()
    for r, name in enumerate(("ha", "hb")):
        re[name].wait(-1)
        for c in range(PAIR):
            res.start(cols(re[name].out, c), r, c, "keep", *ZXY)
    for part in [*mv.values(), *(ga[name] for name in ga if name in WIDE)]:
        part.finish()
    res.finish(out)
    for name in re:
        if name in WIDE:
            re[name].finish()
            re[name].swapped()


def solution(mesh):
    def local_fn(l_blk):
        n = l_blk.shape[0] * 8
        groups = scratch_plan(n)
        spec = pl.BlockSpec(memory_space=pltpu.VMEM)
        call = pl.pallas_call(
            functools.partial(whole_kernel, n, [len(group) for group in groups]),
            out_shape=jax.ShapeDtypeStruct(l_blk.shape, F32),
            in_specs=[spec],
            out_specs=spec,
            scratch_shapes=sum(groups, []),
            compiler_params=pltpu.CompilerParams(
                has_side_effects=True, vmem_limit_bytes=VMEM_LIMIT, collective_id=0),
            name="whole",
        )
        return call(l_blk)

    spec = P(("batch", "row"), "col")
    return jax.shard_map(local_fn, mesh=mesh, in_specs=(spec,), out_specs=spec, check_vma=False)
```

```python
import functools

import jax
import jax.numpy as jnp
from jax import lax
from jax.experimental import pallas as pl
from jax.experimental.pallas import tpu as pltpu
from jax.sharding import PartitionSpec as P

MESH = pl.DeviceIdType.MESH
HIGHEST = lax.Precision.HIGHEST
F32 = jnp.float32
VMEM_LIMIT = 67043328
SIDE, PAIR, SUBLANES = 4, 2, 8


def coords():
    col = lax.axis_index("col")
    row = lax.axis_index("row")
    return {"x": row // 2, "y": col % SIDE, "z": col // 4, "e": row % 2}


def device(at):
    return (0, 4 * at["z"] + at["y"], 2 * at["x"] + at["e"])


def same(p, q):
    return (p["x"] == q["x"]) & (p["y"] == q["y"]) & (p["z"] == q["z"]) & (p["e"] == q["e"])


def mm(a, b, dims=((1,), (0,))):
    return lax.dot_general(a, b, (dims, ((), ())), precision=HIGHEST, preferred_element_type=F32)


def loop(count, body):
    def step(k, carry):
        body(k)
        return carry

    lax.fori_loop(0, count, step, jnp.int32(0))


def push(src, dst, send_sem, recv_sem, to, me):
    here = same(to, me)

    @pl.when(here)
    def _():
        dst[...] = src[...]

    @pl.when(jnp.logical_not(here))
    def _():
        pltpu.make_async_remote_copy(
            src_ref=src, dst_ref=dst, send_sem=send_sem, recv_sem=recv_sem, device_id=device(to), device_id_type=MESH
        ).start()


def sent(src, dst, send_sem, recv_sem, to, me):
    @pl.when(jnp.logical_not(same(to, me)))
    def _():
        pltpu.make_async_remote_copy(
            src_ref=src, dst_ref=dst, send_sem=send_sem, recv_sem=recv_sem, device_id=device(to), device_id_type=MESH
        ).wait_send()


def arrived(dst, send_sem, recv_sem, source, me):
    @pl.when(jnp.logical_not(same(source, me)))
    def _():
        pltpu.make_async_remote_copy(
            src_ref=dst, dst_ref=dst, send_sem=send_sem, recv_sem=recv_sem, device_id=device(source), device_id_type=MESH
        ).wait_recv()


def meet(sources, dests, me):
    barrier = pltpu.get_barrier_semaphore()

    def other(cond, at):
        apart = jnp.logical_not(same(at, me))
        return apart if cond is None else apart & cond

    total = jnp.int32(0)
    for cond, count, which in sources:
        def tell(k, which=which):
            @pl.when(other(None, which(k)))
            def _():
                pl.semaphore_signal(barrier, inc=1, device_id=device(which(k)), device_id_type=MESH)

        if cond is None:
            loop(count, tell)
        else:
            @pl.when(cond)
            def _(count=count, tell=tell):
                loop(count, tell)

    for cond, count, which in dests:
        def add(k, carry, cond=cond, which=which):
            return carry + other(cond, which(k)).astype(jnp.int32)

        total = lax.fori_loop(0, count, add, total)

    @pl.when(total > 0)
    def _():
        pl.semaphore_wait(barrier, total)


def remote(src, dst, send_sem, recv_sem, to):
    return pltpu.make_async_remote_copy(
        src_ref=src, dst_ref=dst, send_sem=send_sem, recv_sem=recv_sem, device_id=device(to), device_id_type=MESH)


def invert_block(left, corner, inv, base):
    half = 3 * base
    rows = lax.broadcasted_iota(jnp.int32, (base, base), 0)
    cols = lax.broadcasted_iota(jnp.int32, (base, base), 1)
    eye = rows == cols

    def block(i, j):
        if j < 3:
            return left[i * base:(i + 1) * base, j * base:(j + 1) * base]
        return corner[(i - 3) * base:(i - 2) * base, (j - 3) * base:(j - 2) * base]

    tri = [block(i, i) for i in range(6)]
    found = []
    for i in range(6):
        diag = jnp.sum(jnp.where(eye, tri[i], 0.0), axis=1, keepdims=True)
        found.append(jnp.where(eye, 1.0 / diag, 0.0))
    size = 1
    while size < base:
        below = ((rows // size) % 2 == 1) & (cols // size == rows // size - 1)
        half_way = [mm(jnp.where(below, tri[i], 0.0), found[i]) for i in range(6)]
        found = [found[i] - mm(found[i], half_way[i]) for i in range(6)]
        size = size * 2
    inv[...] = jnp.zeros(inv.shape, F32)
    for k in (0, 3):
        x0, x1, x2 = found[k:k + 3]
        x10 = -mm(x1, mm(block(k + 1, k), x0))
        x21 = -mm(x2, mm(block(k + 2, k + 1), x1))
        x20 = -mm(x2, mm(block(k + 2, k), x0) + mm(block(k + 2, k + 1), x10))
        for i, j, val in ((0, 0, x0), (1, 1, x1), (2, 2, x2), (1, 0, x10), (2, 1, x21), (2, 0, x20)):
            inv[(k + i) * base:(k + i + 1) * base, (k + j) * base:(k + j + 1) * base] = val
    low = mm(left[half:, :], inv[:half, :half])
    inv[half:, :half] = -mm(inv[half:, half:], low)


def stage0(n, me, sources, dests, l_ref, lt_ref, ct_out, d_out, g_out, dt_out,
           left, corner, cmat, inv_a, inv_b, inv_t, slab_d, slab_t, slab_g,
           ct_send, ct_recv, ab_send, ab_recv, c_send, c_recv, x_send, x_recv, t_send, t_recv):
    x, y, z, e = me["x"], me["y"], me["z"], me["e"]
    big = n // 8
    half = n // 16
    quarter = n // 32
    tile = n // 128
    sib = dict(me, e=1 - e)
    diag = x == z

    slot = (x * (x - 1)) // 2 + z
    def ct_args(i):
        g, k, h, ee = i // 16, i // 4 % SIDE, i // 2 % 2, i % 2
        rows = pl.ds(pl.multiple_of(quarter * ee + tile * g, SUBLANES), tile)
        src = lt_ref.at[rows, pl.ds(pl.multiple_of(half * h, half), half)]
        to = {"x": k, "y": y, "z": 2 * e + h, "e": ee}
        return src, ct_out.at[slot, g], ct_send.at[i], ct_recv.at[slot, g], to, me

    up, down = dict(me, y=(y + 1) % SIDE), dict(me, y=(y + 3) % SIDE)

    def at(b, along_y):
        b = jnp.int32(b)
        return {"x": b, "y": along_y, "z": b, "e": e}

    odd = x % 2

    def dest(kind, i):
        g, j = i // 4, i % SIDE
        if kind == 0:
            return {"x": j, "y": y, "z": g, "e": e}
        if kind == 1:
            return {"x": odd * g + (1 - odd) * j, "y": odd * j + (1 - odd) * g, "z": y, "e": e}
        return {"x": g, "y": j, "z": y, "e": e}

    def full(kind, i):
        return i % SIDE <= y if kind == 0 else i % SIDE >= y

    pairs = [(b_row, b_col) for b_row in range(SIDE) for b_col in range(b_row)]

    def ct_source(b_row, b_col):
        return {"x": jnp.int32(b_row), "y": y, "z": jnp.int32(b_col), "e": z // 2}

    def one(cond, where):
        return cond, 1, lambda k: where

    sources = sources + [one(None, ct_source(*pair)) for pair in pairs] + [one(diag, sib)]
    sources += [one(diag, up), one(diag, down)]
    sources += [(x <= y, 3, lambda b: at(b, y)), (None, 4, lambda b: at(b, z)), one(y >= z, at(1, z))]
    dests = dests + [(x > z, 16, lambda i: ct_args(i)[4]), one(diag, sib)]
    dests += [one(diag, up), one(diag, down)]
    dests += [(diag, 16, lambda i: dest(1, i))]
    for kind, cond in ((0, diag & (x < 3)), (2, diag & (x == 1))):
        dests += [(cond & full(kind, i), 1, lambda k, kind=kind, i=i: dest(kind, jnp.int32(i))) for i in range(16)]

    @pl.when(x > z)
    def _():
        lt_ref[...] = l_ref[...].T

    meet(sources, dests, me)

    place = (y + SIDE - 2 * e) % SIDE
    third = half // 3

    def ab_copies(chunk, way, own):
        dst, first = ((left, 0), (left, half), (corner, 0))[chunk]
        src, start = (l_ref, half * min(chunk, 1)) if own else (dst, first)
        cuts = [(0, half, half)] if chunk == 1 else [(third * i, third, third * i + third) for i in range(3)]
        return [remote(src.at[pl.ds(start + row, tall), pl.ds(0, across)], dst.at[pl.ds(first + row, tall), pl.ds(0, across)],
                       ab_send.at[chunk + 3 * way, i], ab_recv.at[chunk, i], (up, down)[way])
                for i, (row, tall, across) in enumerate(cuts)]

    def ab_came(chunk):
        for copy in ab_copies(chunk, 0, 0):
            copy.wait_recv()

    def ab_start(code):
        for copy in ab_copies(*map(int, code)):
            copy.start()

    ab_sends = [("001", "111", "101", "011"), ("211", "201", "000"), ("200",), ("110",)]

    def c_copy(part, chunk, way, own):
        rows = pl.ds(half * chunk, half)
        dst = cmat.at[part, rows, :]
        src = l_ref.at[rows, :] if own else dst
        return remote(src, dst, c_send.at[chunk + 2 * way], c_recv.at[2 * part + chunk], (up, down)[way])

    def c_came(part, chunk):
        c_copy(part, chunk, 0, 0).wait_recv()

    c_sends = [("0001", "0011", "0101", "0111"), ("1001", "1011", "1101", "1111"), ("1000", "1100"), ("0010", "0110")]

    for part in range(PAIR):
        @pl.when(diag & (place == part))
        def _(part=part):
            for code in ab_sends[part]:
                if int(code[2]):
                    ab_start(code)

    @pl.when(x > z)
    def _():
        loop(64, lambda i: push(*ct_args(i)))

    def swap_args(k):
        mine = [inv_a, inv_b, cmat.at[0], cmat.at[1]][k]
        return mine, mine, x_send.at[k], x_recv.at[k], sib, me

    def swap_came(k):
        arrived(swap_args(k)[1], x_send.at[k], x_recv.at[k], sib, me)

    closing = []

    @pl.when(diag)
    def _():
        for part, order in enumerate(("2", "01", "201", "102")):
            @pl.when(place == part)
            def _(part=part, order=order):
                if part == 0:
                    left[...] = l_ref[...]
                elif part == 1:
                    corner[...] = l_ref[half:, :]
                for chunk in order:
                    ab_came(int(chunk))
                    if part > 0 and chunk == order[0]:
                        ab_start(ab_sends[part][-1])

        for part in range(PAIR):
            @pl.when((e == 1) & (y == part))
            def _(part=part):
                for code in c_sends[part]:
                    c_copy(*map(int, code)).start()
                cmat[part] = l_ref[...]

        invert_block(left, corner, inv_t, n // 48)
        for part in range(PAIR):
            @pl.when((e == 1) & (y == part))
            def _(part=part):
                push(*swap_args(2 + part))

            @pl.when((e == 1) & (y == part + 2))
            def _(part=part):
                c_came(1 - part, 0)
                c_copy(*map(int, c_sends[part + 2][0])).start()

        for core, inv in ((0, inv_a), (1, inv_b)):
            @pl.when(e == core)
            def _(inv=inv):
                inv[...] = inv_t[...]

        lower, across = y >= 2, ((1,), (1,))
        first = pl.multiple_of((y % 2) * half + e * quarter, SUBLANES)
        mine = pl.ds(first, quarter)

        for core in range(PAIR):
            @pl.when(e == core)
            def _(core=core):
                push(*swap_args(core))
                swap_came(1 - core)

        @pl.when(jnp.logical_not(lower))
        def _():
            inv_t[...] = inv_a[...].T
            slab_t[:, :big] = inv_t[mine, :]
            slab_d[:, :big] = inv_a[mine, :]

        @pl.when(lower)
        def _():
            inv_t[...] = inv_b[...].T
            slab_t[:, big:] = inv_t[mine, :]
            slab_g[:, big:] = mm(slab_t[:, big:], inv_b[...])
            slab_d[:, big:] = inv_b[mine, :]

        @pl.when(e == 1)
        def _():
            for part in range(PAIR):
                @pl.when(y == part)
                def _(part=part):
                    c_came(1 - part, 0)
                    c_came(1 - part, 1)
                    push(*swap_args(3 - part))

                @pl.when(y == part + 2)
                def _(part=part):
                    c_came(1 - part, 1)
                    c_copy(*map(int, c_sends[part + 2][1])).start()
                    push(*swap_args(3 - part))
                    c_came(part, 0)
                    c_came(part, 1)
                    push(*swap_args(2 + part))

        @pl.when(e == 0)
        def _():
            swap_came(2)
            swap_came(3)

        def times_c(v):
            return jnp.concatenate([mm(v, cmat[0]), mm(v, cmat[1])], axis=1)

        def spread(kind, i):
            rows = pl.ds(pl.multiple_of(tile * (i // 4), SUBLANES), tile)
            src = (slab_d, slab_g, slab_t)[kind].at[rows, pl.ds(pl.multiple_of(half * (i % SIDE), half), half)]
            dst = (d_out, g_out)[kind].at[x] if kind < 2 else dt_out.at[0]
            recv = t_recv.at[kind, x] if kind < 2 else t_recv.at[2, 0]
            return src, dst, t_send.at[kind * 16 + i], recv, dest(kind, i), me

        def spread_all(use, kind):
            def step(i):
                if kind == 1:
                    use(*spread(kind, i))
                else:
                    @pl.when(full(kind, i))
                    def _():
                        use(*spread(kind, i))

            loop(16, step)

        @pl.when(lower)
        def _():
            slab_d[:, :big] = -mm(times_c(slab_d[:, big:]), inv_a[...])

        @pl.when(x < 3)
        def _():
            spread_all(push, 0)

        @pl.when(jnp.logical_not(lower))
        def _():
            w = mm(slab_t[:, :half], cmat[0], across) + mm(slab_t[:, half:big], cmat[1], across)
            slab_t[:, big:] = -mm(w, inv_b[...], across)

        @pl.when(x == 1)
        def _():
            spread_all(push, 2)

        @pl.when(jnp.logical_not(lower))
        def _():
            slab_g[:, big:] = mm(slab_t[:, big:], inv_b[...])
            slab_g[:, :big] = mm(slab_t[:, :big] - times_c(slab_g[:, big:]), inv_a[...])

        @pl.when(lower)
        def _():
            slab_g[:, :big] = -mm(times_c(slab_g[:, big:]), inv_a[...])

        spread_all(push, 1)

        def close():
            @pl.when(x < 3)
            def _():
                spread_all(sent, 0)

            @pl.when(x == 1)
            def _():
                spread_all(sent, 2)

            spread_all(sent, 1)
            for part in range(SIDE):
                @pl.when(place == part)
                def _(part=part):
                    for code in ab_sends[part]:
                        for copy in ab_copies(*map(int, code)):
                            copy.wait_send()

                @pl.when((e == 1) & (y == part))
                def _(part=part):
                    for code in c_sends[part]:
                        c_copy(*map(int, code)).wait_send()

            for core in range(PAIR):
                @pl.when(e == core)
                def _(core=core):
                    for k in (0,) if core == 0 else (1, 2, 3):
                        sent(*swap_args(k))

        closing.append(close)

    @pl.when(x <= y)
    def _():
        loop(3, lambda b: arrived(d_out.at[b], t_send.at[0], t_recv.at[0, b], at(b, y), me))

    @pl.when(x > y)
    def _():
        d_out[...] = jnp.zeros(d_out.shape, F32)

    for k, pair in enumerate(pairs):
        loop(SIDE, lambda g, k=k, pair=pair: arrived(ct_out.at[k, g], ct_send.at[0], ct_recv.at[k, g], ct_source(*pair), me))

    def late():
        loop(SIDE, lambda b: arrived(g_out.at[b], t_send.at[0], t_recv.at[1, b], at(b, z), me))

        @pl.when(y >= z)
        def _():
            arrived(dt_out.at[0], t_send.at[0], t_recv.at[2, 0], at(1, z), me)

        @pl.when(y < z)
        def _():
            dt_out[...] = jnp.zeros(dt_out.shape, F32)

    def finish():
        @pl.when(diag)
        def _():
            closing[0]()

        @pl.when(x > z)
        def _():
            loop(64, lambda i: sent(*ct_args(i)))

    return late, finish


def moved(turn, digit, back):
    def to(me):
        return {"x": (me["x"] + me[digit]) % SIDE, "y": me[turn[0]], "z": me[turn[1]], "e": me["e"]}

    def source(me):
        found = dict(me, x=me[back])
        found.update(zip(turn, (me["y"], me["z"])))
        found[digit] = (me["x"] + SIDE - me[back]) % SIDE
        return found

    return to, source, back


W_TURN = moved("zx", "y", "z")
H_TURN = moved("xz", "y", "y")
Y_TURN = moved("xy", "z", "y")
YT_TURN = moved("yx", "z", "z")


class Move:
    def __init__(self, way, me, buf, send, recv):
        (self.to, self.source, self.back), self.me, self.buf, self.send, self.recv = way, me, buf, send, recv

    def args(self):
        return self.src, self.buf, self.send.at[0], self.recv.at[0], self.to(self.me), self.me

    def start(self, src):
        self.src = src
        push(*self.args())

    def wait(self):
        arrived(self.buf, self.send.at[0], self.recv.at[0], self.source(self.me), self.me)

    def finish(self):
        sent(*self.args())


class Line:
    def __init__(self, axis, me):
        self.at = me[axis]
        self.up, self.across, self.down = ((self.at + k) % SIDE for k in (1, 2, 3))
        self.above, self.below = dict(me, **{axis: self.up}), dict(me, **{axis: self.down})


class Gather:
    def __init__(self, axis, me, buf, send, recv):
        self.line, self.buf, self.send, self.recv = Line(axis, me), buf, send, recv
        self.shift = None

    def piece(self, slot, half):
        if len(self.buf.shape) > 3:
            return self.buf.at[slot, pl.ds(half, 1)]
        rows = self.buf.shape[1] // 2
        return self.buf.at[slot, pl.ds(half * rows, rows)]

    def copies(self):
        line, buf = self.line, self.buf
        return [
            remote(self.src, buf.at[line.at], self.send.at[0], self.recv.at[0], line.above),
            remote(self.src, buf.at[line.at], self.send.at[1], self.recv.at[1], line.below),
            remote(self.piece(line.down, 0), self.piece(line.down, 0), self.send.at[2], self.recv.at[2], line.above),
            remote(self.piece(line.up, 1), self.piece(line.up, 1), self.send.at[3], self.recv.at[3], line.below)]

    def start(self, src):
        self.src = src
        for copy in self.copies()[:2]:
            copy.start()
        self.buf[self.line.at] = src[...]

    def relay(self):
        line, buf = self.line, self.buf
        onward = self.copies()[2:]
        remote(buf.at[line.down], buf.at[line.down], self.send.at[0], self.recv.at[0], line.below).wait_recv()
        onward[0].start()
        remote(buf.at[line.up], buf.at[line.up], self.send.at[1], self.recv.at[1], line.above).wait_recv()
        onward[1].start()

    def wait(self):
        for half, whom in ((0, self.line.below), (1, self.line.above)):
            piece = self.piece(self.line.across, half)
            remote(piece, piece, self.send.at[2 + half], self.recv.at[2 + half], whom).wait_recv()

    def finish(self):
        for copy in self.copies():
            copy.wait_send()

    def rows(self, block=None):
        places = [k if self.shift is None else (k + self.shift) % SIDE for k in range(SIDE)]
        tiles = [self.buf[k] if block is None else self.buf[k, block] for k in places]
        return jnp.concatenate(tiles, axis=0)


class Reduce:
    def __init__(self, axis, me, part, sib, half, land, out, s_send, s_recv, r_send, r_recv):
        self.line, self.me, self.part, self.sib, self.half, self.land, self.out = Line(axis, me), me, part, sib, half, land, out
        self.s_send, self.s_recv, self.send, self.recv = s_send, s_recv, r_send, r_recv
        self.other = dict(me, e=1 - me["e"])
        self.down, self.tile = out.shape[:2]

    def swap_args(self, d):
        rows = pl.ds(((1 - self.me["e"]) + 2 * d) * (SIDE * self.tile), SIDE * self.tile)
        return self.part.at[rows, :], self.sib.at[d], self.s_send.at[d], self.s_recv.at[d], self.other, self.me

    def put(self, d, value):
        self.part[d * 8 * self.tile:(d + 1) * 8 * self.tile, :] = value
        push(*self.swap_args(d))

    def where(self, k, half=None):
        first = pl.multiple_of(k * self.tile, SUBLANES)
        if half is None:
            return slice(None), pl.ds(first, self.tile)
        if self.down > 1:
            return pl.ds(half, 1), pl.ds(first, self.tile)
        rows = self.tile // 2
        return slice(None), pl.ds(pl.multiple_of(first + half * rows, SUBLANES), rows)

    def copies(self):
        line, sib = self.line, self.sib
        return [
            remote(sib.at[self.where(line.across, 0)], self.half.at[0], self.send.at[0], self.recv.at[0], line.above),
            remote(sib.at[self.where(line.across, 1)], self.half.at[1], self.send.at[1], self.recv.at[1], line.below),
            remote(sib.at[self.where(line.up)], self.land.at[0], self.send.at[2], self.recv.at[2], line.above),
            remote(sib.at[self.where(line.down)], self.land.at[1], self.send.at[3], self.recv.at[3], line.below)]

    def start(self):
        tile = self.tile
        for d in range(self.down):
            arrived(self.sib.at[d], self.s_send.at[d], self.s_recv.at[d], self.other, self.me)
            first = pl.multiple_of((self.me["e"] + 2 * d) * (4 * tile), SUBLANES)
            self.sib[d] = self.part[pl.ds(first, 4 * tile), :] + self.sib[d]
        for copy in self.copies()[:2]:
            copy.start()

    def relay(self):
        line, copies = self.line, self.copies()
        for half, whom, k in ((0, line.below, line.up), (1, line.above, line.down)):
            got = self.half.at[half]
            remote(got, got, self.send.at[half], self.recv.at[half], whom).wait_recv()
            at = self.where(k, half)
            self.sib[at] = self.sib[at] + self.half[half]
            copies[2 + half].start()

    def wait(self, sign=1, more=None):
        for side, whom in ((0, self.line.below), (1, self.line.above)):
            got = self.land.at[side]
            remote(got, got, self.send.at[2 + side], self.recv.at[2 + side], whom).wait_recv()
        total = (self.land[0] + self.land[1]) + self.sib[self.where(self.line.at)]
        total = total if sign > 0 else -total
        self.out[...] = total if more is None else total + more

    def swapped(self):
        for d in range(self.down):
            sent(*self.swap_args(d))

    def finish(self):
        for copy in self.copies():
            copy.wait_send()


def turn(a, b):
    return mm(a, b, ((0,), (0,)))


class Output:
    def __init__(self, n, me, flat, extra, turned, send, f_recv, a_recv, u_recv):
        self.half, self.tile, self.me, self.send = n // 16, n // 128, me, send
        self.into = {"keep": (flat, f_recv), "add": (extra, a_recv), "turn": (turned, u_recv)}
        self.started = []

    def place(self, kind, h, g, ee):
        buf, recv = self.into[kind]
        first = ee * (SIDE * self.tile) + g * self.tile
        if kind == "turn":
            cols = pl.ds(pl.multiple_of(h * self.half, self.half), self.half)
            return buf.at[pl.ds(pl.multiple_of(first, SUBLANES), self.tile), cols], recv.at[h, g, ee]
        return buf.at[pl.ds(pl.multiple_of(first + h * self.half, SUBLANES), self.tile), :], recv.at[h, g, ee]

    def to(self, plan):
        b_row, b_col, kind, rax, cax, gax = plan
        a_r, a_c = self.me[rax], self.me[cax]
        if kind == "turn":
            return {"x": jnp.int32(b_col), "y": a_r, "z": jnp.int32(b_row), "e": a_c // 2}, a_c % 2
        return {"x": jnp.int32(b_row), "y": a_c, "z": jnp.int32(b_col), "e": a_r // 2}, a_r % 2

    def args(self, index):
        plan, src = self.started[index]
        to, h = self.to(plan)
        dst, recv = self.place(plan[2], h, self.me[plan[5]], self.me["e"])
        return src, dst, self.send.at[index], recv, to, self.me

    def start(self, src, *plan):
        self.started.append((plan, src))
        push(*self.args(len(self.started) - 1))

    def incoming(self, plan):
        b_row, b_col, kind, rax, cax, gax = plan
        to_x, to_z = (b_col, b_row) if kind == "turn" else (b_row, b_col)
        y, e = self.me["y"], self.me["e"]

        def find(i):
            h, g, ee = i // 8, i // 2 % SIDE, i % 2
            a_r, a_c = (y, 2 * e + h) if kind == "turn" else (2 * e + h, y)
            return h, g, ee, {rax: a_r, cax: a_c, gax: g, "e": ee}

        return (self.me["x"] == to_x) & (self.me["z"] == to_z), find

    def finish(self, out):
        for plan, _ in self.started:
            cond, find = self.incoming(plan)

            @pl.when(cond)
            def _(plan=plan, find=find):
                def take(i):
                    h, g, ee, at = find(i)
                    dst, recv = self.place(plan[2], h, g, ee)
                    arrived(dst, self.send.at[0], recv, at, self.me)

                loop(16, take)

        kinds = {}
        for plan, _ in self.started:
            where = (plan[1], plan[0]) if plan[2] == "turn" else plan[:2]
            kinds.setdefault(where, set()).add(plan[2])
        for (b_row, b_col), has in kinds.items():
            @pl.when((self.me["x"] == b_row) & (self.me["z"] == b_col))
            def _(has=has):
                terms = [self.into[kind][0][...] for kind in ("keep", "add") if kind in has]
                if "turn" in has:
                    terms.append(self.into["turn"][0][...].T)
                out[...] = sum(terms[1:], terms[0])
        for index in range(len(self.started)):
            sent(*self.args(index))


ZXY, YXZ, ZYX = tuple("zxy"), tuple("yxz"), tuple("zyx")
PLANS = [(r, c, "keep", *ZXY) for r in range(PAIR) for c in range(PAIR)]
PLANS += [(2 + r, c, kind, *YXZ) for r in range(PAIR) for c in range(PAIR) for kind in ("keep", "turn")]
PLANS += [(0, 0, "add", *ZXY), (1, 1, "add", *ZYX), (2, 2, "keep", *ZXY), (3, 3, "keep", *ZYX)]
PLANS += [(r, r - 1, kind, *YXZ) for r, keep in ((1, "add"), (3, "keep")) for kind in (keep, "turn")]
WIDE = ("wa", "wb", "wat", "wbt", "ya", "yb", "ha", "hb")
GATHERS = [("d0", "z"), ("d1", "z"), ("d2", "z"), ("g1", "x"), ("dt", "x"), ("g3", "x"), ("w0", "y"), ("w1", "y"), ("y0", "z"),
           ("y1", "z"), ("x21", "z"), ("w0t", "x"), ("w1t", "x"), ("g2t", "x"), ("yt1t", "x"), ("y1t", "x"), ("wa", "y"),
           ("wb", "y"), ("wat", "x"), ("wbt", "x"), ("ya", "z"), ("yb", "z")]
MOVES = [("w0t", W_TURN), ("w1t", W_TURN), ("g2t", H_TURN), ("yt1t", YT_TURN), ("y1t", Y_TURN), ("wat", W_TURN), ("wbt", W_TURN)]
REDUCES = [("w0", "y"), ("w1", "y"), ("x21", "z"), ("y0", "z"), ("y1", "z"), ("yt1", "z"), ("h0", "y"), ("h1", "y"),
           ("wa", "y"), ("wb", "y"), ("ya", "z"), ("yb", "z"), ("ha", "y"), ("hb", "y")]


def scratch_plan(n):
    big, half, quarter, tile = n // 8, n // 16, n // 32, n // 128
    dma, vmem = pltpu.SemaphoreType.DMA, lambda *shape: pltpu.VMEM(shape, F32)
    pairs, four = 6, 4
    groups = [[vmem(pairs, four, tile, half), vmem(four, tile, half), vmem(four, tile, half), vmem(1, tile, half),
               vmem(big, half), vmem(half, half), vmem(2, big, half)]
              + [vmem(big, big)] * 3 + [vmem(quarter, 2 * big)] * 3
              + [dma((64,)), dma((pairs, four)), dma((6, 3)), dma((3, 3)), dma((four,)), dma((four,)), dma((four,)), dma((four,)),
                 dma((48,)), dma((3, four))]]
    def wide(name):
        return 2 * half if name in WIDE else half

    for name, _ in GATHERS:
        groups.append([vmem(four, tile, wide(name)), dma((four,)), dma((four,))])
    for name, _ in MOVES:
        groups.append([vmem(tile, wide(name)), dma((1,)), dma((1,))])
    for name, _ in REDUCES:
        width = wide(name)
        groups.append([vmem(half, width), vmem(1, quarter, width), vmem(2, 1, tile // 2, width), vmem(2, 1, tile, width),
                       vmem(1, tile, width), dma((1,)), dma((1,)), dma((four,)), dma((four,))])
    hubs = dma((2, four, 2))
    groups.append([vmem(big, half), vmem(big, half), vmem(half, big), dma((len(PLANS),)), hubs, hubs, hubs])
    return groups


def whole_kernel(n, sizes, l_ref, out, *refs):
    half = n // 16
    me = coords()
    groups = []
    for size in sizes:
        groups.append(refs[:size])
        refs = refs[size:]
    first, groups = groups[0], groups[1:]
    ga = {name: Gather(axis, me, *group) for (name, axis), group in zip(GATHERS, groups)}
    groups = groups[len(GATHERS):]
    mv = {name: Move(way, me, *group) for (name, way), group in zip(MOVES, groups)}
    groups = groups[len(MOVES):]
    re = {name: Reduce(axis, me, *group) for (name, axis), group in zip(REDUCES, groups)}
    res = Output(n, me, *groups[-1])

    lines = [(None, 4, lambda k, axis=axis: dict(me, **{axis: k})) for axis in "xyz"]
    turns = [W_TURN, H_TURN, Y_TURN, YT_TURN]
    sources = lines + [(None, 1, lambda k, way=way: way[1](me)) for way in turns]
    dests = lines + [(None, 1, lambda k, way=way: way[0](me)) for way in turns]
    for plan in PLANS:
        cond, find = res.incoming(plan)
        sources.append((cond, 16, lambda i, find=find: find(i)[-1]))
        dests.append((None, 1, lambda k, plan=plan: res.to(plan)[0]))
    ct, d, g, dt = first[:4]
    late, ending = stage0(n, me, sources, dests, l_ref, groups[-1][2], *first)

    def ctr(r, c):
        slot = (r * (r - 1)) // 2 + c
        return jnp.concatenate([ct[slot, k] for k in range(SIDE)], axis=0)

    def cols(array, c):
        return array.at[0, :, pl.ds(c * half, half)]

    for name, src in (("d0", d.at[0]), ("d2", d.at[2])):
        ga[name].start(src)

    def each(names, *steps):
        for step in steps:
            for name in names:
                step(name)

    def gathered(name):
        ga[name].relay()

    def ready(name):
        ga[name].wait()

    def begin(name):
        re[name].start()

    def passed(name):
        re[name].relay()

    def turned(name):
        mv[name].wait()
        ga[name].shift = me[mv[name].back]
        ga[name].start(mv[name].buf)

    each(("d0", "d2"), gathered, ready)
    for name, pair, right in (("w0", (1, 0), "d0"), ("w1", (3, 2), "d2")):
        re[name].put(0, turn(ctr(*pair), ga[right].rows()))
    each(("w0", "w1"), begin, passed)
    late()
    for name, src in (("dt", dt.at[0]), ("g3", g.at[3]), ("g1", g.at[1]), ("d1", d.at[1])):
        ga[name].start(src)
    for name in ("w0", "w1"):
        re[name].wait()
        ga[name].start(re[name].out.at[0])
    for name in ("w1", "w0"):
        mv[name + "t"].start(re[name].out.at[0])
    each(("w0", "w1", "dt", "g3", "g1"), gathered)
    each(("w0", "w1", "dt", "g1", "g3"), ready)
    made = ("x21", "y1", "y0", "yt1")
    for index, (left, right) in enumerate((("dt", "w0"), ("g3", "w1"), ("g1", "w0"), ("w1", "g3"))):
        re[made[index]].put(0, turn(ga[left].rows(), ga[right].rows()))
        if index > 0:
            begin(made[index - 1])
    begin(made[-1])
    each(made[:2], passed)
    for name in ("x21", "y1"):
        re[name].wait(-1)
        ga[name].start(re[name].out.at[0])
    each(("w1t", "w0t"), turned)
    each(made[2:], passed)

    def half_h(name, left, right):
        re[name].put(0, turn(ga[left].rows(), ga[right].rows()))

    each(("x21", "y1", "w1t", "d1"), gathered)
    each(("y1", "w1t"), ready)
    half_h("h1", "w1t", "y1")
    each(("x21", "d1"), ready)
    res.start(g.at[1], 1, 1, "add", *ZYX)
    res.start(g.at[3], 3, 3, "keep", *ZYX)
    for kind in ("keep", "turn"):
        res.start(re["y1"].out.at[0], 3, 2, kind, *YXZ)
    zero, one = ga["d0"].rows(), jnp.concatenate([ga["x21"].rows(), ga["d1"].rows()], axis=1)
    for r, name in enumerate(("wa", "wb")):
        if r == 1:
            begin("h1")
        top = turn(ctr(2 + r, 1), one)
        re[name].put(0, jnp.concatenate([top[:, :half] + turn(ctr(2 + r, 0), zero), top[:, half:]], axis=1))
    passed("h1")
    each(("wa", "wb"), begin)
    for name in ("y0", "yt1"):
        re[name].wait(-1)
    ga["y0"].start(re["y0"].out.at[0])
    for name in ("yt1", "y1"):
        mv[name + "t"].start(re[name].out.at[0])
    each(("wa", "wb"), passed)
    re["h1"].wait(-1, g[2:3])
    mv["g2t"].start(re["h1"].out.at[0])
    each(("yt1t", "y1t"), turned)
    each(("w0t", "y0"), gathered)
    turned("g2t")
    for name in ("wa", "wb"):
        re[name].wait()
        ga[name].start(re[name].out.at[0])
    each(("yt1t", "y1t", "g2t"), gathered)

    def product(name, left, right, r=None, more=False):
        lhs = ga[left].rows()
        lhs = lhs if r is None else lhs[:, r * half:(r + 1) * half]
        value = turn(lhs, ga[right].rows())
        if more:
            re[name].put(0, re[name].part[...] + value)
        else:
            re[name].part[...] = value

    each(("wa", "wb"), gathered)
    each(("wa", "g2t", "yt1t"), ready)
    product("ya", "g2t", "wa")
    product("yb", "yt1t", "wa")
    each(("wb", "y1t"), ready)
    for name in ("wa", "wb"):
        mv[name + "t"].start(re[name].out.at[0])
    product("ya", "y1t", "wb", more=True)
    product("yb", "g3", "wb", more=True)
    for kind in ("add", "turn"):
        res.start(re["y0"].out.at[0], 1, 0, kind, *YXZ)
    res.start(re["h1"].out.at[0], 2, 2, "keep", *ZXY)
    each(("ya", "yb"), begin)
    each(("w0t", "y0"), ready)
    half_h("h0", "w0t", "y0")
    each(("ya", "yb"), passed)
    begin("h0")
    for name in ("ya", "yb"):
        re[name].wait(-1)
        ga[name].start(re[name].out.at[0])
    passed("h0")
    each(("wat", "wbt"), turned)
    each(("ya", "yb", "wat", "wbt"), gathered)
    each(("ya", "wat"), ready)
    for r, name in enumerate(("ha", "hb")):
        product(name, "wat", "ya", r)
    each(("yb", "wbt"), ready)
    for r in range(PAIR):
        for c in range(PAIR):
            for kind in ("keep", "turn"):
                res.start(cols(re["ya" if r == 0 else "yb"].out, c), 2 + r, c, kind, *YXZ)
    for r, name in enumerate(("ha", "hb")):
        product(name, "wbt", "yb", r, True)
    each(("ha", "hb"), begin)
    re["h0"].wait(-1, g[0:1])
    res.start(re["h0"].out.at[0], 0, 0, "add", *ZXY)
    each(("ha", "hb"), passed)
    ending()
    for name in (*made, "w0", "w1", "h1", "h0"):
        re[name].finish()
        re[name].swapped()
    for name in ga:
        if name not in WIDE:
            ga[name].finish()
    for r, name in enumerate(("ha", "hb")):
        re[name].wait(-1)
        for c in range(PAIR):
            res.start(cols(re[name].out, c), r, c, "keep", *ZXY)
    for part in [*mv.values(), *(ga[name] for name in ga if name in WIDE)]:
        part.finish()
    res.finish(out)
    for name in re:
        if name in WIDE:
            re[name].finish()
            re[name].swapped()


def solution(mesh):
    def local_fn(l_blk):
        n = l_blk.shape[0] * 8
        groups = scratch_plan(n)
        spec = pl.BlockSpec(memory_space=pltpu.VMEM)
        call = pl.pallas_call(
            functools.partial(whole_kernel, n, [len(group) for group in groups]),
            out_shape=jax.ShapeDtypeStruct(l_blk.shape, F32),
            in_specs=[spec],
            out_specs=spec,
            scratch_shapes=sum(groups, []),
            compiler_params=pltpu.CompilerParams(
                has_side_effects=True, vmem_limit_bytes=VMEM_LIMIT, collective_id=0),
            name="whole",
        )
        return call(l_blk)

    spec = P(("batch", "row"), "col")
    return jax.shard_map(local_fn, mesh=mesh, in_specs=(spec,), out_specs=spec, check_vma=False)
```

```python
import functools

import jax
import jax.numpy as jnp
from jax import lax
from jax.experimental import pallas as pl
from jax.experimental.pallas import tpu as pltpu
from jax.sharding import PartitionSpec as P

MESH = pl.DeviceIdType.MESH
HIGHEST = lax.Precision.HIGHEST
F32 = jnp.float32
VMEM_LIMIT = 67043328
SIDE, PAIR, SUBLANES = 4, 2, 8


def coords():
    col = lax.axis_index("col")
    row = lax.axis_index("row")
    return {"x": row // 2, "y": col % SIDE, "z": col // 4, "e": row % 2}


def device(at):
    return (0, 4 * at["z"] + at["y"], 2 * at["x"] + at["e"])


def same(p, q):
    return (p["x"] == q["x"]) & (p["y"] == q["y"]) & (p["z"] == q["z"]) & (p["e"] == q["e"])


def mm(a, b, dims=((1,), (0,))):
    return lax.dot_general(a, b, (dims, ((), ())), precision=HIGHEST, preferred_element_type=F32)


def loop(count, body):
    def step(k, carry):
        body(k)
        return carry

    lax.fori_loop(0, count, step, jnp.int32(0))


def push(src, dst, send_sem, recv_sem, to, me):
    here = same(to, me)

    @pl.when(here)
    def _():
        dst[...] = src[...]

    @pl.when(jnp.logical_not(here))
    def _():
        pltpu.make_async_remote_copy(
            src_ref=src, dst_ref=dst, send_sem=send_sem, recv_sem=recv_sem, device_id=device(to), device_id_type=MESH
        ).start()


def sent(src, dst, send_sem, recv_sem, to, me):
    @pl.when(jnp.logical_not(same(to, me)))
    def _():
        pltpu.make_async_remote_copy(
            src_ref=src, dst_ref=dst, send_sem=send_sem, recv_sem=recv_sem, device_id=device(to), device_id_type=MESH
        ).wait_send()


def arrived(dst, send_sem, recv_sem, source, me):
    @pl.when(jnp.logical_not(same(source, me)))
    def _():
        pltpu.make_async_remote_copy(
            src_ref=dst, dst_ref=dst, send_sem=send_sem, recv_sem=recv_sem, device_id=device(source), device_id_type=MESH
        ).wait_recv()


def meet(sources, dests, me):
    barrier = pltpu.get_barrier_semaphore()

    def other(cond, at):
        apart = jnp.logical_not(same(at, me))
        return apart if cond is None else apart & cond

    total = jnp.int32(0)
    for cond, count, which in sources:
        def tell(k, which=which):
            @pl.when(other(None, which(k)))
            def _():
                pl.semaphore_signal(barrier, inc=1, device_id=device(which(k)), device_id_type=MESH)

        if cond is None:
            loop(count, tell)
        else:
            @pl.when(cond)
            def _(count=count, tell=tell):
                loop(count, tell)

    for cond, count, which in dests:
        def add(k, carry, cond=cond, which=which):
            return carry + other(cond, which(k)).astype(jnp.int32)

        total = lax.fori_loop(0, count, add, total)

    @pl.when(total > 0)
    def _():
        pl.semaphore_wait(barrier, total)


def remote(src, dst, send_sem, recv_sem, to):
    return pltpu.make_async_remote_copy(
        src_ref=src, dst_ref=dst, send_sem=send_sem, recv_sem=recv_sem, device_id=device(to), device_id_type=MESH)


def invert_block(left, corner, inv, base):
    half = 3 * base
    rows = lax.broadcasted_iota(jnp.int32, (base, base), 0)
    cols = lax.broadcasted_iota(jnp.int32, (base, base), 1)
    eye = rows == cols

    def block(i, j):
        if j < 3:
            return left[i * base:(i + 1) * base, j * base:(j + 1) * base]
        return corner[(i - 3) * base:(i - 2) * base, (j - 3) * base:(j - 2) * base]

    tri = [block(i, i) for i in range(6)]
    found = []
    for i in range(6):
        diag = jnp.sum(jnp.where(eye, tri[i], 0.0), axis=1, keepdims=True)
        found.append(jnp.where(eye, 1.0 / diag, 0.0))
    size = 1
    while size < base:
        below = ((rows // size) % 2 == 1) & (cols // size == rows // size - 1)
        half_way = [mm(jnp.where(below, tri[i], 0.0), found[i]) for i in range(6)]
        found = [found[i] - mm(found[i], half_way[i]) for i in range(6)]
        size = size * 2
    inv[...] = jnp.zeros(inv.shape, F32)
    for k in (0, 3):
        x0, x1, x2 = found[k:k + 3]
        x10 = -mm(x1, mm(block(k + 1, k), x0))
        x21 = -mm(x2, mm(block(k + 2, k + 1), x1))
        x20 = -mm(x2, mm(block(k + 2, k), x0) + mm(block(k + 2, k + 1), x10))
        for i, j, val in ((0, 0, x0), (1, 1, x1), (2, 2, x2), (1, 0, x10), (2, 1, x21), (2, 0, x20)):
            inv[(k + i) * base:(k + i + 1) * base, (k + j) * base:(k + j + 1) * base] = val
    low = mm(left[half:, :], inv[:half, :half])
    inv[half:, :half] = -mm(inv[half:, half:], low)


def stage0(n, me, sources, dests, gather_ct, l_ref, lt_ref, ct_out, d_out, g_out, dt_out,
           left, corner, cmat, inv_a, inv_b, inv_t, slab_d, slab_t, slab_g,
           ct_send, ct_recv, ab_send, ab_recv, c_send, c_recv, x_send, x_recv, t_send, t_recv):
    x, y, z, e = me["x"], me["y"], me["z"], me["e"]
    big = n // 8
    half = n // 16
    quarter = n // 32
    tile = n // 128
    sib = dict(me, e=1 - e)
    diag = x == z

    slot = (x * (x - 1)) // 2 + z
    def ct_args(i):
        g, h, ee = i // 4, i // 2 % 2, i % 2
        rows = pl.ds(pl.multiple_of(quarter * ee + tile * g, SUBLANES), tile)
        src = lt_ref.at[rows, pl.ds(pl.multiple_of(half * h, half), half)]
        to = {"x": g, "y": y, "z": 2 * e + h, "e": ee}
        return src, ct_out.at[slot], ct_send.at[i], ct_recv.at[slot], to, me

    up, down = dict(me, y=(y + 1) % SIDE), dict(me, y=(y + 3) % SIDE)

    def at(b, along_y):
        b = jnp.int32(b)
        return {"x": b, "y": along_y, "z": b, "e": e}

    odd = x % 2

    def dest(kind, i):
        g, j = i // 4, i % SIDE
        if kind == 0:
            return {"x": j, "y": y, "z": g, "e": e}
        if kind == 1:
            return {"x": odd * g + (1 - odd) * j, "y": odd * j + (1 - odd) * g, "z": y, "e": e}
        return {"x": g, "y": j, "z": y, "e": e}

    def full(kind, i):
        return i % SIDE <= y if kind == 0 else i % SIDE >= y

    pairs = [(b_row, b_col) for b_row in range(SIDE) for b_col in range(b_row)]

    def ct_source(b_row, b_col):
        return {"x": x - x + b_row, "y": y, "z": x - x + b_col, "e": z // 2}

    def one(cond, where):
        return cond, 1, lambda k: where

    sources = sources + [one(None, ct_source(*pair)) for pair in pairs] + [one(diag, sib)]
    sources += [one(diag, up), one(diag, down)]
    sources += [(x <= y, 3, lambda b: at(b, y)), (None, 4, lambda b: at(b, z)), one(y >= z, at(1, z))]
    dests = dests + [(x > z, 16, lambda i: ct_args(i)[4]), one(diag, sib)]
    dests += [one(diag, up), one(diag, down)]
    dests += [(diag, 16, lambda i: dest(1, i))]
    for kind, cond in ((0, diag & (x < 3)), (2, diag & (x == 1))):
        dests += [(cond & full(kind, i), 1, lambda k, kind=kind, i=i: dest(kind, jnp.int32(i))) for i in range(16)]

    @pl.when(x > z)
    def _():
        lt_ref[...] = l_ref[...].T

    meet(sources, dests, me)

    place = (y + SIDE - 2 * e) % SIDE
    third = half // 3

    def ab_copies(chunk, way, own):
        dst, first = ((left, 0), (left, half), (corner, 0))[chunk]
        src, start = (l_ref, half * min(chunk, 1)) if own else (dst, first)
        cuts = [(0, half, half)] if chunk == 1 else [(third * i, third, third * i + third) for i in range(3)]
        return [remote(src.at[pl.ds(start + row, tall), pl.ds(0, across)], dst.at[pl.ds(first + row, tall), pl.ds(0, across)],
                       ab_send.at[chunk + 3 * way, i], ab_recv.at[chunk, i], (up, down)[way])
                for i, (row, tall, across) in enumerate(cuts)]

    def ab_came(chunk):
        for copy in ab_copies(chunk, 0, 0):
            copy.wait_recv()

    def ab_start(code):
        for copy in ab_copies(*map(int, code)):
            copy.start()

    ab_sends = [("001", "111", "101", "011"), ("211", "201", "000"), ("200",), ("110",)]

    def c_copy(part, chunk, way, own):
        rows = pl.ds(half * chunk, half)
        dst = cmat.at[part, rows, :]
        src = l_ref.at[rows, :] if own else dst
        return remote(src, dst, c_send.at[chunk + 2 * way], c_recv.at[2 * part + chunk], (up, down)[way])

    def c_came(part, chunk):
        c_copy(part, chunk, 0, 0).wait_recv()

    c_sends = [("0001", "0011", "0101", "0111"), ("1001", "1011", "1101", "1111"), ("1000", "1100"), ("0010", "0110")]

    for part in range(PAIR):
        @pl.when(diag & (place == part))
        def _(part=part):
            for code in ab_sends[part]:
                if int(code[2]):
                    ab_start(code)

    @pl.when(x > z)
    def _():
        loop(16, lambda i: push(*ct_args(i)))

    def swap_args(k):
        mine = [inv_a, inv_b, cmat.at[0], cmat.at[1]][k]
        return mine, mine, x_send.at[k], x_recv.at[k], sib, me

    def swap_came(k):
        arrived(swap_args(k)[1], x_send.at[k], x_recv.at[k], sib, me)

    closing = []

    def spread_ct():
        for k, pair in enumerate(pairs):
            arrived(ct_out.at[k], ct_send.at[0], ct_recv.at[k], ct_source(*pair), me)
        gather_ct()

    @pl.when(jnp.logical_not(diag))
    def _():
        spread_ct()

    @pl.when(diag)
    def _():
        for part, order in enumerate(("2", "01", "201", "102")):
            @pl.when(place == part)
            def _(part=part, order=order):
                if part == 0:
                    left[...] = l_ref[...]
                elif part == 1:
                    corner[...] = l_ref[half:, :]
                for chunk in order:
                    ab_came(int(chunk))
                    if part > 0 and chunk == order[0]:
                        ab_start(ab_sends[part][-1])

        for part in range(PAIR):
            @pl.when((e == 1) & (y == part))
            def _(part=part):
                for code in c_sends[part]:
                    c_copy(*map(int, code)).start()
                cmat[part] = l_ref[...]

        spread_ct()
        invert_block(left, corner, inv_t, n // 48)
        for part in range(PAIR):
            @pl.when((e == 1) & (y == part))
            def _(part=part):
                push(*swap_args(2 + part))

            @pl.when((e == 1) & (y == part + 2))
            def _(part=part):
                c_came(1 - part, 0)
                c_copy(*map(int, c_sends[part + 2][0])).start()

        for core, inv in ((0, inv_a), (1, inv_b)):
            @pl.when(e == core)
            def _(inv=inv):
                inv[...] = inv_t[...]

        lower, across = y >= 2, ((1,), (1,))
        first = pl.multiple_of((y % 2) * half + e * quarter, SUBLANES)
        mine = pl.ds(first, quarter)

        for core in range(PAIR):
            @pl.when(e == core)
            def _(core=core):
                push(*swap_args(core))
                swap_came(1 - core)

        @pl.when(jnp.logical_not(lower))
        def _():
            inv_t[...] = inv_a[...].T
            slab_t[:, :big] = inv_t[mine, :]
            slab_d[:, :big] = inv_a[mine, :]

        @pl.when(lower)
        def _():
            inv_t[...] = inv_b[...].T
            slab_t[:, big:] = inv_t[mine, :]
            slab_g[:, big:] = mm(slab_t[:, big:], inv_b[...])
            slab_d[:, big:] = inv_b[mine, :]

        @pl.when(e == 1)
        def _():
            for part in range(PAIR):
                @pl.when(y == part)
                def _(part=part):
                    c_came(1 - part, 0)
                    c_came(1 - part, 1)
                    push(*swap_args(3 - part))

                @pl.when(y == part + 2)
                def _(part=part):
                    c_came(1 - part, 1)
                    c_copy(*map(int, c_sends[part + 2][1])).start()
                    push(*swap_args(3 - part))
                    c_came(part, 0)
                    c_came(part, 1)
                    push(*swap_args(2 + part))

        @pl.when(e == 0)
        def _():
            swap_came(2)
            swap_came(3)

        def times_c(v):
            return jnp.concatenate([mm(v, cmat[0]), mm(v, cmat[1])], axis=1)

        def spread(kind, i):
            rows = pl.ds(pl.multiple_of(tile * (i // 4), SUBLANES), tile)
            src = (slab_d, slab_g, slab_t)[kind].at[rows, pl.ds(pl.multiple_of(half * (i % SIDE), half), half)]
            dst = (d_out, g_out)[kind].at[x] if kind < 2 else dt_out.at[0]
            recv = t_recv.at[kind, x] if kind < 2 else t_recv.at[2, 0]
            return src, dst, t_send.at[kind * 16 + i], recv, dest(kind, i), me

        def spread_all(use, kind):
            def step(i):
                if kind == 1:
                    use(*spread(kind, i))
                else:
                    @pl.when(full(kind, i))
                    def _():
                        use(*spread(kind, i))

            loop(16, step)

        @pl.when(lower)
        def _():
            slab_d[:, :big] = -mm(times_c(slab_d[:, big:]), inv_a[...])

        @pl.when(x < 3)
        def _():
            spread_all(push, 0)

        @pl.when(jnp.logical_not(lower))
        def _():
            w = mm(slab_t[:, :half], cmat[0], across) + mm(slab_t[:, half:big], cmat[1], across)
            slab_t[:, big:] = -mm(w, inv_b[...], across)

        @pl.when(x == 1)
        def _():
            spread_all(push, 2)

        @pl.when(jnp.logical_not(lower))
        def _():
            slab_g[:, big:] = mm(slab_t[:, big:], inv_b[...])
            slab_g[:, :big] = mm(slab_t[:, :big] - times_c(slab_g[:, big:]), inv_a[...])

        @pl.when(lower)
        def _():
            slab_g[:, :big] = -mm(times_c(slab_g[:, big:]), inv_a[...])

        spread_all(push, 1)

        def close():
            @pl.when(x < 3)
            def _():
                spread_all(sent, 0)

            @pl.when(x == 1)
            def _():
                spread_all(sent, 2)

            spread_all(sent, 1)
            for part in range(SIDE):
                @pl.when(place == part)
                def _(part=part):
                    for code in ab_sends[part]:
                        for copy in ab_copies(*map(int, code)):
                            copy.wait_send()

                @pl.when((e == 1) & (y == part))
                def _(part=part):
                    for code in c_sends[part]:
                        c_copy(*map(int, code)).wait_send()

            for core in range(PAIR):
                @pl.when(e == core)
                def _(core=core):
                    for k in (0,) if core == 0 else (1, 2, 3):
                        sent(*swap_args(k))

        closing.append(close)

    @pl.when(x <= y)
    def _():
        loop(3, lambda b: arrived(d_out.at[b], t_send.at[0], t_recv.at[0, b], at(b, y), me))

    @pl.when(x > y)
    def _():
        d_out[...] = jnp.zeros(d_out.shape, F32)

    def late():
        loop(SIDE, lambda b: arrived(g_out.at[b], t_send.at[0], t_recv.at[1, b], at(b, z), me))

        @pl.when(y >= z)
        def _():
            arrived(dt_out.at[0], t_send.at[0], t_recv.at[2, 0], at(1, z), me)

        @pl.when(y < z)
        def _():
            dt_out[...] = jnp.zeros(dt_out.shape, F32)

    def finish():
        @pl.when(diag)
        def _():
            closing[0]()

        @pl.when(x > z)
        def _():
            loop(16, lambda i: sent(*ct_args(i)))

    return late, finish


def moved(turn, digit, back):
    def to(me):
        return {"x": (me["x"] + me[digit]) % SIDE, "y": me[turn[0]], "z": me[turn[1]], "e": me["e"]}

    def source(me):
        found = dict(me, x=me[back])
        found.update(zip(turn, (me["y"], me["z"])))
        found[digit] = (me["x"] + SIDE - me[back]) % SIDE
        return found

    return to, source, back


W_TURN = moved("zx", "y", "z")
H_TURN = moved("xz", "y", "y")
Y_TURN = moved("xy", "z", "y")
YT_TURN = moved("yx", "z", "z")


class Move:
    def __init__(self, way, me, buf, send, recv):
        (self.to, self.source, self.back), self.me, self.buf, self.send, self.recv = way, me, buf, send, recv

    def args(self):
        return self.src, self.buf, self.send.at[0], self.recv.at[0], self.to(self.me), self.me

    def start(self, src):
        self.src = src
        push(*self.args())

    def wait(self):
        arrived(self.buf, self.send.at[0], self.recv.at[0], self.source(self.me), self.me)

    def finish(self):
        sent(*self.args())


class Line:
    def __init__(self, axis, me):
        self.at = me[axis]
        self.up, self.across, self.down = ((self.at + k) % SIDE for k in (1, 2, 3))
        self.above, self.below = dict(me, **{axis: self.up}), dict(me, **{axis: self.down})


class Gather:
    def __init__(self, axis, me, buf, send, recv):
        self.line, self.buf, self.send, self.recv = Line(axis, me), buf, send, recv
        self.shift = None

    def piece(self, slot, half):
        if len(self.buf.shape) > 3:
            return self.buf.at[slot, pl.ds(half, 1)]
        rows = self.buf.shape[1] // 2
        return self.buf.at[slot, pl.ds(half * rows, rows)]

    def copies(self):
        line, buf = self.line, self.buf
        return [
            remote(self.src, buf.at[line.at], self.send.at[0], self.recv.at[0], line.above),
            remote(self.src, buf.at[line.at], self.send.at[1], self.recv.at[1], line.below),
            remote(self.piece(line.down, 0), self.piece(line.down, 0), self.send.at[2], self.recv.at[2], line.above),
            remote(self.piece(line.up, 1), self.piece(line.up, 1), self.send.at[3], self.recv.at[3], line.below)]

    def start(self, src):
        self.src = src
        for copy in self.copies()[:2]:
            copy.start()
        self.buf[self.line.at] = src[...]

    def relay(self):
        line, buf = self.line, self.buf
        onward = self.copies()[2:]
        remote(buf.at[line.down], buf.at[line.down], self.send.at[0], self.recv.at[0], line.below).wait_recv()
        onward[0].start()
        remote(buf.at[line.up], buf.at[line.up], self.send.at[1], self.recv.at[1], line.above).wait_recv()
        onward[1].start()

    def wait(self):
        for half, whom in ((0, self.line.below), (1, self.line.above)):
            piece = self.piece(self.line.across, half)
            remote(piece, piece, self.send.at[2 + half], self.recv.at[2 + half], whom).wait_recv()

    def finish(self):
        for copy in self.copies():
            copy.wait_send()

    def rows(self, block=None):
        places = [k if self.shift is None else (k + self.shift) % SIDE for k in range(SIDE)]
        tiles = [self.buf[k] if block is None else self.buf[k, block] for k in places]
        return jnp.concatenate(tiles, axis=0)


class Reduce:
    def __init__(self, axis, me, part, sib, half, land, out, s_send, s_recv, r_send, r_recv):
        self.line, self.me, self.part, self.sib, self.half, self.land, self.out = Line(axis, me), me, part, sib, half, land, out
        self.s_send, self.s_recv, self.send, self.recv = s_send, s_recv, r_send, r_recv
        self.other = dict(me, e=1 - me["e"])
        self.down, self.tile = out.shape[:2]

    def swap_args(self, d):
        rows = pl.ds(((1 - self.me["e"]) + 2 * d) * (SIDE * self.tile), SIDE * self.tile)
        return self.part.at[rows, :], self.sib.at[d], self.s_send.at[d], self.s_recv.at[d], self.other, self.me

    def put(self, d, value):
        self.part[d * 8 * self.tile:(d + 1) * 8 * self.tile, :] = value
        push(*self.swap_args(d))

    def where(self, k, half=None):
        first = pl.multiple_of(k * self.tile, SUBLANES)
        if half is None:
            return slice(None), pl.ds(first, self.tile)
        if self.down > 1:
            return pl.ds(half, 1), pl.ds(first, self.tile)
        rows = self.tile // 2
        return slice(None), pl.ds(pl.multiple_of(first + half * rows, SUBLANES), rows)

    def copies(self):
        line, sib = self.line, self.sib
        return [
            remote(sib.at[self.where(line.across, 0)], self.half.at[0], self.send.at[0], self.recv.at[0], line.above),
            remote(sib.at[self.where(line.across, 1)], self.half.at[1], self.send.at[1], self.recv.at[1], line.below),
            remote(sib.at[self.where(line.up)], self.land.at[0], self.send.at[2], self.recv.at[2], line.above),
            remote(sib.at[self.where(line.down)], self.land.at[1], self.send.at[3], self.recv.at[3], line.below)]

    def start(self):
        tile = self.tile
        for d in range(self.down):
            arrived(self.sib.at[d], self.s_send.at[d], self.s_recv.at[d], self.other, self.me)
            first = pl.multiple_of((self.me["e"] + 2 * d) * (4 * tile), SUBLANES)
            self.sib[d] = self.part[pl.ds(first, 4 * tile), :] + self.sib[d]
        for copy in self.copies()[:2]:
            copy.start()

    def relay(self):
        line, copies = self.line, self.copies()
        for half, whom, k in ((0, line.below, line.up), (1, line.above, line.down)):
            got = self.half.at[half]
            remote(got, got, self.send.at[half], self.recv.at[half], whom).wait_recv()
            at = self.where(k, half)
            self.sib[at] = self.sib[at] + self.half[half]
            copies[2 + half].start()

    def wait(self, sign=1, more=None):
        for side, whom in ((0, self.line.below), (1, self.line.above)):
            got = self.land.at[side]
            remote(got, got, self.send.at[2 + side], self.recv.at[2 + side], whom).wait_recv()
        total = (self.land[0] + self.land[1]) + self.sib[self.where(self.line.at)]
        total = total if sign > 0 else -total
        self.out[...] = total if more is None else total + more

    def swapped(self):
        for d in range(self.down):
            sent(*self.swap_args(d))

    def finish(self):
        for copy in self.copies():
            copy.wait_send()


def turn(a, b):
    return mm(a, b, ((0,), (0,)))


class Output:
    def __init__(self, n, me, flat, extra, turned, send, f_recv, a_recv, u_recv):
        self.half, self.tile, self.me, self.send = n // 16, n // 128, me, send
        self.into = {"keep": (flat, f_recv), "add": (extra, a_recv), "turn": (turned, u_recv)}
        self.started = []

    def place(self, kind, h, g, ee):
        buf, recv = self.into[kind]
        first = ee * (SIDE * self.tile) + g * self.tile
        if kind == "turn":
            cols = pl.ds(pl.multiple_of(h * self.half, self.half), self.half)
            return buf.at[pl.ds(pl.multiple_of(first, SUBLANES), self.tile), cols], recv.at[h, g, ee]
        return buf.at[pl.ds(pl.multiple_of(first + h * self.half, SUBLANES), self.tile), :], recv.at[h, g, ee]

    def to(self, plan):
        b_row, b_col, kind, rax, cax, gax = plan
        a_r, a_c = self.me[rax], self.me[cax]
        if kind == "turn":
            return {"x": jnp.int32(b_col), "y": a_r, "z": jnp.int32(b_row), "e": a_c // 2}, a_c % 2
        return {"x": jnp.int32(b_row), "y": a_c, "z": jnp.int32(b_col), "e": a_r // 2}, a_r % 2

    def args(self, index):
        plan, src = self.started[index]
        to, h = self.to(plan)
        dst, recv = self.place(plan[2], h, self.me[plan[5]], self.me["e"])
        return src, dst, self.send.at[index], recv, to, self.me

    def start(self, src, *plan):
        self.started.append((plan, src))
        push(*self.args(len(self.started) - 1))

    def incoming(self, plan):
        b_row, b_col, kind, rax, cax, gax = plan
        to_x, to_z = (b_col, b_row) if kind == "turn" else (b_row, b_col)
        y, e = self.me["y"], self.me["e"]

        def find(i):
            h, g, ee = i // 8, i // 2 % SIDE, i % 2
            a_r, a_c = (y, 2 * e + h) if kind == "turn" else (2 * e + h, y)
            return h, g, ee, {rax: a_r, cax: a_c, gax: g, "e": ee}

        return (self.me["x"] == to_x) & (self.me["z"] == to_z), find

    def finish(self, out):
        for plan, _ in self.started:
            cond, find = self.incoming(plan)

            @pl.when(cond)
            def _(plan=plan, find=find):
                def take(i):
                    h, g, ee, at = find(i)
                    dst, recv = self.place(plan[2], h, g, ee)
                    arrived(dst, self.send.at[0], recv, at, self.me)

                loop(16, take)

        kinds = {}
        for plan, _ in self.started:
            where = (plan[1], plan[0]) if plan[2] == "turn" else plan[:2]
            kinds.setdefault(where, set()).add(plan[2])
        for (b_row, b_col), has in kinds.items():
            @pl.when((self.me["x"] == b_row) & (self.me["z"] == b_col))
            def _(has=has):
                terms = [self.into[kind][0][...] for kind in ("keep", "add") if kind in has]
                if "turn" in has:
                    terms.append(self.into["turn"][0][...].T)
                out[...] = sum(terms[1:], terms[0])
        for index in range(len(self.started)):
            sent(*self.args(index))


ZXY, YXZ, ZYX = tuple("zxy"), tuple("yxz"), tuple("zyx")
PLANS = [(r, c, "keep", *ZXY) for r in range(PAIR) for c in range(PAIR)]
PLANS += [(2 + r, c, kind, *YXZ) for r in range(PAIR) for c in range(PAIR) for kind in ("keep", "turn")]
PLANS += [(0, 0, "add", *ZXY), (1, 1, "add", *ZYX), (2, 2, "keep", *ZXY), (3, 3, "keep", *ZYX)]
PLANS += [(r, r - 1, kind, *YXZ) for r, keep in ((1, "add"), (3, "keep")) for kind in (keep, "turn")]
WIDE = ("wa", "wb", "wat", "wbt", "ya", "yb", "ha", "hb")
GATHERS = [("d0", "z"), ("d1", "z"), ("d2", "z"), ("g1", "x"), ("dt", "x"), ("g3", "x"), ("w0", "y"), ("w1", "y"), ("y0", "z"),
           ("y1", "z"), ("x21", "z"), ("w0t", "x"), ("w1t", "x"), ("g2t", "x"), ("yt1t", "x"), ("y1t", "x"), ("wa", "y"),
           ("wb", "y"), ("wat", "x"), ("wbt", "x"), ("ya", "z"), ("yb", "z")]
GATHERS += [(f"ct{k}", "x") for k in range(6)]
MOVES = [("w0t", W_TURN), ("w1t", W_TURN), ("g2t", H_TURN), ("yt1t", YT_TURN), ("y1t", Y_TURN), ("wat", W_TURN), ("wbt", W_TURN)]
REDUCES = [("w0", "y"), ("w1", "y"), ("x21", "z"), ("y0", "z"), ("y1", "z"), ("yt1", "z"), ("h0", "y"), ("h1", "y"),
           ("wa", "y"), ("wb", "y"), ("ya", "z"), ("yb", "z"), ("ha", "y"), ("hb", "y")]


def scratch_plan(n):
    big, half, quarter, tile = n // 8, n // 16, n // 32, n // 128
    dma, vmem = pltpu.SemaphoreType.DMA, lambda *shape: pltpu.VMEM(shape, F32)
    pairs, four = 6, 4
    groups = [[vmem(pairs, tile, half), vmem(four, tile, half), vmem(four, tile, half), vmem(1, tile, half),
               vmem(big, half), vmem(half, half), vmem(2, big, half)]
              + [vmem(big, big)] * 3 + [vmem(quarter, 2 * big)] * 3
              + [dma((16,)), dma((pairs,)), dma((6, 3)), dma((3, 3)), dma((four,)), dma((four,)), dma((four,)), dma((four,)),
                 dma((48,)), dma((3, four))]]
    def wide(name):
        return 2 * half if name in WIDE else half

    for name, _ in GATHERS:
        groups.append([vmem(four, tile, wide(name)), dma((four,)), dma((four,))])
    for name, _ in MOVES:
        groups.append([vmem(tile, wide(name)), dma((1,)), dma((1,))])
    for name, _ in REDUCES:
        width = wide(name)
        groups.append([vmem(half, width), vmem(1, quarter, width), vmem(2, 1, tile // 2, width), vmem(2, 1, tile, width),
                       vmem(1, tile, width), dma((1,)), dma((1,)), dma((four,)), dma((four,))])
    hubs = dma((2, four, 2))
    groups.append([vmem(big, half), vmem(big, half), vmem(half, big), dma((len(PLANS),)), hubs, hubs, hubs])
    return groups


def whole_kernel(n, sizes, l_ref, out, *refs):
    half = n // 16
    me = coords()
    groups = []
    for size in sizes:
        groups.append(refs[:size])
        refs = refs[size:]
    first, groups = groups[0], groups[1:]
    ga = {name: Gather(axis, me, *group) for (name, axis), group in zip(GATHERS, groups)}
    groups = groups[len(GATHERS):]
    mv = {name: Move(way, me, *group) for (name, way), group in zip(MOVES, groups)}
    groups = groups[len(MOVES):]
    re = {name: Reduce(axis, me, *group) for (name, axis), group in zip(REDUCES, groups)}
    res = Output(n, me, *groups[-1])

    lines = [(None, 4, lambda k, axis=axis: dict(me, **{axis: k})) for axis in "xyz"]
    turns = [W_TURN, H_TURN, Y_TURN, YT_TURN]
    sources = lines + [(None, 1, lambda k, way=way: way[1](me)) for way in turns]
    dests = lines + [(None, 1, lambda k, way=way: way[0](me)) for way in turns]
    for plan in PLANS:
        cond, find = res.incoming(plan)
        sources.append((cond, 16, lambda i, find=find: find(i)[-1]))
        dests.append((None, 1, lambda k, plan=plan: res.to(plan)[0]))
    ct, d, g, dt = first[:4]
    cts = {f"ct{k}": k for k in (0, 5, 1, 2, 3, 4)}

    views = {name: ct.at[k] for name, k in cts.items()}

    def gather_ct():
        for name, src in views.items():
            ga[name].start(src)

    late, ending = stage0(n, me, sources, dests, gather_ct, l_ref, groups[-1][2], *first)

    def ctr(r, c):
        return ga[f"ct{(r * (r - 1)) // 2 + c}"].rows()

    def cols(array, c):
        return array.at[0, :, pl.ds(c * half, half)]

    for name, src in (("d0", d.at[0]), ("d2", d.at[2])):
        ga[name].start(src)

    def each(names, *steps):
        for step in steps:
            for name in names:
                step(name)

    def gathered(name):
        ga[name].relay()

    def ready(name):
        ga[name].wait()

    def begin(name):
        re[name].start()

    def passed(name):
        re[name].relay()

    def turned(name):
        mv[name].wait()
        ga[name].shift = me[mv[name].back]
        ga[name].start(mv[name].buf)

    each(("d0", "d2", "ct0", "ct5"), gathered, ready)
    for name, pair, right in (("w0", (1, 0), "d0"), ("w1", (3, 2), "d2")):
        re[name].put(0, turn(ctr(*pair), ga[right].rows()))
    each(("w0", "w1"), begin, passed)
    late()
    for name, src in (("dt", dt.at[0]), ("g3", g.at[3]), ("g1", g.at[1]), ("d1", d.at[1])):
        ga[name].start(src)
    for name in ("w0", "w1"):
        re[name].wait()
        ga[name].start(re[name].out.at[0])
    for name in ("w1", "w0"):
        mv[name + "t"].start(re[name].out.at[0])
    each(("w0", "w1", "dt", "g3", "g1"), gathered)
    each(("w0", "w1", "dt", "g1", "g3"), ready)
    made = ("x21", "y1", "y0", "yt1")
    for index, (left, right) in enumerate((("dt", "w0"), ("g3", "w1"), ("g1", "w0"), ("w1", "g3"))):
        re[made[index]].put(0, turn(ga[left].rows(), ga[right].rows()))
        if index > 0:
            begin(made[index - 1])
    begin(made[-1])
    each(made[:2], passed)
    for name in ("x21", "y1"):
        re[name].wait(-1)
        ga[name].start(re[name].out.at[0])
    each(("w1t", "w0t"), turned)
    each(made[2:], passed)

    def half_h(name, left, right):
        re[name].put(0, turn(ga[left].rows(), ga[right].rows()))

    tops = [f"ct{k}" for k in range(1, 5)]
    each(("x21", "y1", "w1t", "d1", *tops), gathered)
    each(("y1", "w1t"), ready)
    half_h("h1", "w1t", "y1")
    each(("x21", "d1", *tops), ready)
    res.start(g.at[1], 1, 1, "add", *ZYX)
    res.start(g.at[3], 3, 3, "keep", *ZYX)
    for kind in ("keep", "turn"):
        res.start(re["y1"].out.at[0], 3, 2, kind, *YXZ)
    zero, one = ga["d0"].rows(), jnp.concatenate([ga["x21"].rows(), ga["d1"].rows()], axis=1)
    for r, name in enumerate(("wa", "wb")):
        if r == 1:
            begin("h1")
        top = turn(ctr(2 + r, 1), one)
        re[name].put(0, jnp.concatenate([top[:, :half] + turn(ctr(2 + r, 0), zero), top[:, half:]], axis=1))
    passed("h1")
    each(("wa", "wb"), begin)
    for name in ("y0", "yt1"):
        re[name].wait(-1)
    ga["y0"].start(re["y0"].out.at[0])
    for name in ("yt1", "y1"):
        mv[name + "t"].start(re[name].out.at[0])
    each(("wa", "wb"), passed)
    re["h1"].wait(-1, g[2:3])
    mv["g2t"].start(re["h1"].out.at[0])
    each(("yt1t", "y1t"), turned)
    each(("w0t", "y0"), gathered)
    turned("g2t")
    for name in ("wa", "wb"):
        re[name].wait()
        ga[name].start(re[name].out.at[0])
    each(("yt1t", "y1t", "g2t"), gathered)

    def product(name, left, right, r=None, more=False):
        lhs = ga[left].rows()
        lhs = lhs if r is None else lhs[:, r * half:(r + 1) * half]
        value = turn(lhs, ga[right].rows())
        if more:
            re[name].put(0, re[name].part[...] + value)
        else:
            re[name].part[...] = value

    each(("wa", "wb"), gathered)
    each(("wa", "g2t", "yt1t"), ready)
    product("ya", "g2t", "wa")
    product("yb", "yt1t", "wa")
    each(("wb", "y1t"), ready)
    for name in ("wa", "wb"):
        mv[name + "t"].start(re[name].out.at[0])
    product("ya", "y1t", "wb", more=True)
    product("yb", "g3", "wb", more=True)
    for kind in ("add", "turn"):
        res.start(re["y0"].out.at[0], 1, 0, kind, *YXZ)
    res.start(re["h1"].out.at[0], 2, 2, "keep", *ZXY)
    each(("ya", "yb"), begin)
    each(("w0t", "y0"), ready)
    half_h("h0", "w0t", "y0")
    each(("ya", "yb"), passed)
    begin("h0")
    for name in ("ya", "yb"):
        re[name].wait(-1)
        ga[name].start(re[name].out.at[0])
    passed("h0")
    each(("wat", "wbt"), turned)
    each(("ya", "yb", "wat", "wbt"), gathered)
    each(("ya", "wat"), ready)
    for r, name in enumerate(("ha", "hb")):
        product(name, "wat", "ya", r)
    each(("yb", "wbt"), ready)
    for r in range(PAIR):
        for c in range(PAIR):
            for kind in ("keep", "turn"):
                res.start(cols(re["ya" if r == 0 else "yb"].out, c), 2 + r, c, kind, *YXZ)
    for r, name in enumerate(("ha", "hb")):
        product(name, "wbt", "yb", r, True)
    each(("ha", "hb"), begin)
    re["h0"].wait(-1, g[0:1])
    res.start(re["h0"].out.at[0], 0, 0, "add", *ZXY)
    each(("ha", "hb"), passed)
    ending()
    for name in (*made, "w0", "w1", "h1", "h0"):
        re[name].finish()
        re[name].swapped()
    for name in ga:
        if name not in WIDE:
            ga[name].finish()
    for r, name in enumerate(("ha", "hb")):
        re[name].wait(-1)
        for c in range(PAIR):
            res.start(cols(re[name].out, c), r, c, "keep", *ZXY)
    for part in [*mv.values(), *(ga[name] for name in ga if name in WIDE)]:
        part.finish()
    res.finish(out)
    for name in re:
        if name in WIDE:
            re[name].finish()
            re[name].swapped()


def solution(mesh):
    def local_fn(l_blk):
        n = l_blk.shape[0] * 8
        groups = scratch_plan(n)
        spec = pl.BlockSpec(memory_space=pltpu.VMEM)
        call = pl.pallas_call(
            functools.partial(whole_kernel, n, [len(group) for group in groups]),
            out_shape=jax.ShapeDtypeStruct(l_blk.shape, F32),
            in_specs=[spec],
            out_specs=spec,
            scratch_shapes=sum(groups, []),
            compiler_params=pltpu.CompilerParams(
                has_side_effects=True, vmem_limit_bytes=VMEM_LIMIT, collective_id=0),
            name="whole",
        )
        return call(l_blk)

    spec = P(("batch", "row"), "col")
    return jax.shard_map(local_fn, mesh=mesh, in_specs=(spec,), out_specs=spec, check_vma=False)
```
